32 devices in a mesh: groups: 2 (over y), wide: 8 (over z, x), narrow: 2 (over core).
Axes of the slice: x: 2, y: 2, z: 4, core: 2. Of those that a mesh axis runs over, the one named last changes fastest.
Arguments:
- hidden_in: bfloat16 [6400, 1024], P(('groups', 'wide')), parts along dimension 0, may hold values from -6 to 6
- ffn_gain: bfloat16 [1024], replicated, may hold values from 0.5 to 1.5
- wi_gate: bfloat16 [1024, 2816], P('wide', 'narrow'), may hold values from -0.1875 to 0.1875
- wi_up: bfloat16 [1024, 2816], P('wide', 'narrow'), may hold values from -0.1875 to 0.1875
- wo_down: bfloat16 [2816, 1024], P('narrow', 'wide'), may hold values from -0.109375 to 0.109375
- final_gain: bfloat16 [1024], replicated, may hold values from 0.5 to 1.5
- key_w: bfloat16 [1024, 1024], P('wide', 'narrow'), may hold values from -0.1875 to 0.1875
- value_w: bfloat16 [1024, 1024], P('wide', 'narrow'), may hold values from -0.1875 to 0.1875
- query_w: bfloat16 [1024, 1024], P('wide', 'narrow'), may hold values from -8 to 8
- out_w: bfloat16 [1024, 1024], P('narrow', 'wide'), may hold values from -0.1875 to 0.1875
- dec_gain: bfloat16 [1024], replicated, may hold values from 0.5 to 1.5
- embed: bfloat16 [32128, 1024], P('wide'), may hold values from -6 to 6
- lengths: int32 [32], P(('groups', 'wide')), parts along dimension 0, may hold values from 40 to 200
- answer_ids: int32 [8, 32], P('groups'), parts along dimension 0, may hold values from 0 to 32127
Outputs:
- memory: bfloat16 [6400, 1024], P(('groups', 'wide')), parts along dimension 0
- decoded: bfloat16 [256, 1024], P('groups', 'narrow'), parts along dimension 0
The draws below stay inside these ranges and needn't reach their ends.
There are 2 independent parts, one for each index of `groups`. The reference program is written for one: setup_inputs(seed, part) draws one part's arguments, and reference() takes and returns one part's arrays. A program takes and returns all parts, laid end to end along the dimension named above; an argument that names none is the same for every part. Nothing has to cross between parts.
All inputs are finite; a program needn't handle non-finite values.
Results may differ from the reference program's by a relative error of at most 0.0095.
The reference program's roundings to bfloat16 on the way (of `enc_in`, `inner`, `embedded`, `dec_in`, `query` and `attended`) count: a program that leaves them out, or rounds other values in their place, can miss the bound.
Values may be sent and summed in bfloat16 or wider, within the bound.
A program may use at most 64 MiB of HBM per device.

```python
import math
import jax
import jax.numpy as jnp
from jax import lax

D = 1024
HEADS = 16
HEAD_DIM = 64
FF = 2816
VOCAB = 32128
SEG = 200
QUEST = 4
ANS = 32
PASSAGES = 16
TOKENS = 3200
PER_Q = 4
QROWS = 128


def draw_query_w(key, part):
    base = jax.random.normal(jax.random.fold_in(key, 11), (D, D), jnp.float32)
    picked = jax.random.permutation(jax.random.fold_in(key, 12), HEADS)[:2]
    column_head = jnp.arange(D, dtype=jnp.int32) // HEAD_DIM
    strengths = jnp.array([60.0, 100.0], jnp.float32)
    factor = jnp.ones((D,), jnp.float32)
    factor = jnp.where(column_head == picked[0], strengths[0], factor)
    factor = jnp.where(column_head == picked[1], strengths[1], factor)
    scaled = base * (factor / math.sqrt(D))[None, :]
    return jnp.clip(scaled, -8.0, 8.0).astype(jnp.bfloat16)


def set_ends(result, own_key, least, largest):
    place = [jax.random.randint(jax.random.fold_in(own_key, axis), (), 0, length) for axis, length in enumerate(result.shape)]
    longest = result.shape.index(max(result.shape))
    neighbour = place[:longest] + [(place[longest] + 1) % result.shape[longest]] + place[longest + 1:]
    return result.at[tuple(place)].set(least).at[tuple(neighbour)].set(largest)


def shard_levels(rng, shape, split, low, top_value):
    factor_of, own = 1.0, jax.random.fold_in(rng, 6)
    for axis_at, shards_of in split:
        heights = jnp.exp(jax.random.uniform(jax.random.fold_in(own, axis_at), (shards_of,), jnp.float32, low / len(split), top_value / len(split)))
        factor_of = factor_of * jnp.repeat(heights, shape[axis_at] // shards_of).reshape([-1 if axis == axis_at else 1 for axis in range(len(shape))])
    return factor_of


def normal_values(own_key, dims, width, reach, shards=(), kind=jnp.bfloat16):
    drawn = width * jax.random.normal(own_key, dims, jnp.float32)
    if shards:
        drawn = drawn * shard_levels(own_key, dims, shards, -0.22, 0.18)
    return jnp.clip(drawn, -reach, reach).astype(kind)


def setup_inputs(seed: int = 0, part: int = 0) -> dict:
    splits = jax.random.split(jax.random.key(seed), 15)
    part_keys = jax.random.split(jax.random.fold_in(splits[14], part), 15)
    return {
        "hidden_in": normal_values(part_keys[0], (TOKENS, D), 1.0, 6.0, ((0, 8),)),
        "ffn_gain": jnp.clip(1.0 + 0.1 * jax.random.normal(splits[1], (D,), jnp.float32), 0.5, 1.5).astype(jnp.bfloat16),
        "wi_gate": normal_values(splits[2], (D, FF), D ** -0.5, 0.1875, ((0, 8), (1, 2))),
        "wi_up": normal_values(splits[3], (D, FF), D ** -0.5, 0.1875, ((0, 8), (1, 2))),
        "wo_down": normal_values(splits[4], (FF, D), FF ** -0.5, 0.109375, ((0, 2), (1, 8))),
        "final_gain": jnp.clip(1.0 + 0.1 * jax.random.normal(splits[5], (D,), jnp.float32), 0.5, 1.5).astype(jnp.bfloat16),
        "key_w": normal_values(splits[6], (D, D), D ** -0.5, 0.1875, ((0, 8), (1, 2))),
        "value_w": normal_values(splits[7], (D, D), D ** -0.5, 0.1875, ((0, 8), (1, 2))),
        "query_w": draw_query_w(jax.random.fold_in(splits[14], 71), part),
        "out_w": normal_values(splits[9], (D, D), D ** -0.5, 0.1875, ((0, 2), (1, 8))),
        "dec_gain": jnp.clip(1.0 + 0.1 * jax.random.normal(splits[10], (D,), jnp.float32), 0.5, 1.5).astype(jnp.bfloat16),
        "embed": normal_values(splits[11], (VOCAB, D), 1.0, 6.0, ((0, 8),)),
        "lengths": set_ends(jax.random.randint(part_keys[12], (PASSAGES,), SEG // 5, SEG + 1), jax.random.fold_in(part_keys[12], 1), SEG // 5, SEG).astype(jnp.int32),
        "answer_ids": set_ends(jax.random.randint(part_keys[13], (QUEST, ANS), 0, VOCAB), jax.random.fold_in(part_keys[13], 1), 0, VOCAB - 1).astype(jnp.int32),
    }


EPS = 1e-06
FLOOR = -1e+30

def rms_scale(values, gain):
    mean_square = lax.optimization_barrier(jnp.mean(values * values, axis=-1, keepdims=True))
    return values * lax.rsqrt(mean_square + EPS) * gain.astype(jnp.float32)

def reference(hidden_in, ffn_gain, wi_gate, wi_up, wo_down, final_gain, key_w, value_w, query_w, out_w, dec_gain, embed, lengths, answer_ids):

    def encode(block):
        resid_in = block.astype(jnp.float32)
        enc_in = rms_scale(resid_in, ffn_gain).astype(jnp.bfloat16)
        gate = jnp.dot(enc_in, wi_gate, preferred_element_type=jnp.float32)
        up = jnp.dot(enc_in, wi_up, preferred_element_type=jnp.float32)
        inner = (jax.nn.gelu(gate, approximate=True) * up).astype(jnp.bfloat16)
        resid = resid_in + jnp.dot(inner, wo_down, preferred_element_type=jnp.float32)
        memory = rms_scale(resid, final_gain).astype(jnp.bfloat16)
        keys = jnp.dot(memory, key_w, preferred_element_type=jnp.float32).astype(jnp.bfloat16)
        values = jnp.dot(memory, value_w, preferred_element_type=jnp.float32).astype(jnp.bfloat16)
        return (memory, keys, values)
    blocks = hidden_in.reshape(PASSAGES, SEG, D)
    memory, keys, values = lax.map(encode, blocks)
    flat_ids = answer_ids.reshape(QROWS)
    embedded = jnp.take(embed, flat_ids, axis=0)
    dec_in = rms_scale(embedded.astype(jnp.float32), dec_gain).astype(jnp.bfloat16)
    query = jnp.dot(dec_in, query_w, preferred_element_type=jnp.float32).astype(jnp.bfloat16)
    query_four = query.reshape(QUEST, ANS, HEADS, HEAD_DIM).astype(jnp.float32)
    keys_four = keys.reshape(QUEST, PER_Q * SEG, HEADS, HEAD_DIM).astype(jnp.float32)
    values_four = values.reshape(QUEST, PER_Q * SEG, HEADS, HEAD_DIM).astype(jnp.float32)
    position = jnp.arange(SEG, dtype=jnp.int32)
    live = (position[None, :] < lengths[:, None]).reshape(QUEST, PER_Q * SEG)
    scores = jnp.einsum('qahd,qkhd->qahk', query_four, keys_four, precision=lax.Precision.HIGHEST) * (1.0 / math.sqrt(HEAD_DIM))
    scores = jnp.where(live[:, None, None, :], scores, FLOOR)
    weights = jax.nn.softmax(scores, axis=-1)
    attended = jnp.einsum('qahk,qkhd->qahd', weights, values_four, precision=lax.Precision.HIGHEST)
    attended = attended.reshape(QROWS, D).astype(jnp.bfloat16)
    decoded = embedded.astype(jnp.float32) + jnp.dot(attended, out_w, preferred_element_type=jnp.float32)
    return (memory.reshape(TOKENS, D), decoded.astype(jnp.bfloat16))
```

```python
import functools
import math

import jax
import jax.numpy as jnp
from jax import lax
from jax.experimental import pallas as pl
from jax.experimental.pallas import tpu as pltpu
from jax.sharding import PartitionSpec as P

HEAD_DIM = 64
QUEST = 4


EPS = 1e-06
FLOOR = -1e30


def swap(values, axis, distance=1):
    pairs = [(i, i ^ distance) for i in range(lax.axis_size(axis))]
    return jax.tree.map(lambda a: lax.ppermute(a, axis, pairs), values)


def ordered(bit, own, other, dim):
    first = jnp.where(bit == 0, own, other)
    second = jnp.where(bit == 0, other, own)
    return jnp.concatenate([first, second], axis=dim)


def part(values, index, count, dim):
    size = values.shape[dim] // count
    return lax.dynamic_slice_in_dim(values, index * size, size, dim)


def line_gather(block, place, count):
    size = lax.axis_size("wide")
    stride = size // count
    if count > 8:
        groups = [[i * stride + j for i in range(count)] for j in range(stride)]
        return lax.all_gather(block, "wide", axis_index_groups=groups)
    up = [(i, i + stride) for i in range(size - stride)]
    down = [(i + stride, i) for i in range(size - stride)]
    below, above = [], []
    from_below = from_above = block
    for _ in range(count - 1):
        from_below = lax.ppermute(from_below, "wide", up)
        from_above = lax.ppermute(from_above, "wide", down)
        below.insert(0, from_below)
        above.append(from_above)
    return lax.dynamic_slice_in_dim(
        jnp.stack(below + [block] + above), count - 1 - place, count, 0
    )


def rms_scale(values, gain):
    mean_square = jnp.mean(values * values, axis=-1, keepdims=True)
    return values * lax.rsqrt(mean_square + EPS) * gain.astype(jnp.float32)


def add_rows(left, piece):
    return jnp.dot(left, piece, preferred_element_type=jnp.float32)


def join_partial(first, second):
    top = jnp.maximum(first[0], second[0])
    factor_first = jnp.exp(first[0] - top)
    factor_second = jnp.exp(second[0] - top)
    return (
        top,
        first[1] * factor_first + second[1] * factor_second,
        first[2] * factor_first + second[2] * factor_second,
    )


def per_device_any(
    hidden_in,
    ffn_gain,
    wi_gate,
    wi_up,
    wo_down,
    final_gain,
    key_w,
    value_w,
    query_w,
    out_w,
    dec_gain,
    embed,
    lengths,
    answer_ids,
):
    rows, features = hidden_in.shape
    wide = lax.axis_size("wide")
    group, place, core = (lax.axis_index(a) for a in ("groups", "wide", "narrow"))
    side, pair = place % 2, place // 2
    pairs = wide // 2
    quarters = 2 * lax.axis_size("groups")
    lanes = 128

    def for_side(target, pieces):
        quarter = target * (quarters // 2) + group
        return jnp.concatenate(
            [part(a, quarter, quarters, dim).reshape(-1, lanes) for a, dim in pieces]
        )

    def paired(pieces):
        own = for_side(side, pieces)
        other = swap(for_side(1 - side, pieces), "wide")
        return ordered(side, own[None], other[None], 0)

    def gathered(both):
        return line_gather(both, pair, pairs).reshape(wide, *both.shape[1:])

    hidden_units = wi_gate.shape[1] // quarters
    depth = wi_gate.shape[0]
    ffn = gathered(paired(((wi_gate.T, 0), (wi_up.T, 0), (wo_down, 0))))
    ffn = ffn.reshape(wide, 3, hidden_units, depth).transpose(1, 2, 0, 3)
    gate_t, up_t, down = ffn.reshape(3, hidden_units, features)

    def over_plane(own):
        couple = jnp.concatenate([own, swap(own, "wide")])
        return jnp.concatenate([couple, swap(couple, "groups")])

    def both_halves(own):
        return ordered(core, own, swap(own, "narrow"), 1)

    answers = answer_ids.shape[1]
    per_question = wide // QUEST
    qrows = answer_ids.shape[0] * answers
    vocab_rows = embed.shape[0]
    local_ids = answer_ids.reshape(qrows) - place * vocab_rows
    onehot = (local_ids[:, None] == jnp.arange(vocab_rows, dtype=jnp.int32)[None, :]).astype(
        jnp.bfloat16
    )
    found = jnp.dot(onehot, embed, preferred_element_type=jnp.float32).astype(jnp.bfloat16)
    found = part(found, core, 2, 1)
    distance = wide // 2
    while distance:
        if distance >= per_question:
            bit = place // distance % 2
            found = part(found, bit, 2, 0) + swap(part(found, 1 - bit, 2, 0), "wide", distance)
        else:
            found = found + swap(found, "wide", distance)
        distance //= 2
    embedded_half = found.astype(jnp.float32)
    dec_own = rms_scale(both_halves(found).astype(jnp.float32), dec_gain).astype(jnp.bfloat16)
    dec_in = jnp.concatenate([dec_own, swap(dec_own, "groups")])

    columns = key_w.shape[1] // quarters
    att_pair = paired(((key_w, 1), (value_w, 1), (query_w, 1), (out_w, 0)))
    lengths_all = over_plane(lengths)

    resid_in = hidden_in.astype(jnp.float32)
    enc_own = rms_scale(resid_in, ffn_gain).astype(jnp.bfloat16)
    enc_in = both_halves(over_plane(part(enc_own, core, 2, 1)))
    enc_in, dec_in, lengths_all, att_pair, embedded_half = lax.optimization_barrier(
        (enc_in, dec_in, lengths_all, att_pair, embedded_half)
    )
    contract_last = (((1,), (1,)), ((), ()))
    gate = lax.dot_general(enc_in, gate_t, contract_last, preferred_element_type=jnp.float32)
    up = lax.dot_general(enc_in, up_t, contract_last, preferred_element_type=jnp.float32)
    inner = (jax.nn.gelu(gate, approximate=True) * up).astype(jnp.bfloat16)
    sent_half = add_rows(inner, part(down, 1 - core, 2, 1))
    received_half = swap(sent_half, "narrow")
    sums = add_rows(inner, part(down, core, 2, 1)) + received_half

    def keep_half(values):
        return part(values, core, 2, 1) + swap(part(values, 1 - core, 2, 1), "narrow")

    blocks = sums.reshape(4, rows, -1)
    middle = blocks.shape[2] // 2
    early, late = blocks[:, :, :middle], blocks[:, :, middle:]
    early = early[:2] + swap(early[2:], "groups")
    late = late[::2] + swap(late[1::2], "wide")
    early = early[0] + swap(early[1], "wide")
    late = late[0] + swap(late[1], "groups")
    share = jnp.concatenate([early, late], axis=1)
    resid_half = part(resid_in, core, 2, 1) + share
    own_squares = jnp.sum(resid_half * resid_half, axis=1)
    squares = (own_squares + swap(own_squares, "narrow"))[:, None]
    gain_half = part(final_gain, core, 2, 0).astype(jnp.float32)
    memory_half = (resid_half * lax.rsqrt(squares / features + EPS) * gain_half).astype(
        jnp.bfloat16
    )
    memory_early, memory_late = memory_half[:, :middle], memory_half[:, middle:]
    twin = jnp.stack([memory_late, swap(memory_late, "groups")])
    late_all = jnp.stack([twin, swap(twin, "wide")], axis=1).reshape(4 * rows, middle)
    early_all = over_plane(memory_early)
    early_other, late_other = swap(early_all, "narrow"), swap(late_all, "narrow")
    other_half = jnp.concatenate([early_other[:rows], late_other[:rows]], axis=1)
    memory = ordered(core, memory_half, other_half, 1)

    att = gathered(att_pair)
    att = att.reshape(wide, 4, -1)
    key_q, value_q, query_q = (att[:, i].reshape(features, columns) for i in range(3))
    out_q = att[:, 3].reshape(wide, columns, depth).transpose(1, 0, 2).reshape(columns, features)

    def project(weight):
        own, other = part(weight, core, 2, 0), part(weight, 1 - core, 2, 0)
        return (
            add_rows(early_all, own[:middle])
            + add_rows(late_all, own[middle:])
            + add_rows(early_other, other[:middle])
            + add_rows(late_other, other[middle:])
        ).astype(jnp.bfloat16)

    heads = columns // HEAD_DIM
    keys = project(key_q).reshape(2, 2 * rows, columns)
    values = project(value_q).reshape(2, 2 * rows, columns).astype(jnp.float32)
    query = add_rows(dec_in, query_q).astype(jnp.bfloat16)
    in_head = (
        jnp.arange(columns, dtype=jnp.int32)[None, :] // HEAD_DIM
        == jnp.arange(heads, dtype=jnp.int32)[:, None]
    )[None, :, None, :]
    query_heads = jnp.where(in_head, query.reshape(2, 1, answers, columns), 0)
    scores = jnp.einsum(
        "qhac,qkc->qhak", query_heads, keys, preferred_element_type=jnp.float32
    ) * (1.0 / math.sqrt(HEAD_DIM))
    passage_len = rows // lengths.shape[0]
    live = jnp.arange(passage_len, dtype=jnp.int32)[None, :] < lengths_all[:, None]
    scores = jnp.where(live.reshape(2, 1, 1, 2 * rows), scores, FLOOR)
    top = jnp.max(scores, axis=3, keepdims=True)
    weights = jnp.exp(scores - top)
    total = jnp.sum(weights, axis=3, keepdims=True)
    acc = jnp.einsum("qhak,qkc->qhac", weights, values, precision=lax.Precision.HIGHEST)
    state = (top, total, acc)
    distance = 2
    while distance < per_question:
        state = join_partial(state, swap(state, "wide", distance))
        distance *= 2
    attended = jnp.sum(jnp.where(in_head, state[2] / state[1], 0.0), axis=1)
    attended = attended.astype(jnp.bfloat16).reshape(2 * answers, columns)
    partial_out = keep_half(jnp.dot(attended, out_q, preferred_element_type=jnp.float32))
    share_out = partial_out[:answers] + swap(partial_out[answers:], "groups")
    share_out = share_out + swap(share_out, "wide")
    decoded = (embedded_half + share_out).astype(jnp.bfloat16)
    distance = per_question
    while distance < wide:
        decoded = ordered(place // distance % 2, decoded, swap(decoded, "wide", distance), 0)
        distance *= 2
    return (memory, decoded)


MESH = pl.DeviceIdType.MESH
PLANES = 4
CHIPS = 4
CORES = 2
QUANT = 32767.0


def dot_t(left, right):
    return lax.dot_general(
        left, right, (((1,), (1,)), ((), ())), preferred_element_type=jnp.float32
    )


def reader(
    hid,
    gain_in,
    gate_w,
    up_w,
    down_w,
    gain_out,
    key_w,
    value_w,
    query_w,
    out_w,
    gain_dec,
    embed,
    lens,
    ids,
    memory_out,
    decoded_out,
    turned,
    gu,
    gu_side,
    dn,
    at,
    at_side,
    enc,
    acts,
    inner,
    table,
    part_own,
    part_out,
    part_in,
    share_out,
    share_in,
    resid,
    mem,
    found,
    found_in,
    pair_out,
    pair_in,
    half_in,
    lens_all,
    weight_k,
    weight_v,
    weight_q,
    weight_o,
    keys,
    values,
    tail_out,
    tail_in,
    tail_sum,
    tail_pair,
    dec_all,
    gu_s,
    gu_r,
    dn_s,
    dn_r,
    at_s,
    at_r,
    at_ys,
    at_yr,
    x_s,
    enc_s,
    enc_r,
    part_s,
    part_r,
    share_s,
    share_r,
    emb_s,
    emb_r,
    one_s,
    one_r,
    mem_s,
    mem_r,
    dec_s,
    dec_r,
    table_sem,
):
    y, place, n = (lax.axis_index(a) for a in ("groups", "wide", "narrow"))
    z, x = place // 2, place % 2
    upper = z // 2
    w = z + upper * (PLANES - 1 - 2 * z)

    def plane(mirrored):
        return mirrored + upper * (PLANES - 1 - 2 * mirrored)

    order = [z, plane(1 - w), plane(2), plane(3)]
    slot_rows = hid.shape[0]
    unit = gu.shape[2] // 2
    head_cols = at.shape[4]

    def on(x_at, y_at, z_at, n_at):
        return {"groups": y_at, "wide": z_at * 2 + x_at, "narrow": n_at}

    across = on(1 - x, y, z, n)
    aside = on(x, 1 - y, z, n)
    corner = on(1 - x, 1 - y, z, n)
    twin = on(x, y, z, 1 - n)
    next_a = on(x, y, order[1], n)
    next_b = on(x, y, plane(2), n)
    inside = w == 1
    pending = []

    def send(source, target, send_sem, recv_sem, device, cond=None):
        def copy():
            return pltpu.make_async_remote_copy(
                source, target, send_sem, recv_sem, device_id=device, device_id_type=MESH
            )

        if cond is None:
            copy().start()
        else:
            pl.when(cond)(lambda: copy().start())
        pending.append((copy, cond))

    def arrived(target, recv_sem):
        pltpu.make_async_remote_copy(
            target, target, recv_sem, recv_sem, device_id=twin, device_id_type=MESH
        ).wait_recv()

    barrier = pltpu.get_barrier_semaphore()
    peers = [across, aside, corner, twin]
    peers += [on(x, y, (z + d) % PLANES, n) for d in range(1, PLANES)]
    for peer in peers:
        pl.semaphore_signal(barrier, inc=1, device_id=peer, device_id_type=MESH)

    table_copy = pltpu.make_async_copy(
        embed.at[:, pl.ds(pl.multiple_of(n * table.shape[1], 128), table.shape[1])],
        table,
        table_sem,
    )
    table_copy.start()

    lanes = 128
    for k in range(gate_w.shape[1] // lanes):
        cols = pl.ds(k * lanes, lanes)
        turned[0, cols, :] = gate_w[:, cols].T
        turned[1, cols, :] = up_w[:, cols].T
    mine = pl.multiple_of((2 * x + y) * unit, 16)
    theirs = pl.multiple_of((2 * (1 - x) + y) * unit, 16)
    for j in range(2):
        gu_side[pl.ds(j * unit, unit), :] = turned[j, pl.ds(theirs, unit), :]
        gu[z, x, pl.ds(j * unit, unit), :] = turned[j, pl.ds(mine, unit), :]
    dn[z, x] = down_w[pl.ds(mine, unit), :]
    col_mine = pl.multiple_of((2 * x + y) * head_cols, head_cols)
    col_theirs = pl.multiple_of((2 * (1 - x) + y) * head_cols, head_cols)
    depth = key_w.shape[0]
    for j, array in enumerate((key_w, value_w, query_w)):
        rows = pl.ds(j * depth, depth)
        at[0, z, x, rows, :] = array[:, pl.ds(col_mine, head_cols)]
        at_side[rows, :] = array[:, pl.ds(col_theirs, head_cols)]
    at[0, z, x, pl.ds(3 * depth, head_cols), :] = out_w[pl.ds(col_mine, head_cols), :]
    at_side[pl.ds(3 * depth, head_cols), :] = out_w[pl.ds(col_theirs, head_cols), :]
    lens_all[x] = lens[...]

    pl.semaphore_wait(barrier, len(peers))

    def stream(buf, s_sem, r_sem, k, side):
        at_z = order[k]
        if k == 0:
            send(buf.at[at_z, side], buf.at[at_z, side], s_sem.at[0, side], r_sem.at[at_z, side], next_a)
            send(buf.at[at_z, side], buf.at[at_z, side], s_sem.at[4, side], r_sem.at[at_z, side], next_b, inside)
        else:
            target = next_b if k == 1 else next_a
            send(buf.at[at_z, side], buf.at[at_z, side], s_sem.at[k, side], r_sem.at[at_z, side], target, inside)

    def got(buf, r_sem, k, side):
        arrived(buf.at[order[k], side], r_sem.at[order[k], side])

    send(gu_side, gu.at[z, x], x_s.at[0], gu_r.at[z, x], across)
    stream(gu, gu_s, gu_r, 0, x)
    stream(dn, dn_s, dn_r, 0, x)

    hidden = hid[...].astype(jnp.float32)
    slot = (2 * x + y) * CORES + n
    enc[slot] = rms_scale(hidden, gain_in[...]).astype(jnp.bfloat16)
    for j, peer in enumerate((across, aside, twin)):
        send(enc.at[slot], enc.at[slot], enc_s.at[j], enc_r.at[slot], peer)
    send(down_w.at[pl.ds(theirs, unit), :], dn.at[z, x], x_s.at[1], dn_r.at[z, x], across)
    send(lens_all.at[x], lens_all.at[x], x_s.at[3], one_r.at[0], across)

    got(gu, gu_r, 0, 1 - x)
    stream(gu, gu_s, gu_r, 0, 1 - x)
    got(gu, gu_r, 1, x)
    stream(gu, gu_s, gu_r, 1, x)
    got(gu, gu_r, 1, 1 - x)
    stream(gu, gu_s, gu_r, 1, 1 - x)

    feat_half = enc.shape[2] // 2
    slot_x = (2 * (1 - x) + y) * CORES + n
    slot_y = (2 * x + 1 - y) * CORES + n
    slot_d = (2 * (1 - x) + 1 - y) * CORES + n
    arrived(enc.at[slot_x], enc_r.at[slot_x])
    left = enc.at[slot_x, :, pl.ds(0, feat_half)]
    send(left, left, enc_s.at[3], enc_r.at[8], aside)
    arrived(enc.at[slot_y], enc_r.at[slot_y])
    right = enc.at[slot_y, :, pl.ds(feat_half, feat_half)]
    send(right, right, enc_s.at[4], enc_r.at[9], across)
    send(enc.at[slot_x], enc.at[slot_x], enc_s.at[5], enc_r.at[slot_x], twin)
    send(enc.at[slot_y], enc.at[slot_y], enc_s.at[6], enc_r.at[slot_y], twin)
    send(at_side, at.at[0, z, x], x_s.at[2], at_r.at[z, x], across)

    got(gu, gu_r, 2, x)
    stream(gu, gu_s, gu_r, 2, x)

    table_copy.wait()
    vocab = table.shape[0]
    chunk = 1024
    hits = jnp.zeros((ids.shape[1], table.shape[1]), jnp.float32)
    for base in range(0, vocab, chunk):
        size = min(chunk, vocab - base)
        row = lax.broadcasted_iota(jnp.int32, (size, ids.shape[1]), 0) + (place * vocab + base)
        onehot = (row == ids[...]).astype(jnp.bfloat16)
        hits = hits + lax.dot_general(
            onehot,
            table[pl.ds(base, size), :],
            (((0,), (0,)), ((), ())),
            preferred_element_type=jnp.float32,
        )
    answers = found.shape[1]
    for q in range(PLANES):
        found[q] = hits[q * answers : (q + 1) * answers].astype(jnp.bfloat16)

    got(gu, gu_r, 2, 1 - x)
    stream(gu, gu_s, gu_r, 2, 1 - x)

    d_left = enc.at[slot_d, :, pl.ds(0, feat_half)]
    d_right = enc.at[slot_d, :, pl.ds(feat_half, feat_half)]
    arrived(d_left, enc_r.at[8])
    arrived(d_right, enc_r.at[9])
    send(enc.at[slot_d], enc.at[slot_d], enc_s.at[7], enc_r.at[slot_d], twin)
    for other in (slot, slot_x, slot_y, slot_d):
        flipped = other + 1 - 2 * n
        arrived(enc.at[flipped], enc_r.at[flipped])

    def gate_up(k):
        at_z = order[k]
        width = 2 * gu.shape[3]
        cols = pl.ds(pl.multiple_of(at_z * width, width), width)
        weights = [
            jnp.concatenate(
                [gu[at_z, 0, pl.ds(j * unit, unit), :], gu[at_z, 1, pl.ds(j * unit, unit), :]], axis=1
            )
            for j in range(2)
        ]

        def body(i, carry):
            rows = enc[i, :, cols]
            for j in range(2):
                value = dot_t(rows, weights[j])
                if k:
                    value = value + acts[j, i]
                acts[j, i] = value
            return carry

        lax.fori_loop(0, CHIPS * CORES, body, 0)

    gate_up(0)
    gate_up(1)
    gate_up(2)
    got(gu, gu_r, 3, x)
    stream(gu, gu_s, gu_r, 3, x)
    got(dn, dn_r, 0, 1 - x)
    stream(dn, dn_s, dn_r, 0, 1 - x)
    got(gu, gu_r, 3, 1 - x)
    stream(gu, gu_s, gu_r, 3, 1 - x)
    gate_up(3)

    def activate(i, carry):
        inner[i] = (jax.nn.gelu(acts[0, i], approximate=True) * acts[1, i]).astype(jnp.bfloat16)
        return carry

    lax.fori_loop(0, CHIPS * CORES, activate, 0)

    targets = [(2, across, 1 - x, y), (1, aside, x, 1 - y), (3, corner, 1 - x, 1 - y)]

    def block_cols(at_z):
        width = 2 * dn.shape[3]
        return pl.ds(pl.multiple_of(at_z * width, width), width)

    def down_first(k):
        at_z = order[k]
        weights = jnp.concatenate([dn[at_z, 0], dn[at_z, 1]], axis=1)

        def body(c, carry):
            part_out[at_z, c] = add_rows(inner[c * CORES + 1 - n], weights)
            return carry

        lax.fori_loop(0, CHIPS, body, 0)
        send(part_out.at[at_z], part_in.at[at_z], part_s.at[at_z], part_r.at[at_z], twin)

        def body_own(c, carry):
            part_own[c] = add_rows(inner[c * CORES + n], weights)
            return carry

        lax.fori_loop(0, CHIPS, body_own, 0)

    def down_second(k):
        at_z = order[k]
        arrived(part_in.at[at_z], part_r.at[at_z])
        for j, (_, peer, xt, yt) in enumerate(targets):
            c = 2 * xt + yt
            total = part_own[c] + part_in[at_z, c]
            top = jnp.max(jnp.max(jnp.abs(total), axis=0, keepdims=True), axis=1, keepdims=True)
            power = jnp.ceil(jnp.log(jnp.maximum(top, 1e-30) / QUANT) * (1.0 / math.log(2.0)) + 0.01)
            coded = jnp.round(total * jnp.exp2(-power))
            row = lax.broadcasted_iota(jnp.int32, coded.shape, 0)
            coded = jnp.where(row < slot_rows - 8, coded, power)
            share_out[at_z, j] = coded.astype(jnp.int32).astype(jnp.int16)
            send(
                share_out.at[at_z, j], share_in.at[at_z, j], share_s.at[at_z, j], share_r.at[at_z, j], peer
            )
        c = 2 * x + y
        cols = block_cols(at_z)
        resid[:, cols] = hid[:, cols].astype(jnp.float32) + part_own[c] + part_in[at_z, c]

    def att_to_side(k, side):
        at_z = order[k]
        send(
            at.at[0, at_z, side], at.at[1, at_z, side], at_ys.at[at_z, side], at_yr.at[at_z, side], aside
        )

    def att_take(k, side):
        got(at.at[0], at_r, k, side)
        stream(at.at[0], at_s, at_r, k, side)
        att_to_side(k, side)

    down_first(0)
    got(dn, dn_r, 1, x)
    stream(dn, dn_s, dn_r, 1, x)
    down_second(0)
    got(dn, dn_r, 1, 1 - x)
    stream(dn, dn_s, dn_r, 1, 1 - x)
    down_first(1)
    got(dn, dn_r, 2, x)
    stream(dn, dn_s, dn_r, 2, x)
    down_second(1)
    got(dn, dn_r, 2, 1 - x)
    stream(dn, dn_s, dn_r, 2, 1 - x)
    stream(at.at[0], at_s, at_r, 0, x)
    att_take(0, 1 - x)
    att_to_side(0, x)
    down_first(2)
    for d in range(1, PLANES):
        q = (z + d) % PLANES
        send(found.at[q], found_in.at[z], emb_s.at[d], emb_r.at[z], on(x, y, q, n))
    down_second(2)
    got(dn, dn_r, 3, x)
    stream(dn, dn_s, dn_r, 3, x)
    got(dn, dn_r, 3, 1 - x)
    stream(dn, dn_s, dn_r, 3, 1 - x)
    down_first(3)
    att_take(1, x)
    down_second(3)
    att_take(1, 1 - x)

    summed = found[z].astype(jnp.float32)
    for d in range(1, PLANES):
        q = (z + d) % PLANES
        arrived(found_in.at[q], emb_r.at[q])
        summed = summed + found_in[q].astype(jnp.float32)
    pair_out[...] = summed.astype(jnp.bfloat16)
    send(pair_out, pair_in, one_s.at[1], one_r.at[1], across)
    att_take(2, x)
    att_take(2, 1 - x)
    arrived(pair_in, one_r.at[1])
    half = (pair_out[...].astype(jnp.float32) + pair_in[...].astype(jnp.float32)).astype(jnp.bfloat16)
    half_in[n] = half
    send(half_in.at[n], half_in.at[n], one_s.at[2], one_r.at[2], twin)

    for k in range(PLANES):
        at_z = order[k]
        cols = block_cols(at_z)
        for j in range(len(targets)):
            arrived(share_in.at[at_z, j], share_r.at[at_z, j])
        total = resid[:, cols]
        for j in range(len(targets)):
            coded = share_in[at_z, j].astype(jnp.int32).astype(jnp.float32)
            total = total + coded * jnp.exp2(coded[slot_rows - 8 : slot_rows - 7, 0:1])
        resid[:, cols] = total
    spot = 2 * x + n
    mem[spot] = rms_scale(resid[...], gain_out[...]).astype(jnp.bfloat16)
    send(mem.at[spot], mem.at[spot], mem_s.at[0], mem_r.at[spot], across)
    send(mem.at[spot], mem.at[spot], mem_s.at[1], mem_r.at[spot], twin)

    att_take(3, x)
    att_take(3, 1 - x)
    arrived(half_in.at[1 - n], one_r.at[2])
    embedded = jnp.concatenate([half_in[0], half_in[1]], axis=1).astype(jnp.float32)
    dec_in = rms_scale(embedded, gain_dec[...]).astype(jnp.bfloat16)
    for h in range(2):
        for k in range(PLANES):
            for side in range(2):
                if h:
                    arrived(at.at[1, k, side], at_yr.at[k, side])
                cols = pl.ds(pl.multiple_of((y + h - 2 * y * h) * head_cols, head_cols), head_cols)
                rows = pl.ds((2 * k + side) * depth, depth)
                for j, array in enumerate((weight_k, weight_v, weight_q)):
                    array[rows, cols] = at[h, k, side, pl.ds(j * depth, depth), :]
                weight_o[cols, rows] = at[h, k, side, pl.ds(3 * depth, head_cols), :]
    query = add_rows(dec_in, weight_q[...]).astype(jnp.bfloat16)

    def project(j):
        keys[j] = add_rows(mem[j], weight_k[...]).astype(jnp.bfloat16)
        values[j] = add_rows(mem[j], weight_v[...]).astype(jnp.bfloat16)

    project(spot)
    spot_twin = 2 * x + 1 - n
    arrived(mem.at[spot_twin], mem_r.at[spot_twin])
    memory_out[n] = mem[spot]
    memory_out[1 - n] = mem[spot_twin]
    project(spot_twin)
    spot_x = 2 * (1 - x) + n
    arrived(mem.at[spot_x], mem_r.at[spot_x])
    send(mem.at[spot_x], mem.at[spot_x], mem_s.at[2], mem_r.at[spot_x], twin)
    project(spot_x)
    spot_far = 2 * (1 - x) + 1 - n
    arrived(mem.at[spot_far], mem_r.at[spot_far])
    project(spot_far)
    arrived(lens_all.at[1 - x], one_r.at[0])

    columns = 2 * head_cols
    heads = columns // HEAD_DIM
    lane_head = lax.broadcasted_iota(jnp.int32, (answers, columns), 1) // HEAD_DIM
    stacked = jnp.concatenate(
        [jnp.where(lane_head == h, query.astype(jnp.float32), 0.0) for h in range(heads)], axis=0
    ).astype(jnp.bfloat16)
    tokens = 2 * CORES * slot_rows
    key_rows = keys[...].reshape(tokens, columns)
    value_rows = values[...].reshape(tokens, columns)
    scores = dot_t(stacked, key_rows) * (1.0 / math.sqrt(HEAD_DIM))
    token = lax.broadcasted_iota(jnp.int32, (1, tokens), 1)
    live = token < 0
    for j in range(2 * CORES):
        length = lens_all[j // CORES, j % CORES : j % CORES + 1, 0:1]
        live = live | ((token >= j * slot_rows) & (token < j * slot_rows + length))
    scores = jnp.where(live, scores, FLOOR)
    peak = jnp.max(scores, axis=1, keepdims=True)
    weights = jnp.exp(scores - peak)
    total = jnp.sum(weights, axis=1, keepdims=True)
    coarse = weights.astype(jnp.bfloat16)
    fine = (weights - coarse.astype(jnp.float32)).astype(jnp.bfloat16)
    mixed = (add_rows(coarse, value_rows) + add_rows(fine, value_rows)) / total
    attended = jnp.where(lane_head == 0, mixed[:answers], 0.0)
    for h in range(1, heads):
        attended = jnp.where(lane_head == h, mixed[h * answers : (h + 1) * answers], attended)
    partial = add_rows(attended.astype(jnp.bfloat16), weight_o[...])
    half_cols = partial.shape[1] // 2
    low, high = partial[:, :half_cols], partial[:, half_cols:]
    tail_out[...] = jnp.where(n == 0, high, low)
    send(tail_out, tail_in, one_s.at[3], one_r.at[3], twin)
    own = jnp.where(n == 0, low, high)
    arrived(tail_in, one_r.at[3])
    own = own + tail_in[...]
    tail_sum[...] = own
    send(tail_sum, tail_pair, one_s.at[4], one_r.at[4], across)
    base = half_in[n].astype(jnp.float32)
    arrived(tail_pair, one_r.at[4])
    dec_all[z] = (base + (own + tail_pair[...])).astype(jnp.bfloat16)
    for d in range(1, PLANES):
        q = (z + d) % PLANES
        send(dec_all.at[z], dec_all.at[z], dec_s.at[d], dec_r.at[z], on(x, y, q, n))
    for d in range(1, PLANES):
        q = (z + d) % PLANES
        arrived(dec_all.at[q], dec_r.at[q])
    decoded_out[...] = dec_all[...].reshape(decoded_out.shape)
    for copy, cond in pending:
        if cond is None:
            copy().wait_send()
        else:
            pl.when(cond)(lambda copy=copy: copy().wait_send())


def per_device(
    hidden_in,
    ffn_gain,
    wi_gate,
    wi_up,
    wo_down,
    final_gain,
    key_w,
    value_w,
    query_w,
    out_w,
    dec_gain,
    embed,
    lengths,
    answer_ids,
):
    sizes = tuple(lax.axis_size(a) for a in ("groups", "wide", "narrow"))
    if sizes != (2, 2 * PLANES, CORES) or QUEST != PLANES:
        return per_device_any(
            hidden_in,
            ffn_gain,
            wi_gate,
            wi_up,
            wo_down,
            final_gain,
            key_w,
            value_w,
            query_w,
            out_w,
            dec_gain,
            embed,
            lengths,
            answer_ids,
        )
    core = lax.axis_index("narrow")
    rows, features = hidden_in.shape
    seg = rows // lengths.shape[0]
    slot_rows = -(-(seg + 8) // 16) * 16
    slot_rows = slot_rows if slot_rows - 8 >= seg else slot_rows + 16
    hid = jnp.pad(part(hidden_in, core, CORES, 0), ((0, slot_rows - seg), (0, 0)))
    depth = wi_gate.shape[0]
    unit = wi_gate.shape[1] // CHIPS
    head_cols = key_w.shape[1] // CHIPS
    answers = answer_ids.shape[1]
    width = features // PLANES
    half = features // 2
    lens = jnp.pad(jnp.broadcast_to(lengths[:, None], (lengths.shape[0], 128)), ((0, 8 - lengths.shape[0]), (0, 0)))
    ids = answer_ids.reshape(1, -1)
    bf, f32 = jnp.bfloat16, jnp.float32
    slots = CHIPS * CORES
    others = CHIPS - 1
    dma = pltpu.SemaphoreType.DMA
    vmem = pl.BlockSpec(memory_space=pltpu.VMEM)
    memory, decoded = pl.pallas_call(
        reader,
        out_shape=(
            jax.ShapeDtypeStruct((CORES, slot_rows, features), bf),
            jax.ShapeDtypeStruct((QUEST * answers, half), bf),
        ),
        in_specs=[vmem] * 11 + [pl.BlockSpec(memory_space=pl.ANY)] + [vmem] * 2,
        out_specs=(vmem, vmem),
        scratch_shapes=[
            pltpu.VMEM((2, wi_gate.shape[1], depth), bf),
            pltpu.VMEM((PLANES, 2, 2 * unit, depth), bf),
            pltpu.VMEM((2 * unit, depth), bf),
            pltpu.VMEM((PLANES, 2, unit, depth), bf),
            pltpu.VMEM((2, PLANES, 2, 3 * depth + head_cols, head_cols), bf),
            pltpu.VMEM((3 * depth + head_cols, head_cols), bf),
            pltpu.VMEM((slots, slot_rows, features), bf),
            pltpu.VMEM((2, slots, slot_rows, unit), f32),
            pltpu.VMEM((slots, slot_rows, unit), bf),
            pltpu.VMEM((embed.shape[0], half), bf),
            pltpu.VMEM((CHIPS, slot_rows, width), f32),
            pltpu.VMEM((PLANES, CHIPS, slot_rows, width), f32),
            pltpu.VMEM((PLANES, CHIPS, slot_rows, width), f32),
            pltpu.VMEM((PLANES, others, slot_rows, width), jnp.int16),
            pltpu.VMEM((PLANES, others, slot_rows, width), jnp.int16),
            pltpu.VMEM((slot_rows, features), f32),
            pltpu.VMEM((2 * CORES, slot_rows, features), bf),
            pltpu.VMEM((QUEST, answers, half), bf),
            pltpu.VMEM((QUEST, answers, half), bf),
            pltpu.VMEM((answers, half), bf),
            pltpu.VMEM((answers, half), bf),
            pltpu.VMEM((CORES, answers, half), bf),
            pltpu.VMEM((2, 8, 128), jnp.int32),
            pltpu.VMEM((features, 2 * head_cols), bf),
            pltpu.VMEM((features, 2 * head_cols), bf),
            pltpu.VMEM((features, 2 * head_cols), bf),
            pltpu.VMEM((2 * head_cols, features), bf),
            pltpu.VMEM((2 * CORES, slot_rows, 2 * head_cols), bf),
            pltpu.VMEM((2 * CORES, slot_rows, 2 * head_cols), bf),
            pltpu.VMEM((answers, half), f32),
            pltpu.VMEM((answers, half), f32),
            pltpu.VMEM((answers, half), f32),
            pltpu.VMEM((answers, half), f32),
            pltpu.VMEM((QUEST, answers, half), bf),
            dma((5, 2)),
            dma((PLANES, 2)),
            dma((5, 2)),
            dma((PLANES, 2)),
            dma((5, 2)),
            dma((PLANES, 2)),
            dma((PLANES, 2)),
            dma((PLANES, 2)),
            dma((4,)),
            dma((8,)),
            dma((slots + 2,)),
            dma((PLANES,)),
            dma((PLANES,)),
            dma((PLANES, others)),
            dma((PLANES, others)),
            dma((PLANES,)),
            dma((PLANES,)),
            dma((5,)),
            dma((5,)),
            dma((3,)),
            dma((2 * CORES,)),
            dma((PLANES,)),
            dma((PLANES,)),
            dma,
        ],
        compiler_params=pltpu.CompilerParams(
            collective_id=0, has_side_effects=True, vmem_limit_bytes=62 * 2**20
        ),
    )(
        hid,
        ffn_gain[None],
        wi_gate,
        wi_up,
        wo_down,
        final_gain[None],
        key_w,
        value_w,
        query_w,
        out_w,
        dec_gain[None],
        embed,
        lens,
        ids,
    )
    return memory[:, :seg].reshape(rows, features), decoded


def solution(mesh):
    placed = (
        P(("groups", "wide"), None),
        P(),
        P("wide", "narrow"),
        P("wide", "narrow"),
        P("narrow", "wide"),
        P(),
        P("wide", "narrow"),
        P("wide", "narrow"),
        P("wide", "narrow"),
        P("narrow", "wide"),
        P(),
        P("wide", None),
        P(("groups", "wide")),
        P("groups", None),
    )
    return jax.shard_map(
        per_device,
        mesh=mesh,
        in_specs=placed,
        out_specs=(P(("groups", "wide"), None), P("groups", "narrow")),
        check_vma=False,
    )
```

```python
import functools
import math

import jax
import jax.numpy as jnp
from jax import lax
from jax.experimental import pallas as pl
from jax.experimental.pallas import tpu as pltpu
from jax.sharding import PartitionSpec as P

HEAD_DIM = 64
QUEST = 4


EPS = 1e-06
FLOOR = -1e30


def swap(values, axis, distance=1):
    pairs = [(i, i ^ distance) for i in range(lax.axis_size(axis))]
    return jax.tree.map(lambda a: lax.ppermute(a, axis, pairs), values)


def ordered(bit, own, other, dim):
    first = jnp.where(bit == 0, own, other)
    second = jnp.where(bit == 0, other, own)
    return jnp.concatenate([first, second], axis=dim)


def part(values, index, count, dim):
    size = values.shape[dim] // count
    return lax.dynamic_slice_in_dim(values, index * size, size, dim)


def line_gather(block, place, count):
    size = lax.axis_size("wide")
    stride = size // count
    if count > 8:
        groups = [[i * stride + j for i in range(count)] for j in range(stride)]
        return lax.all_gather(block, "wide", axis_index_groups=groups)
    up = [(i, i + stride) for i in range(size - stride)]
    down = [(i + stride, i) for i in range(size - stride)]
    below, above = [], []
    from_below = from_above = block
    for _ in range(count - 1):
        from_below = lax.ppermute(from_below, "wide", up)
        from_above = lax.ppermute(from_above, "wide", down)
        below.insert(0, from_below)
        above.append(from_above)
    return lax.dynamic_slice_in_dim(
        jnp.stack(below + [block] + above), count - 1 - place, count, 0
    )


def rms_scale(values, gain):
    mean_square = jnp.mean(values * values, axis=-1, keepdims=True)
    return values * lax.rsqrt(mean_square + EPS) * gain.astype(jnp.float32)


def add_rows(left, piece):
    return jnp.dot(left, piece, preferred_element_type=jnp.float32)


def join_partial(first, second):
    top = jnp.maximum(first[0], second[0])
    factor_first = jnp.exp(first[0] - top)
    factor_second = jnp.exp(second[0] - top)
    return (
        top,
        first[1] * factor_first + second[1] * factor_second,
        first[2] * factor_first + second[2] * factor_second,
    )


def per_device_any(
    hidden_in,
    ffn_gain,
    wi_gate,
    wi_up,
    wo_down,
    final_gain,
    key_w,
    value_w,
    query_w,
    out_w,
    dec_gain,
    embed,
    lengths,
    answer_ids,
):
    rows, features = hidden_in.shape
    wide = lax.axis_size("wide")
    group, place, core = (lax.axis_index(a) for a in ("groups", "wide", "narrow"))
    side, pair = place % 2, place // 2
    pairs = wide // 2
    quarters = 2 * lax.axis_size("groups")
    lanes = 128

    def for_side(target, pieces):
        quarter = target * (quarters // 2) + group
        return jnp.concatenate(
            [part(a, quarter, quarters, dim).reshape(-1, lanes) for a, dim in pieces]
        )

    def paired(pieces):
        own = for_side(side, pieces)
        other = swap(for_side(1 - side, pieces), "wide")
        return ordered(side, own[None], other[None], 0)

    def gathered(both):
        return line_gather(both, pair, pairs).reshape(wide, *both.shape[1:])

    hidden_units = wi_gate.shape[1] // quarters
    depth = wi_gate.shape[0]
    ffn = gathered(paired(((wi_gate.T, 0), (wi_up.T, 0), (wo_down, 0))))
    ffn = ffn.reshape(wide, 3, hidden_units, depth).transpose(1, 2, 0, 3)
    gate_t, up_t, down = ffn.reshape(3, hidden_units, features)

    def over_plane(own):
        couple = jnp.concatenate([own, swap(own, "wide")])
        return jnp.concatenate([couple, swap(couple, "groups")])

    def both_halves(own):
        return ordered(core, own, swap(own, "narrow"), 1)

    answers = answer_ids.shape[1]
    per_question = wide // QUEST
    qrows = answer_ids.shape[0] * answers
    vocab_rows = embed.shape[0]
    local_ids = answer_ids.reshape(qrows) - place * vocab_rows
    onehot = (local_ids[:, None] == jnp.arange(vocab_rows, dtype=jnp.int32)[None, :]).astype(
        jnp.bfloat16
    )
    found = jnp.dot(onehot, embed, preferred_element_type=jnp.float32).astype(jnp.bfloat16)
    found = part(found, core, 2, 1)
    distance = wide // 2
    while distance:
        if distance >= per_question:
            bit = place // distance % 2
            found = part(found, bit, 2, 0) + swap(part(found, 1 - bit, 2, 0), "wide", distance)
        else:
            found = found + swap(found, "wide", distance)
        distance //= 2
    embedded_half = found.astype(jnp.float32)
    dec_own = rms_scale(both_halves(found).astype(jnp.float32), dec_gain).astype(jnp.bfloat16)
    dec_in = jnp.concatenate([dec_own, swap(dec_own, "groups")])

    columns = key_w.shape[1] // quarters
    att_pair = paired(((key_w, 1), (value_w, 1), (query_w, 1), (out_w, 0)))
    lengths_all = over_plane(lengths)

    resid_in = hidden_in.astype(jnp.float32)
    enc_own = rms_scale(resid_in, ffn_gain).astype(jnp.bfloat16)
    enc_in = both_halves(over_plane(part(enc_own, core, 2, 1)))
    enc_in, dec_in, lengths_all, att_pair, embedded_half = lax.optimization_barrier(
        (enc_in, dec_in, lengths_all, att_pair, embedded_half)
    )
    contract_last = (((1,), (1,)), ((), ()))
    gate = lax.dot_general(enc_in, gate_t, contract_last, preferred_element_type=jnp.float32)
    up = lax.dot_general(enc_in, up_t, contract_last, preferred_element_type=jnp.float32)
    inner = (jax.nn.gelu(gate, approximate=True) * up).astype(jnp.bfloat16)
    sent_half = add_rows(inner, part(down, 1 - core, 2, 1))
    received_half = swap(sent_half, "narrow")
    sums = add_rows(inner, part(down, core, 2, 1)) + received_half

    def keep_half(values):
        return part(values, core, 2, 1) + swap(part(values, 1 - core, 2, 1), "narrow")

    blocks = sums.reshape(4, rows, -1)
    middle = blocks.shape[2] // 2
    early, late = blocks[:, :, :middle], blocks[:, :, middle:]
    early = early[:2] + swap(early[2:], "groups")
    late = late[::2] + swap(late[1::2], "wide")
    early = early[0] + swap(early[1], "wide")
    late = late[0] + swap(late[1], "groups")
    share = jnp.concatenate([early, late], axis=1)
    resid_half = part(resid_in, core, 2, 1) + share
    own_squares = jnp.sum(resid_half * resid_half, axis=1)
    squares = (own_squares + swap(own_squares, "narrow"))[:, None]
    gain_half = part(final_gain, core, 2, 0).astype(jnp.float32)
    memory_half = (resid_half * lax.rsqrt(squares / features + EPS) * gain_half).astype(
        jnp.bfloat16
    )
    memory_early, memory_late = memory_half[:, :middle], memory_half[:, middle:]
    twin = jnp.stack([memory_late, swap(memory_late, "groups")])
    late_all = jnp.stack([twin, swap(twin, "wide")], axis=1).reshape(4 * rows, middle)
    early_all = over_plane(memory_early)
    early_other, late_other = swap(early_all, "narrow"), swap(late_all, "narrow")
    other_half = jnp.concatenate([early_other[:rows], late_other[:rows]], axis=1)
    memory = ordered(core, memory_half, other_half, 1)

    att = gathered(att_pair)
    att = att.reshape(wide, 4, -1)
    key_q, value_q, query_q = (att[:, i].reshape(features, columns) for i in range(3))
    out_q = att[:, 3].reshape(wide, columns, depth).transpose(1, 0, 2).reshape(columns, features)

    def project(weight):
        own, other = part(weight, core, 2, 0), part(weight, 1 - core, 2, 0)
        return (
            add_rows(early_all, own[:middle])
            + add_rows(late_all, own[middle:])
            + add_rows(early_other, other[:middle])
            + add_rows(late_other, other[middle:])
        ).astype(jnp.bfloat16)

    heads = columns // HEAD_DIM
    keys = project(key_q).reshape(2, 2 * rows, columns)
    values = project(value_q).reshape(2, 2 * rows, columns).astype(jnp.float32)
    query = add_rows(dec_in, query_q).astype(jnp.bfloat16)
    in_head = (
        jnp.arange(columns, dtype=jnp.int32)[None, :] // HEAD_DIM
        == jnp.arange(heads, dtype=jnp.int32)[:, None]
    )[None, :, None, :]
    query_heads = jnp.where(in_head, query.reshape(2, 1, answers, columns), 0)
    scores = jnp.einsum(
        "qhac,qkc->qhak", query_heads, keys, preferred_element_type=jnp.float32
    ) * (1.0 / math.sqrt(HEAD_DIM))
    passage_len = rows // lengths.shape[0]
    live = jnp.arange(passage_len, dtype=jnp.int32)[None, :] < lengths_all[:, None]
    scores = jnp.where(live.reshape(2, 1, 1, 2 * rows), scores, FLOOR)
    top = jnp.max(scores, axis=3, keepdims=True)
    weights = jnp.exp(scores - top)
    total = jnp.sum(weights, axis=3, keepdims=True)
    acc = jnp.einsum("qhak,qkc->qhac", weights, values, precision=lax.Precision.HIGHEST)
    state = (top, total, acc)
    distance = 2
    while distance < per_question:
        state = join_partial(state, swap(state, "wide", distance))
        distance *= 2
    attended = jnp.sum(jnp.where(in_head, state[2] / state[1], 0.0), axis=1)
    attended = attended.astype(jnp.bfloat16).reshape(2 * answers, columns)
    partial_out = keep_half(jnp.dot(attended, out_q, preferred_element_type=jnp.float32))
    share_out = partial_out[:answers] + swap(partial_out[answers:], "groups")
    share_out = share_out + swap(share_out, "wide")
    decoded = (embedded_half + share_out).astype(jnp.bfloat16)
    distance = per_question
    while distance < wide:
        decoded = ordered(place // distance % 2, decoded, swap(decoded, "wide", distance), 0)
        distance *= 2
    return (memory, decoded)


MESH = pl.DeviceIdType.MESH
PLANES = 4
CHIPS = 4
CORES = 2
QUANT = 32767.0


def dot_t(left, right):
    return lax.dot_general(
        left, right, (((1,), (1,)), ((), ())), preferred_element_type=jnp.float32
    )


def reader(
    hidden,
    gain_in,
    gate_w,
    up_w,
    down_w,
    gain_out,
    key_w,
    value_w,
    query_w,
    out_w,
    gain_dec,
    embed,
    lengths,
    ids,
    memory_out,
    decoded_out,
    hid,
    turned,
    gu,
    gu_side,
    dn,
    at,
    at_side,
    enc,
    acts,
    inner,
    table,
    part_own,
    part_out,
    part_in,
    share_out,
    share_in,
    kept,
    last_out,
    last_in,
    dec_rows,
    query_rows,
    query_out,
    resid,
    mem,
    found,
    found_in,
    pair_out,
    pair_in,
    half_in,
    lens_all,
    weight_k,
    weight_v,
    weight_q,
    weight_o,
    keys,
    values,
    tail_out,
    tail_in,
    tail_sum,
    tail_pair,
    dec_all,
    gu_s,
    gu_r,
    dn_s,
    dn_r,
    at_s,
    at_r,
    at_ys,
    at_yr,
    x_s,
    enc_s,
    enc_r,
    part_s,
    part_r,
    share_s,
    share_r,
    last_s,
    last_r,
    emb_s,
    emb_r,
    one_s,
    one_r,
    mem_s,
    mem_r,
    dec_s,
    dec_r,
    table_sem,
):
    y, place, n = (lax.axis_index(a) for a in ("groups", "wide", "narrow"))
    z, x = place // 2, place % 2
    upper = z // 2
    w = z + upper * (PLANES - 1 - 2 * z)

    def plane(mirrored):
        return mirrored + upper * (PLANES - 1 - 2 * mirrored)

    order = [z, plane(1 - w), plane(2), plane(3)]
    slot_rows = hid.shape[0]
    unit = gu.shape[2] // 2
    head_cols = at.shape[4]

    def on(x_at, y_at, z_at, n_at):
        return {"groups": y_at, "wide": z_at * 2 + x_at, "narrow": n_at}

    across = on(1 - x, y, z, n)
    aside = on(x, 1 - y, z, n)
    corner = on(1 - x, 1 - y, z, n)
    twin = on(x, y, z, 1 - n)
    next_a = on(x, y, order[1], n)
    next_b = on(x, y, plane(2), n)
    inside = w == 1
    pending = []

    def send(source, target, send_sem, recv_sem, device, cond=None):
        def copy():
            return pltpu.make_async_remote_copy(
                source, target, send_sem, recv_sem, device_id=device, device_id_type=MESH
            )

        if cond is None:
            copy().start()
        else:
            pl.when(cond)(lambda: copy().start())
        pending.append((copy, cond))

    def arrived(target, recv_sem):
        pltpu.make_async_remote_copy(
            target, target, recv_sem, recv_sem, device_id=twin, device_id_type=MESH
        ).wait_recv()

    barrier = pltpu.get_barrier_semaphore()
    peers = [across, aside, corner, twin]
    peers += [on(x, y, (z + d) % PLANES, n) for d in range(1, PLANES)]
    for peer in peers:
        pl.semaphore_signal(barrier, inc=1, device_id=peer, device_id_type=MESH)

    table_copy = pltpu.make_async_copy(
        embed.at[:, pl.ds(pl.multiple_of(n * table.shape[1], 128), table.shape[1])],
        table,
        table_sem,
    )
    table_copy.start()

    seg = hidden.shape[0] // CORES
    late = hidden.shape[0] - slot_rows
    low = hidden[pl.ds(0, slot_rows), :].astype(jnp.float32)
    high = hidden[pl.ds(late, slot_rows), :].astype(jnp.float32)
    skip = seg - late
    hid[...] = jnp.where(n == 0, low, jnp.concatenate([high[skip:], high[:skip]], axis=0))

    lanes = 128
    for k in range(gate_w.shape[1] // lanes):
        cols = pl.ds(k * lanes, lanes)
        turned[0, cols, :] = gate_w[:, cols].T
        turned[1, cols, :] = up_w[:, cols].T
    mine = pl.multiple_of((2 * x + y) * unit, 16)
    theirs = pl.multiple_of((2 * (1 - x) + y) * unit, 16)
    for j in range(2):
        gu_side[pl.ds(j * unit, unit), :] = turned[j, pl.ds(theirs, unit), :]
        gu[z, x, pl.ds(j * unit, unit), :] = turned[j, pl.ds(mine, unit), :]
    dn[z, x] = down_w[pl.ds(mine, unit), :]
    col_mine = pl.multiple_of((2 * x + y) * head_cols, head_cols)
    col_theirs = pl.multiple_of((2 * (1 - x) + y) * head_cols, head_cols)
    depth = key_w.shape[0]
    kv_rows = pl.ds(0, 2 * depth)
    o_rows = pl.ds(2 * depth, head_cols)
    q_rows = pl.ds(2 * depth + head_cols, depth)
    for rows, array in (
        (pl.ds(0, depth), key_w),
        (pl.ds(depth, depth), value_w),
        (q_rows, query_w),
    ):
        at[0, z, x, rows, :] = array[:, pl.ds(col_mine, head_cols)]
        at_side[rows, :] = array[:, pl.ds(col_theirs, head_cols)]
    at[0, z, x, o_rows, :] = out_w[pl.ds(col_mine, head_cols), :]
    at_side[o_rows, :] = out_w[pl.ds(col_theirs, head_cols), :]
    tile_row = lax.broadcasted_iota(jnp.int32, lens_all.shape[1:], 0)
    lens_all[x] = jnp.where(tile_row == 0, lengths[0], lengths[1])

    pl.semaphore_wait(barrier, len(peers))

    def stream(buf, s_sem, r_sem, k, side):
        at_z = order[k]
        if k == 0:
            send(buf.at[at_z, side], buf.at[at_z, side], s_sem.at[0, side], r_sem.at[at_z, side], next_a)
            send(buf.at[at_z, side], buf.at[at_z, side], s_sem.at[4, side], r_sem.at[at_z, side], next_b, inside)
        else:
            target = next_b if k == 1 else next_a
            send(buf.at[at_z, side], buf.at[at_z, side], s_sem.at[k, side], r_sem.at[at_z, side], target, inside)

    def att_side(k, side, parts=(0,)):
        at_z = order[k]
        for j, rows in enumerate((kv_rows, o_rows)):
            if j in parts:
                send(
                    at.at[0, at_z, side, rows],
                    at.at[1, at_z, side, rows],
                    at_ys.at[at_z, side, j],
                    at_yr.at[at_z, side, j],
                    aside,
                )

    def got(buf, r_sem, k, side):
        arrived(buf.at[order[k], side], r_sem.at[order[k], side])

    send(gu_side, gu.at[z, x], x_s.at[0], gu_r.at[z, x], across)
    stream(gu, gu_s, gu_r, 0, x)
    stream(dn, dn_s, dn_r, 0, x)

    slot = n * CHIPS + 2 * x + y
    enc[slot] = rms_scale(hid[...], gain_in[...][None]).astype(jnp.bfloat16)
    for j, peer in enumerate((across, aside, twin)):
        send(enc.at[slot], enc.at[slot], enc_s.at[j], enc_r.at[slot], peer)
    send(down_w.at[pl.ds(theirs, unit), :], dn.at[z, x], x_s.at[1], dn_r.at[z, x], across)
    send(lens_all.at[x], lens_all.at[x], x_s.at[3], one_r.at[0], across)
    send(at_side, at.at[0, z, x], x_s.at[2], at_r.at[z, x], across)
    att_side(0, x, (0, 1))

    def pass_on(buf, s_sem, r_sem, k, side):
        @pl.when(inside)
        def _():
            got(buf, r_sem, k, side)

        stream(buf, s_sem, r_sem, k, side)

    def end_got(buf, r_sem, k):
        @pl.when(w == 0)
        def _():
            for side in (x, 1 - x):
                got(buf, r_sem, k, side)

    got(gu, gu_r, 0, 1 - x)
    stream(gu, gu_s, gu_r, 0, 1 - x)
    for side in (x, 1 - x):
        for k in (2, 1):
            pass_on(gu, gu_s, gu_r, k, side)

    feat_half = enc.shape[2] // 2
    slot_x = n * CHIPS + 2 * (1 - x) + y
    slot_y = n * CHIPS + 2 * x + 1 - y
    slot_d = n * CHIPS + 2 * (1 - x) + 1 - y
    arrived(enc.at[slot_x], enc_r.at[slot_x])
    left = enc.at[slot_x, :, pl.ds(0, feat_half)]
    send(left, left, enc_s.at[3], enc_r.at[8], aside)
    arrived(enc.at[slot_y], enc_r.at[slot_y])
    right = enc.at[slot_y, :, pl.ds(feat_half, feat_half)]
    send(right, right, enc_s.at[4], enc_r.at[9], across)
    send(enc.at[slot_x], enc.at[slot_x], enc_s.at[5], enc_r.at[slot_x], twin)
    send(enc.at[slot_y], enc.at[slot_y], enc_s.at[6], enc_r.at[slot_y], twin)

    pass_on(gu, gu_s, gu_r, 3, x)
    table_copy.wait()
    vocab = table.shape[0]
    total_ids = ids.shape[0] * ids.shape[1]
    all_ids = jnp.concatenate([ids[q : q + 1, :] for q in range(ids.shape[0])], axis=1)
    chunk = 1024
    hits = jnp.zeros((total_ids, table.shape[1]), jnp.float32)
    for base in range(0, vocab, chunk):
        size = min(chunk, vocab - base)
        row = lax.broadcasted_iota(jnp.int32, (size, total_ids), 0) + (place * vocab + base)
        onehot = (row == all_ids).astype(jnp.bfloat16)
        hits = hits + lax.dot_general(
            onehot,
            table[pl.ds(base, size), :],
            (((0,), (0,)), ((), ())),
            preferred_element_type=jnp.float32,
        )
    answers = found.shape[1]
    for q in range(PLANES):
        found[q] = hits[q * answers : (q + 1) * answers].astype(jnp.bfloat16)

    d_left = enc.at[slot_d, :, pl.ds(0, feat_half)]
    d_right = enc.at[slot_d, :, pl.ds(feat_half, feat_half)]
    arrived(d_left, enc_r.at[8])
    arrived(d_right, enc_r.at[9])
    send(enc.at[slot_d], enc.at[slot_d], enc_s.at[7], enc_r.at[slot_d], twin)
    for other in (slot, slot_x, slot_y, slot_d):
        flipped = other + (1 - 2 * n) * CHIPS
        arrived(enc.at[flipped], enc_r.at[flipped])

    def gate_up(k):
        at_z = order[k]
        width = 2 * gu.shape[3]
        cols = pl.ds(pl.multiple_of(at_z * width, width), width)
        weights = [
            jnp.concatenate(
                [gu[at_z, 0, pl.ds(j * unit, unit), :], gu[at_z, 1, pl.ds(j * unit, unit), :]], axis=1
            )
            for j in range(2)
        ]

        def body(i, carry):
            span = pl.ds(i * CHIPS, CHIPS)
            rows = enc[span, :, cols].reshape(CHIPS * slot_rows, width)
            for j in range(2):
                value = dot_t(rows, weights[j]).reshape(CHIPS, slot_rows, unit)
                if k:
                    value = value + acts[j, span]
                acts[j, span] = value
            return carry

        lax.fori_loop(0, CORES, body, 0)

    pass_on(gu, gu_s, gu_r, 3, 1 - x)
    got(dn, dn_r, 0, 1 - x)
    stream(dn, dn_s, dn_r, 0, 1 - x)
    pass_on(dn, dn_s, dn_r, 2, x)
    pass_on(dn, dn_s, dn_r, 1, x)
    got(at.at[0], at_r, 0, 1 - x)
    att_side(0, 1 - x, (0, 1))
    gate_up(0)
    pass_on(dn, dn_s, dn_r, 2, 1 - x)
    pass_on(dn, dn_s, dn_r, 1, 1 - x)
    end_got(gu, gu_r, 1)
    gate_up(1)
    pass_on(dn, dn_s, dn_r, 3, x)
    end_got(gu, gu_r, 2)
    gate_up(2)
    pass_on(dn, dn_s, dn_r, 3, 1 - x)
    for side in (x, 1 - x):
        stream(at.at[0], at_s, at_r, 0, side)
    end_got(gu, gu_r, 3)
    gate_up(3)

    def activate(i, carry):
        inner[i] = (jax.nn.gelu(acts[0, i], approximate=True) * acts[1, i]).astype(jnp.bfloat16)
        return carry

    lax.fori_loop(0, CHIPS * CORES, activate, 0)

    def encode(total):
        top = jnp.max(jnp.max(jnp.abs(total), axis=0, keepdims=True), axis=1, keepdims=True)
        power = jnp.ceil(jnp.log(jnp.maximum(top, 1e-30) / QUANT) * (1.0 / math.log(2.0)) + 0.01)
        coded = jnp.round(total * jnp.exp2(-power))
        row = lax.broadcasted_iota(jnp.int32, coded.shape, 0)
        return jnp.where(row < slot_rows - 8, coded, power).astype(jnp.int32).astype(jnp.int16)

    def decode(coded):
        coded = coded.astype(jnp.int32).astype(jnp.float32)
        return coded * jnp.exp2(coded[slot_rows - 8 : slot_rows - 7, 0:1])

    wing = dn.shape[3]
    here, by_x, by_y = 2 * x + y, 2 * (1 - x) + y, 2 * x + 1 - y
    far = 2 * (1 - x) + 1 - y
    routes = [(across, (by_x, far), by_y, aside), (aside, (by_y, far), by_x, across)]

    def wing_cols(at_z, j):
        return pl.ds(pl.multiple_of((at_z * 2 + j) * wing, wing), wing)

    def down_first(k):
        at_z = order[k]
        weights = jnp.concatenate([dn[at_z, 0], dn[at_z, 1]], axis=1)

        def half(which):
            span = pl.ds(which * CHIPS, CHIPS)
            rows = inner[span].reshape(CHIPS * slot_rows, unit)
            return add_rows(rows, weights).reshape(CHIPS, slot_rows, weights.shape[1])

        part_out[at_z] = half(1 - n)
        send(part_out.at[at_z], part_in.at[at_z], part_s.at[at_z], part_r.at[at_z], twin)
        part_own[...] = half(n)

    def down_second(k):
        at_z = order[k]
        arrived(part_in.at[at_z], part_r.at[at_z])
        for j, (peer, away, near, _) in enumerate(routes):
            lane = pl.ds(j * wing, wing)

            def total(c):
                return part_own[c, :, lane] + part_in[at_z, c, :, lane]

            for i, c in enumerate(away):
                share_out[at_z, j, i] = encode(total(c))
            send(share_out.at[at_z, j], share_in.at[at_z, j], share_s.at[at_z, j], share_r.at[at_z, j], peer)
            kept[at_z, j] = total(near)
            cols = wing_cols(at_z, j)
            resid[:, cols] = hid[:, cols] + total(here)

    def down_third(k):
        at_z = order[k]
        for j, (_, _, _, peer) in enumerate(routes):
            arrived(share_in.at[at_z, j], share_r.at[at_z, j])
            last_out[at_z, j] = encode(kept[at_z, j] + decode(share_in[at_z, j, 1]))
            send(last_out.at[at_z, j], last_in.at[at_z, j], last_s.at[at_z, j], last_r.at[at_z, j], peer)
            cols = wing_cols(at_z, j)
            resid[:, cols] = resid[:, cols] + decode(share_in[at_z, j, 0])

    def take_att(k, side):
        pass_on(at.at[0], at_s, at_r, k, side)

    down_first(0)
    down_second(0)
    take_att(2, x)
    take_att(1, x)
    end_got(dn, dn_r, 1)
    down_first(1)
    down_second(1)
    down_third(0)
    take_att(2, 1 - x)
    take_att(1, 1 - x)
    for d in range(1, PLANES):
        q = (z + d) % PLANES
        send(found.at[q], found_in.at[z], emb_s.at[d], emb_r.at[z], on(x, y, q, n))
    end_got(dn, dn_r, 2)
    down_first(2)
    down_second(2)
    down_third(1)
    for side in (x, 1 - x):
        take_att(3, side)
    end_got(dn, dn_r, 3)
    down_first(3)
    down_second(3)
    down_third(2)
    end_got(at.at[0], at_r, 1)
    down_third(3)
    end_got(at.at[0], at_r, 2)
    for k in (1, 2):
        for side in (x, 1 - x):
            att_side(k, side)

    summed = found[z].astype(jnp.float32)
    for d in range(1, PLANES):
        q = (z + d) % PLANES
        arrived(found_in.at[q], emb_r.at[q])
        summed = summed + found_in[q].astype(jnp.float32)
    pair_out[...] = summed.astype(jnp.bfloat16)
    send(pair_out, pair_in, one_s.at[1], one_r.at[1], across)
    arrived(pair_in, one_r.at[1])
    half = (pair_out[...].astype(jnp.float32) + pair_in[...].astype(jnp.float32)).astype(jnp.bfloat16)
    half_in[n] = half
    send(half_in.at[n], half_in.at[n], one_s.at[2], one_r.at[2], twin)
    arrived(half_in.at[1 - n], one_r.at[2])
    embedded = jnp.concatenate([half_in[0], half_in[1]], axis=1).astype(jnp.float32)
    dec_rows[0] = rms_scale(embedded, gain_dec[...][None]).astype(jnp.bfloat16)
    send(dec_rows.at[0], dec_rows.at[1], one_s.at[5], one_r.at[5], aside)

    for k in range(PLANES):
        at_z = order[k]
        for j in range(2):
            arrived(last_in.at[at_z, j], last_r.at[at_z, j])
            cols = wing_cols(at_z, j)
            resid[:, cols] = resid[:, cols] + decode(last_in[at_z, j])
    spot = 2 * x + n
    mem[spot] = rms_scale(resid[...], gain_out[...][None]).astype(jnp.bfloat16)
    send(mem.at[spot], mem.at[spot], mem_s.at[0], mem_r.at[spot], across)
    send(mem.at[spot], mem.at[spot], mem_s.at[1], mem_r.at[spot], twin)

    end_got(at.at[0], at_r, 3)
    for side in (x, 1 - x):
        att_side(3, side)
    for k in range(1, PLANES):
        for side in (x, 1 - x):
            att_side(k, side, (1,))
    for k in range(PLANES):
        for side in range(2):
            rows = pl.ds((2 * k + side) * depth, depth)
            weight_q[rows, :] = at[0, k, side, q_rows, :]
    arrived(dec_rows.at[1], one_r.at[5])
    both = dec_rows[...].reshape(2 * answers, dec_rows.shape[2])
    query_two = add_rows(both, weight_q[...]).astype(jnp.bfloat16)
    query_rows[0] = query_two[:answers]
    query_out[...] = query_two[answers:]
    send(query_out, query_rows.at[1], one_s.at[6], one_r.at[6], aside)
    for k in range(PLANES):
        for side in range(2):
            arrived(at.at[1, k, side, kv_rows], at_yr.at[k, side, 0])
    for h in range(2):
        for k in range(PLANES):
            for side in range(2):
                cols = pl.ds(h * head_cols, head_cols)
                rows = pl.ds((2 * k + side) * depth, depth)
                for j, array in enumerate((weight_k, weight_v)):
                    array[rows, cols] = at[h, k, side, pl.ds(j * depth, depth), :]

    def project(j):
        keys[j] = add_rows(mem[j], weight_k[...]).astype(jnp.bfloat16)
        values[j] = add_rows(mem[j], weight_v[...]).astype(jnp.bfloat16)

    project(spot)
    spot_twin = 2 * x + 1 - n
    arrived(mem.at[spot_twin], mem_r.at[spot_twin])
    first = mem[2 * x]
    second = mem[2 * x + 1]
    memory_out[pl.ds(0, late), :] = first[:late]
    first, second = first.astype(jnp.float32), second.astype(jnp.float32)
    middle = jnp.concatenate([first[late:seg], second[: slot_rows - seg]], axis=0)
    memory_out[pl.ds(late, slot_rows - late), :] = middle.astype(jnp.bfloat16)
    memory_out[pl.ds(slot_rows, late), :] = second[slot_rows - seg : seg].astype(jnp.bfloat16)
    project(spot_twin)
    spot_x = 2 * (1 - x) + n
    arrived(mem.at[spot_x], mem_r.at[spot_x])
    send(mem.at[spot_x], mem.at[spot_x], mem_s.at[2], mem_r.at[spot_x], twin)
    project(spot_x)
    spot_far = 2 * (1 - x) + 1 - n
    arrived(mem.at[spot_far], mem_r.at[spot_far])
    project(spot_far)
    arrived(lens_all.at[1 - x], one_r.at[0])

    arrived(query_rows.at[1], one_r.at[6])
    query = jnp.concatenate([query_rows[0], query_rows[1]], axis=1)
    columns = 2 * head_cols
    heads = columns // HEAD_DIM
    lane_head = lax.broadcasted_iota(jnp.int32, (answers, columns), 1) // HEAD_DIM
    stacked = jnp.concatenate(
        [jnp.where(lane_head == h, query.astype(jnp.float32), 0.0) for h in range(heads)], axis=0
    ).astype(jnp.bfloat16)
    tokens = 2 * CORES * slot_rows
    key_rows = keys[...].reshape(tokens, columns)
    value_rows = values[...].reshape(tokens, columns)
    scores = dot_t(stacked, key_rows) * (1.0 / math.sqrt(HEAD_DIM))
    token = lax.broadcasted_iota(jnp.int32, (1, tokens), 1)
    live = token < 0
    for j in range(2 * CORES):
        length = lens_all[j // CORES, j % CORES : j % CORES + 1, 0:1]
        live = live | ((token >= j * slot_rows) & (token < j * slot_rows + length))
    scores = jnp.where(live, scores, FLOOR)
    peak = jnp.max(scores, axis=1, keepdims=True)
    weights = jnp.exp(scores - peak)
    total = jnp.sum(weights, axis=1, keepdims=True)
    coarse = weights.astype(jnp.bfloat16)
    fine = (weights - coarse.astype(jnp.float32)).astype(jnp.bfloat16)
    mixed = (add_rows(coarse, value_rows) + add_rows(fine, value_rows)) / total
    attended = jnp.where(lane_head == 0, mixed[:answers], 0.0)
    for h in range(1, heads):
        attended = jnp.where(lane_head == h, mixed[h * answers : (h + 1) * answers], attended)
    for k in range(PLANES):
        for side in range(2):
            arrived(at.at[1, k, side, o_rows], at_yr.at[k, side, 1])
    for h in range(2):
        for k in range(PLANES):
            for side in range(2):
                cols = pl.ds((2 * k + side) * depth, depth)
                weight_o[pl.ds(h * head_cols, head_cols), cols] = at[h, k, side, o_rows, :]
    partial = add_rows(attended.astype(jnp.bfloat16), weight_o[...])
    half_cols = partial.shape[1] // 2
    low, high = partial[:, :half_cols], partial[:, half_cols:]
    tail_out[...] = jnp.where(n == 0, high, low)
    send(tail_out, tail_in, one_s.at[3], one_r.at[3], twin)
    own = jnp.where(n == 0, low, high)
    arrived(tail_in, one_r.at[3])
    own = own + tail_in[...]
    tail_sum[...] = own
    send(tail_sum, tail_pair, one_s.at[4], one_r.at[4], across)
    base = half_in[n].astype(jnp.float32)
    arrived(tail_pair, one_r.at[4])
    dec_all[z] = (base + (own + tail_pair[...])).astype(jnp.bfloat16)
    for d in range(1, PLANES):
        q = (z + d) % PLANES
        send(dec_all.at[z], dec_all.at[z], dec_s.at[d], dec_r.at[z], on(x, y, q, n))
    for d in range(1, PLANES):
        q = (z + d) % PLANES
        arrived(dec_all.at[q], dec_r.at[q])
    decoded_out[...] = dec_all[...].reshape(decoded_out.shape)
    for copy, cond in pending:
        if cond is None:
            copy().wait_send()
        else:
            pl.when(cond)(lambda copy=copy: copy().wait_send())


def per_device(
    hidden_in,
    ffn_gain,
    wi_gate,
    wi_up,
    wo_down,
    final_gain,
    key_w,
    value_w,
    query_w,
    out_w,
    dec_gain,
    embed,
    lengths,
    answer_ids,
):
    sizes = tuple(lax.axis_size(a) for a in ("groups", "wide", "narrow"))
    rows_ok = hidden_in.shape[0] % 16 == 0 and lengths.shape[0] == CORES
    if sizes != (2, 2 * PLANES, CORES) or QUEST != PLANES or not rows_ok:
        return per_device_any(
            hidden_in,
            ffn_gain,
            wi_gate,
            wi_up,
            wo_down,
            final_gain,
            key_w,
            value_w,
            query_w,
            out_w,
            dec_gain,
            embed,
            lengths,
            answer_ids,
        )
    rows, features = hidden_in.shape
    slot_rows = -(-(rows // CORES) // 16) * 16
    depth = wi_gate.shape[0]
    unit = wi_gate.shape[1] // CHIPS
    head_cols = key_w.shape[1] // CHIPS
    answers = answer_ids.shape[1]
    width = features // PLANES
    half = features // 2
    bf, f32 = jnp.bfloat16, jnp.float32
    slots = CHIPS * CORES
    wing = width // 2
    dma = pltpu.SemaphoreType.DMA
    vmem = pl.BlockSpec(memory_space=pltpu.VMEM)
    memory, decoded = pl.pallas_call(
        reader,
        out_shape=(
            jax.ShapeDtypeStruct((rows, features), bf),
            jax.ShapeDtypeStruct((QUEST * answers, half), bf),
        ),
        in_specs=[vmem] * 11
        + [pl.BlockSpec(memory_space=pl.ANY), pl.BlockSpec(memory_space=pltpu.SMEM), vmem],
        out_specs=(vmem, vmem),
        scratch_shapes=[
            pltpu.VMEM((slot_rows, features), f32),
            pltpu.VMEM((2, wi_gate.shape[1], depth), bf),
            pltpu.VMEM((PLANES, 2, 2 * unit, depth), bf),
            pltpu.VMEM((2 * unit, depth), bf),
            pltpu.VMEM((PLANES, 2, unit, depth), bf),
            pltpu.VMEM((2, PLANES, 2, 3 * depth + head_cols, head_cols), bf),
            pltpu.VMEM((3 * depth + head_cols, head_cols), bf),
            pltpu.VMEM((slots, slot_rows, features), bf),
            pltpu.VMEM((2, slots, slot_rows, unit), f32),
            pltpu.VMEM((slots, slot_rows, unit), bf),
            pltpu.VMEM((embed.shape[0], half), bf),
            pltpu.VMEM((CHIPS, slot_rows, width), f32),
            pltpu.VMEM((PLANES, CHIPS, slot_rows, width), f32),
            pltpu.VMEM((PLANES, CHIPS, slot_rows, width), f32),
            pltpu.VMEM((PLANES, 2, 2, slot_rows, wing), jnp.int16),
            pltpu.VMEM((PLANES, 2, 2, slot_rows, wing), jnp.int16),
            pltpu.VMEM((PLANES, 2, slot_rows, wing), f32),
            pltpu.VMEM((PLANES, 2, slot_rows, wing), jnp.int16),
            pltpu.VMEM((PLANES, 2, slot_rows, wing), jnp.int16),
            pltpu.VMEM((2, answers, features), bf),
            pltpu.VMEM((2, answers, head_cols), bf),
            pltpu.VMEM((answers, head_cols), bf),
            pltpu.VMEM((slot_rows, features), f32),
            pltpu.VMEM((2 * CORES, slot_rows, features), bf),
            pltpu.VMEM((QUEST, answers, half), bf),
            pltpu.VMEM((QUEST, answers, half), bf),
            pltpu.VMEM((answers, half), bf),
            pltpu.VMEM((answers, half), bf),
            pltpu.VMEM((CORES, answers, half), bf),
            pltpu.VMEM((2, 8, 128), jnp.int32),
            pltpu.VMEM((features, 2 * head_cols), bf),
            pltpu.VMEM((features, 2 * head_cols), bf),
            pltpu.VMEM((features, head_cols), bf),
            pltpu.VMEM((2 * head_cols, features), bf),
            pltpu.VMEM((2 * CORES, slot_rows, 2 * head_cols), bf),
            pltpu.VMEM((2 * CORES, slot_rows, 2 * head_cols), bf),
            pltpu.VMEM((answers, half), f32),
            pltpu.VMEM((answers, half), f32),
            pltpu.VMEM((answers, half), f32),
            pltpu.VMEM((answers, half), f32),
            pltpu.VMEM((QUEST, answers, half), bf),
            dma((5, 2)),
            dma((PLANES, 2)),
            dma((5, 2)),
            dma((PLANES, 2)),
            dma((5, 2)),
            dma((PLANES, 2)),
            dma((PLANES, 2, 2)),
            dma((PLANES, 2, 2)),
            dma((4,)),
            dma((8,)),
            dma((slots + 2,)),
            dma((PLANES,)),
            dma((PLANES,)),
            dma((PLANES, 2)),
            dma((PLANES, 2)),
            dma((PLANES, 2)),
            dma((PLANES, 2)),
            dma((PLANES,)),
            dma((PLANES,)),
            dma((7,)),
            dma((7,)),
            dma((3,)),
            dma((2 * CORES,)),
            dma((PLANES,)),
            dma((PLANES,)),
            dma,
        ],
        compiler_params=pltpu.CompilerParams(
            collective_id=0, has_side_effects=True, vmem_limit_bytes=62 * 2**20
        ),
    )(
        hidden_in,
        ffn_gain,
        wi_gate,
        wi_up,
        wo_down,
        final_gain,
        key_w,
        value_w,
        query_w,
        out_w,
        dec_gain,
        embed,
        lengths,
        answer_ids,
    )
    return memory, decoded


def solution(mesh):
    placed = (
        P(("groups", "wide"), None),
        P(),
        P("wide", "narrow"),
        P("wide", "narrow"),
        P("narrow", "wide"),
        P(),
        P("wide", "narrow"),
        P("wide", "narrow"),
        P("wide", "narrow"),
        P("narrow", "wide"),
        P(),
        P("wide", None),
        P(("groups", "wide")),
        P("groups", None),
    )
    return jax.shard_map(
        per_device,
        mesh=mesh,
        in_specs=placed,
        out_specs=(P(("groups", "wide"), None), P("groups", "narrow")),
        check_vma=False,
    )
```

```python
import functools
import math

import jax
import jax.numpy as jnp
from jax import lax
from jax.experimental import pallas as pl
from jax.experimental.pallas import tpu as pltpu
from jax.sharding import PartitionSpec as P

HEAD_DIM = 64
QUEST = 4


EPS = 1e-06
FLOOR = -1e30


def swap(values, axis, distance=1):
    pairs = [(i, i ^ distance) for i in range(lax.axis_size(axis))]
    return jax.tree.map(lambda a: lax.ppermute(a, axis, pairs), values)


def ordered(bit, own, other, dim):
    first = jnp.where(bit == 0, own, other)
    second = jnp.where(bit == 0, other, own)
    return jnp.concatenate([first, second], axis=dim)


def part(values, index, count, dim):
    size = values.shape[dim] // count
    return lax.dynamic_slice_in_dim(values, index * size, size, dim)


def line_gather(block, place, count):
    size = lax.axis_size("wide")
    stride = size // count
    if count > 8:
        groups = [[i * stride + j for i in range(count)] for j in range(stride)]
        return lax.all_gather(block, "wide", axis_index_groups=groups)
    up = [(i, i + stride) for i in range(size - stride)]
    down = [(i + stride, i) for i in range(size - stride)]
    below, above = [], []
    from_below = from_above = block
    for _ in range(count - 1):
        from_below = lax.ppermute(from_below, "wide", up)
        from_above = lax.ppermute(from_above, "wide", down)
        below.insert(0, from_below)
        above.append(from_above)
    return lax.dynamic_slice_in_dim(
        jnp.stack(below + [block] + above), count - 1 - place, count, 0
    )


def rms_scale(values, gain):
    mean_square = jnp.mean(values * values, axis=-1, keepdims=True)
    return values * lax.rsqrt(mean_square + EPS) * gain.astype(jnp.float32)


def add_rows(left, piece):
    return jnp.dot(left, piece, preferred_element_type=jnp.float32)


def join_partial(first, second):
    top = jnp.maximum(first[0], second[0])
    factor_first = jnp.exp(first[0] - top)
    factor_second = jnp.exp(second[0] - top)
    return (
        top,
        first[1] * factor_first + second[1] * factor_second,
        first[2] * factor_first + second[2] * factor_second,
    )


def per_device_any(
    hidden_in,
    ffn_gain,
    wi_gate,
    wi_up,
    wo_down,
    final_gain,
    key_w,
    value_w,
    query_w,
    out_w,
    dec_gain,
    embed,
    lengths,
    answer_ids,
):
    rows, features = hidden_in.shape
    wide = lax.axis_size("wide")
    group, place, core = (lax.axis_index(a) for a in ("groups", "wide", "narrow"))
    side, pair = place % 2, place // 2
    pairs = wide // 2
    quarters = 2 * lax.axis_size("groups")
    lanes = 128

    def for_side(target, pieces):
        quarter = target * (quarters // 2) + group
        return jnp.concatenate(
            [part(a, quarter, quarters, dim).reshape(-1, lanes) for a, dim in pieces]
        )

    def paired(pieces):
        own = for_side(side, pieces)
        other = swap(for_side(1 - side, pieces), "wide")
        return ordered(side, own[None], other[None], 0)

    def gathered(both):
        return line_gather(both, pair, pairs).reshape(wide, *both.shape[1:])

    hidden_units = wi_gate.shape[1] // quarters
    depth = wi_gate.shape[0]
    ffn = gathered(paired(((wi_gate.T, 0), (wi_up.T, 0), (wo_down, 0))))
    ffn = ffn.reshape(wide, 3, hidden_units, depth).transpose(1, 2, 0, 3)
    gate_t, up_t, down = ffn.reshape(3, hidden_units, features)

    def over_plane(own):
        couple = jnp.concatenate([own, swap(own, "wide")])
        return jnp.concatenate([couple, swap(couple, "groups")])

    def both_halves(own):
        return ordered(core, own, swap(own, "narrow"), 1)

    answers = answer_ids.shape[1]
    per_question = wide // QUEST
    qrows = answer_ids.shape[0] * answers
    vocab_rows = embed.shape[0]
    local_ids = answer_ids.reshape(qrows) - place * vocab_rows
    onehot = (local_ids[:, None] == jnp.arange(vocab_rows, dtype=jnp.int32)[None, :]).astype(
        jnp.bfloat16
    )
    found = jnp.dot(onehot, embed, preferred_element_type=jnp.float32).astype(jnp.bfloat16)
    found = part(found, core, 2, 1)
    distance = wide // 2
    while distance:
        if distance >= per_question:
            bit = place // distance % 2
            found = part(found, bit, 2, 0) + swap(part(found, 1 - bit, 2, 0), "wide", distance)
        else:
            found = found + swap(found, "wide", distance)
        distance //= 2
    embedded_half = found.astype(jnp.float32)
    dec_own = rms_scale(both_halves(found).astype(jnp.float32), dec_gain).astype(jnp.bfloat16)
    dec_in = jnp.concatenate([dec_own, swap(dec_own, "groups")])

    columns = key_w.shape[1] // quarters
    att_pair = paired(((key_w, 1), (value_w, 1), (query_w, 1), (out_w, 0)))
    lengths_all = over_plane(lengths)

    resid_in = hidden_in.astype(jnp.float32)
    enc_own = rms_scale(resid_in, ffn_gain).astype(jnp.bfloat16)
    enc_in = both_halves(over_plane(part(enc_own, core, 2, 1)))
    enc_in, dec_in, lengths_all, att_pair, embedded_half = lax.optimization_barrier(
        (enc_in, dec_in, lengths_all, att_pair, embedded_half)
    )
    contract_last = (((1,), (1,)), ((), ()))
    gate = lax.dot_general(enc_in, gate_t, contract_last, preferred_element_type=jnp.float32)
    up = lax.dot_general(enc_in, up_t, contract_last, preferred_element_type=jnp.float32)
    inner = (jax.nn.gelu(gate, approximate=True) * up).astype(jnp.bfloat16)
    sent_half = add_rows(inner, part(down, 1 - core, 2, 1))
    received_half = swap(sent_half, "narrow")
    sums = add_rows(inner, part(down, core, 2, 1)) + received_half

    def keep_half(values):
        return part(values, core, 2, 1) + swap(part(values, 1 - core, 2, 1), "narrow")

    blocks = sums.reshape(4, rows, -1)
    middle = blocks.shape[2] // 2
    early, late = blocks[:, :, :middle], blocks[:, :, middle:]
    early = early[:2] + swap(early[2:], "groups")
    late = late[::2] + swap(late[1::2], "wide")
    early = early[0] + swap(early[1], "wide")
    late = late[0] + swap(late[1], "groups")
    share = jnp.concatenate([early, late], axis=1)
    resid_half = part(resid_in, core, 2, 1) + share
    own_squares = jnp.sum(resid_half * resid_half, axis=1)
    squares = (own_squares + swap(own_squares, "narrow"))[:, None]
    gain_half = part(final_gain, core, 2, 0).astype(jnp.float32)
    memory_half = (resid_half * lax.rsqrt(squares / features + EPS) * gain_half).astype(
        jnp.bfloat16
    )
    memory_early, memory_late = memory_half[:, :middle], memory_half[:, middle:]
    twin = jnp.stack([memory_late, swap(memory_late, "groups")])
    late_all = jnp.stack([twin, swap(twin, "wide")], axis=1).reshape(4 * rows, middle)
    early_all = over_plane(memory_early)
    early_other, late_other = swap(early_all, "narrow"), swap(late_all, "narrow")
    other_half = jnp.concatenate([early_other[:rows], late_other[:rows]], axis=1)
    memory = ordered(core, memory_half, other_half, 1)

    att = gathered(att_pair)
    att = att.reshape(wide, 4, -1)
    key_q, value_q, query_q = (att[:, i].reshape(features, columns) for i in range(3))
    out_q = att[:, 3].reshape(wide, columns, depth).transpose(1, 0, 2).reshape(columns, features)

    def project(weight):
        own, other = part(weight, core, 2, 0), part(weight, 1 - core, 2, 0)
        return (
            add_rows(early_all, own[:middle])
            + add_rows(late_all, own[middle:])
            + add_rows(early_other, other[:middle])
            + add_rows(late_other, other[middle:])
        ).astype(jnp.bfloat16)

    heads = columns // HEAD_DIM
    keys = project(key_q).reshape(2, 2 * rows, columns)
    values = project(value_q).reshape(2, 2 * rows, columns).astype(jnp.float32)
    query = add_rows(dec_in, query_q).astype(jnp.bfloat16)
    in_head = (
        jnp.arange(columns, dtype=jnp.int32)[None, :] // HEAD_DIM
        == jnp.arange(heads, dtype=jnp.int32)[:, None]
    )[None, :, None, :]
    query_heads = jnp.where(in_head, query.reshape(2, 1, answers, columns), 0)
    scores = jnp.einsum(
        "qhac,qkc->qhak", query_heads, keys, preferred_element_type=jnp.float32
    ) * (1.0 / math.sqrt(HEAD_DIM))
    passage_len = rows // lengths.shape[0]
    live = jnp.arange(passage_len, dtype=jnp.int32)[None, :] < lengths_all[:, None]
    scores = jnp.where(live.reshape(2, 1, 1, 2 * rows), scores, FLOOR)
    top = jnp.max(scores, axis=3, keepdims=True)
    weights = jnp.exp(scores - top)
    total = jnp.sum(weights, axis=3, keepdims=True)
    acc = jnp.einsum("qhak,qkc->qhac", weights, values, precision=lax.Precision.HIGHEST)
    state = (top, total, acc)
    distance = 2
    while distance < per_question:
        state = join_partial(state, swap(state, "wide", distance))
        distance *= 2
    attended = jnp.sum(jnp.where(in_head, state[2] / state[1], 0.0), axis=1)
    attended = attended.astype(jnp.bfloat16).reshape(2 * answers, columns)
    partial_out = keep_half(jnp.dot(attended, out_q, preferred_element_type=jnp.float32))
    share_out = partial_out[:answers] + swap(partial_out[answers:], "groups")
    share_out = share_out + swap(share_out, "wide")
    decoded = (embedded_half + share_out).astype(jnp.bfloat16)
    distance = per_question
    while distance < wide:
        decoded = ordered(place // distance % 2, decoded, swap(decoded, "wide", distance), 0)
        distance *= 2
    return (memory, decoded)


MESH = pl.DeviceIdType.MESH
PLANES = 4
CHIPS = 4
CORES = 2
QUANT = 32767.0


def dot_t(left, right):
    return lax.dot_general(
        left, right, (((1,), (1,)), ((), ())), preferred_element_type=jnp.float32
    )


def reader(
    hidden_hbm,
    gain_in,
    gate_hbm,
    up_hbm,
    down_hbm,
    gain_out,
    key_hbm,
    value_hbm,
    query_hbm,
    out_hbm,
    gain_dec,
    embed,
    lengths,
    ids,
    memory_out,
    decoded_out,
    hidden,
    gate_w,
    up_w,
    down_w,
    key_w,
    value_w,
    query_w,
    out_w,
    hid,
    turned,
    gu,
    gu_side,
    dn,
    at_kv,
    at_q,
    at_o,
    side_kv,
    side_q,
    side_o,
    enc,
    acts,
    inner,
    table,
    part_own,
    part_out,
    part_in,
    share_out,
    share_in,
    kept,
    last_out,
    last_in,
    full_out,
    full_in,
    memory_buf,
    dec_rows,
    query_rows,
    query_out,
    resid,
    mem,
    found,
    found_in,
    pair_out,
    pair_in,
    half_in,
    lens_all,
    weight_k,
    weight_v,
    weight_q,
    weight_o,
    keys,
    values,
    tail_out,
    tail_in,
    dec_all,
    gu_s,
    gu_r,
    gu_half_s,
    x_r,
    dn_s,
    dn_r,
    at_s,
    at_r,
    at_ys,
    at_yr,
    x_s,
    enc_s,
    enc_r,
    part_s,
    part_r,
    share_s,
    share_r,
    last_s,
    last_r,
    full_s,
    full_r,
    store_sem,
    tail_s,
    tail_r,
    load_sem,
    emb_s,
    emb_r,
    one_s,
    one_r,
    mem_s,
    mem_r,
    dec_s,
    dec_r,
    table_sem,
):
    y, place, n = (lax.axis_index(a) for a in ("groups", "wide", "narrow"))
    z, x = place // 2, place % 2
    upper = z // 2
    w = z + upper * (PLANES - 1 - 2 * z)

    def plane(mirrored):
        return mirrored + upper * (PLANES - 1 - 2 * mirrored)

    order = [z, plane(1 - w), plane(2), plane(3)]
    slot_rows = hid.shape[0]
    unit = gu.shape[2] // 2
    head_cols = at_kv.shape[4]

    def on(x_at, y_at, z_at, n_at):
        return {"groups": y_at, "wide": z_at * 2 + x_at, "narrow": n_at}

    across = on(1 - x, y, z, n)
    aside = on(x, 1 - y, z, n)
    corner = on(1 - x, 1 - y, z, n)
    twin = on(x, y, z, 1 - n)
    across_twin = on(1 - x, y, z, 1 - n)
    next_a = on(x, y, order[1], n)
    next_b = on(x, y, plane(2), n)
    inside = w == 1
    pending = []

    def send(source, target, send_sem, recv_sem, device, cond=None):
        def copy():
            return pltpu.make_async_remote_copy(
                source, target, send_sem, recv_sem, device_id=device, device_id_type=MESH
            )

        if cond is None:
            copy().start()
        else:
            pl.when(cond)(lambda: copy().start())
        pending.append((copy, cond))

    def arrived(target, recv_sem):
        pltpu.make_async_remote_copy(
            target, target, recv_sem, recv_sem, device_id=twin, device_id_type=MESH
        ).wait_recv()

    barrier = pltpu.get_barrier_semaphore()
    peers = [across, aside, corner, twin, across_twin]
    peers += [on(x, y, (z + d) % PLANES, n) for d in range(1, PLANES)]
    for peer in peers:
        pl.semaphore_signal(barrier, inc=1, device_id=peer, device_id_type=MESH)

    loads = [
        pltpu.make_async_copy(source, target, load_sem.at[j])
        for j, (source, target) in enumerate(
            (
                (gate_hbm, gate_w),
                (up_hbm, up_w),
                (hidden_hbm, hidden),
                (down_hbm, down_w),
                (key_hbm, key_w),
                (value_hbm, value_w),
                (query_hbm, query_w),
                (out_hbm, out_w),
            )
        )
    ]
    for copy in loads:
        copy.start()
    table_copy = pltpu.make_async_copy(
        embed.at[:, pl.ds(pl.multiple_of(n * table.shape[1], 128), table.shape[1])],
        table,
        table_sem,
    )
    table_copy.start()

    lanes = 128
    for j, array in enumerate((gate_w, up_w)):
        loads[j].wait()
        for k in range(array.shape[1] // lanes):
            cols = pl.ds(k * lanes, lanes)
            turned[j, cols, :] = array[:, cols].T
    mine = pl.multiple_of((2 * x + y) * unit, 16)
    theirs = pl.multiple_of((2 * (1 - x) + y) * unit, 16)
    for j in range(2):
        gu_side[pl.ds(j * unit, unit), :] = turned[j, pl.ds(theirs, unit), :]
        gu[z, x, pl.ds(j * unit, unit), :] = turned[j, pl.ds(mine, unit), :]
    pl.semaphore_wait(barrier, len(peers))

    def stream(buf, s_sem, r_sem, k, side):
        at_z = order[k]
        if k == 0:
            send(buf.at[at_z, side], buf.at[at_z, side], s_sem.at[0, side], r_sem.at[at_z, side], next_a)
            send(buf.at[at_z, side], buf.at[at_z, side], s_sem.at[4, side], r_sem.at[at_z, side], next_b, inside)
        else:
            target = next_b if k == 1 else next_a
            send(buf.at[at_z, side], buf.at[at_z, side], s_sem.at[k, side], r_sem.at[at_z, side], target, inside)

    streams = ((at_kv.at[0], 0), (at_q, 1), (at_o.at[0], 2))

    def att_stream(j, k):
        buf = streams[j][0].at[order[k]]
        if k == 0:
            send(buf, buf, at_s.at[j, 0], at_r.at[j, order[0]], next_a)
            send(buf, buf, at_s.at[j, 4], at_r.at[j, order[0]], next_b, inside)
        else:
            send(buf, buf, at_s.at[j, k], at_r.at[j, order[k]], next_b if k == 1 else next_a, inside)

    def att_got(j, k):
        arrived(streams[j][0].at[order[k]], at_r.at[j, order[k]])

    def att_pass(j, k):
        pl.when(inside)(lambda: att_got(j, k))
        att_stream(j, k)

    def att_end(j, k):
        pl.when(w == 0)(lambda: att_got(j, k))

    def att_side_send(j, k):
        buf, sem = ((at_kv, 0), None, (at_o, 1))[j]
        at_z = order[k]
        send(buf.at[0, at_z], buf.at[1, at_z], at_ys.at[sem, at_z], at_yr.at[sem, at_z], aside)

    def got(buf, r_sem, k, side):
        arrived(buf.at[order[k], side], r_sem.at[order[k], side])

    for j in range(2):
        rows = pl.ds(j * unit, unit)
        send(gu_side.at[rows], gu.at[z, x, rows], x_s.at[4 + j], x_r.at[j], across)
    stream(gu, gu_s, gu_r, 0, x)

    loads[2].wait()
    seg = hidden.shape[0] // CORES
    late = hidden.shape[0] - slot_rows
    low = hidden[pl.ds(0, slot_rows), :].astype(jnp.float32)
    high = hidden[pl.ds(late, slot_rows), :].astype(jnp.float32)
    skip = seg - late
    hid[...] = jnp.where(n == 0, low, jnp.concatenate([high[skip:], high[:skip]], axis=0))
    enc[n] = rms_scale(hid[...], gain_in[...][None]).astype(jnp.bfloat16)
    for j, (peer, r) in enumerate(((across, 1), (aside, 2), (twin, 0))):
        send(enc.at[n], enc.at[2 * r + n], enc_s.at[j], enc_r.at[2 * r + n], peer)
    for copy in loads[3:]:
        copy.wait()
    dn[z, x] = down_w[pl.ds(mine, unit), :]
    depth = key_w.shape[0]

    at_side = (side_kv, side_q, side_o)

    def columns_of(x_at, y_at):
        return pl.ds(pl.multiple_of((2 * x_at + y_at) * head_cols, head_cols), head_cols)

    for x_at, targets in ((x, (at_kv.at[0, z, x], at_q.at[z, x], at_o.at[0, z, x])), (1 - x, at_side)):
        for j, array in enumerate((key_w, value_w)):
            targets[0][pl.ds(j * depth, depth), :] = array[:, columns_of(x_at, y)]
        targets[1][...] = query_w[:, columns_of(x_at, y)]
        targets[2][...] = out_w[columns_of(x_at, y), :]
    tile_row = lax.broadcasted_iota(jnp.int32, lens_all.shape[1:], 0)
    lens_all[x] = jnp.where(tile_row == 0, lengths[0], lengths[1])

    send(down_w.at[pl.ds(theirs, unit), :], dn.at[z, x], x_s.at[1], dn_r.at[z, x], across)
    send(lens_all.at[x], lens_all.at[x], x_s.at[3], one_r.at[0], across)
    for j, target in enumerate((at_kv.at[0], at_q, at_o.at[0])):
        send(at_side[j], target.at[z, x], x_s.at[6 + j], x_r.at[2 + j], across)

    def pass_on(buf, s_sem, r_sem, k, side):
        @pl.when(inside)
        def _():
            got(buf, r_sem, k, side)

        stream(buf, s_sem, r_sem, k, side)

    def end_got(buf, r_sem, k):
        @pl.when(w == 0)
        def _():
            for side in (x, 1 - x):
                got(buf, r_sem, k, side)

    for j in range(2):
        rows = pl.ds(j * unit, unit)
        piece = gu.at[z, 1 - x, rows]
        arrived(piece, x_r.at[j])
        send(piece, piece, gu_half_s.at[j, 0], gu_r.at[z, 1 - x], next_a)
        send(piece, piece, gu_half_s.at[j, 1], gu_r.at[z, 1 - x], next_b, inside)
    for side in (x, 1 - x):
        for k in (2, 1):
            pass_on(gu, gu_s, gu_r, k, side)

    feat_half = enc.shape[2] // 2
    halves = [pl.ds(0, feat_half), pl.ds(feat_half, feat_half)]
    for j, (r, peer) in enumerate(((1, aside), (2, across))):
        arrived(enc.at[2 * r + n], enc_r.at[2 * r + n])
        send(
            enc.at[2 * r + n, :, halves[j]], enc.at[6 + n, :, halves[j]], enc_s.at[3 + j], enc_r.at[8 + j], peer
        )
    for r in (1, 2):
        send(enc.at[2 * r + n], enc.at[2 * r + n], enc_s.at[4 + r], enc_r.at[2 * r + n], twin)

    pass_on(gu, gu_s, gu_r, 3, x)

    table_copy.wait()
    vocab = table.shape[0]
    total_ids = ids.shape[0] * ids.shape[1]
    all_ids = jnp.concatenate([ids[q : q + 1, :] for q in range(ids.shape[0])], axis=1)
    chunk = 1024
    hits = jnp.zeros((total_ids, table.shape[1]), jnp.float32)
    for base in range(0, vocab, chunk):
        size = min(chunk, vocab - base)
        row = lax.broadcasted_iota(jnp.int32, (size, total_ids), 0) + (place * vocab + base)
        onehot = (row == all_ids).astype(jnp.bfloat16)
        hits = hits + lax.dot_general(
            onehot,
            table[pl.ds(base, size), :],
            (((0,), (0,)), ((), ())),
            preferred_element_type=jnp.float32,
        )
    answers = found.shape[1]
    for q in range(PLANES):
        found[q] = hits[q * answers : (q + 1) * answers].astype(jnp.bfloat16)

    def gate_up(k, first_r, last_r, which=None):
        at_z = order[k]
        width = 2 * gu.shape[3]
        cols = pl.ds(pl.multiple_of(at_z * width, width), width)
        weights = [
            jnp.concatenate(
                [gu[at_z, 0, pl.ds(j * unit, unit), :], gu[at_z, 1, pl.ds(j * unit, unit), :]], axis=1
            )
            for j in range(2)
        ]

        def rows_of(first, second):
            rows = jnp.concatenate([enc[first, :, cols], enc[second, :, cols]], axis=0)
            for j in range(2):
                value = dot_t(rows, weights[j])
                for i, at_slot in enumerate((first, second)):
                    part_value = value[i * slot_rows : (i + 1) * slot_rows]
                    acts[j, at_slot] = part_value + acts[j, at_slot] if k else part_value

        def body(i, carry):
            rows_of(2 * i, 2 * i + 1)
            return carry

        if which is None:
            lax.fori_loop(first_r, last_r, body, 0)
        else:

            def body_half(i, carry):
                rows_of(4 * i + which, 4 * i + 2 + which)
                return carry

            lax.fori_loop(0, CHIPS // 2, body_half, 0)

    for r in (0, 1, 2):
        arrived(enc.at[2 * r + 1 - n], enc_r.at[2 * r + 1 - n])
    gate_up(0, 0, 3)
    pass_on(gu, gu_s, gu_r, 3, 1 - x)
    for d in range(1, PLANES):
        q = (z + d) % PLANES
        send(found.at[q], found_in.at[z], emb_s.at[d], emb_r.at[z], on(x, y, q, n))
    stream(dn, dn_s, dn_r, 0, x)
    end_got(gu, gu_r, 1)
    gate_up(1, 0, 3)
    end_got(gu, gu_r, 2)
    gate_up(2, 0, 3)
    got(dn, dn_r, 0, 1 - x)
    stream(dn, dn_s, dn_r, 0, 1 - x)
    for j in range(2):
        arrived(enc.at[6 + n, :, halves[j]], enc_r.at[8 + j])
    send(enc.at[6 + n], enc.at[6 + n], enc_s.at[7], enc_r.at[6 + n], twin)
    pass_on(dn, dn_s, dn_r, 2, x)
    pass_on(dn, dn_s, dn_r, 1, x)
    for j, (buf, _) in enumerate(streams):
        arrived(buf.at[z, 1 - x], x_r.at[2 + j])
    att_side_send(0, 0)
    att_side_send(2, 0)
    arrived(enc.at[7 - n], enc_r.at[7 - n])
    for k in range(3):
        gate_up(k, 3, 4)
    pass_on(dn, dn_s, dn_r, 2, 1 - x)
    pass_on(dn, dn_s, dn_r, 1, 1 - x)
    end_got(gu, gu_r, 3)

    def activate(which):
        def body(i, carry):
            at_slot = 2 * i + which
            inner[at_slot] = (
                jax.nn.gelu(acts[0, at_slot], approximate=True) * acts[1, at_slot]
            ).astype(jnp.bfloat16)
            return carry

        lax.fori_loop(0, CHIPS, body, 0)

    def exponent(top):
        return jnp.ceil(jnp.log(jnp.maximum(top, 1e-30) / QUANT) * (1.0 / math.log(2.0)) + 0.01)

    def encode(total):
        top = jnp.max(jnp.max(jnp.abs(total), axis=0, keepdims=True), axis=1, keepdims=True)
        power = exponent(top)
        coded = jnp.round(total * jnp.exp2(-power))
        row = lax.broadcasted_iota(jnp.int32, coded.shape, 0)
        return jnp.where(row < slot_rows - 8, coded, power).astype(jnp.int32).astype(jnp.int16)

    def decode(coded):
        coded = coded.astype(jnp.int32).astype(jnp.float32)
        return coded * jnp.exp2(coded[slot_rows - 8 : slot_rows - 7, 0:1])

    here, by_x, by_y, far = range(CHIPS)
    wing = dn.shape[3]

    def wing_cols(at_z, j):
        return pl.ds(pl.multiple_of((at_z * 2 + j) * wing, wing), wing)

    def down_half(k, which):
        at_z = order[k]
        weights = jnp.concatenate([dn[at_z, 0], dn[at_z, 1]], axis=1)
        rows = jnp.concatenate([inner[2 * r + which] for r in range(CHIPS)], axis=0)
        return add_rows(rows, weights).reshape(CHIPS, slot_rows, weights.shape[1])

    def down_send(k):
        at_z = order[k]
        part_out[at_z] = down_half(k, 1 - n)
        send(part_out.at[at_z], part_in.at[at_z], part_s.at[at_z], part_r.at[at_z], twin)

    def down_first(k):
        down_send(k)
        part_own[...] = down_half(k, n)

    def down_second(k):
        at_z = order[k]
        arrived(part_in.at[at_z], part_r.at[at_z])
        for j, (peer, away, stay) in enumerate(
            ((across, (by_x, far), (here, by_y)), (aside, (by_y, far), (here, by_x)))
        ):
            lane = pl.ds(j * wing, wing)

            def total(c):
                return part_own[c, :, lane] + part_in[at_z, c, :, lane]

            for i, c in enumerate(away):
                share_out[at_z, j, i] = encode(total(c))
            send(share_out.at[at_z, j], share_in.at[at_z, j], share_s.at[at_z, j], share_r.at[at_z, j], peer)
            kept[at_z, j, 0] = total(stay[0]) + hid[:, wing_cols(at_z, j)]
            kept[at_z, j, 1] = total(stay[1])

    def down_third(k):
        at_z = order[k]
        arrived(share_in.at[at_z, 0], share_r.at[at_z, 0])
        last_out[at_z, 2] = encode(kept[at_z, 0, 1] + decode(share_in[at_z, 0, 1]))
        send(last_out.at[at_z, 2], last_in.at[at_z, 2], last_s.at[at_z, 0], last_r.at[at_z, 0], aside)
        resid[0, :, wing_cols(at_z, 0)] = kept[at_z, 0, 0] + decode(share_in[at_z, 0, 0])
        arrived(share_in.at[at_z, 1], share_r.at[at_z, 1])
        pair = pl.ds(0, 2)
        for i in range(2):
            total = kept[at_z, 1, i] + decode(share_in[at_z, 1, i])
            last_out[at_z, i] = encode(total)
            resid[i, :, wing_cols(at_z, 1)] = total
        send(last_out.at[at_z, pair], last_in.at[at_z, pair], last_s.at[at_z, 1], last_r.at[at_z, 1], across)

    def down_fourth(k):
        at_z = order[k]
        arrived(last_in.at[at_z, 2], last_r.at[at_z, 0])
        cols = wing_cols(at_z, 0)
        total = resid[0, :, cols] + decode(last_in[at_z, 2])
        resid[0, :, cols] = total
        full_out[at_z] = encode(total)
        send(full_out.at[at_z], full_in.at[at_z], full_s.at[at_z], full_r.at[at_z], across)
        arrived(last_in.at[at_z, pl.ds(0, 2)], last_r.at[at_z, 1])
        cols = wing_cols(at_z, 1)
        for i in range(2):
            resid[i, :, cols] = resid[i, :, cols] + decode(last_in[at_z, 1 - i])

    att_stream(0, 0)
    gate_up(3, 0, 0, 1 - n)
    activate(1 - n)
    down_send(0)
    pass_on(dn, dn_s, dn_r, 3, x)
    gate_up(3, 0, 0, n)
    activate(n)
    part_own[...] = down_half(0, n)
    pass_on(dn, dn_s, dn_r, 3, 1 - x)
    for j in (1, 2):
        att_stream(j, 0)
    summed = found[z].astype(jnp.float32)
    for d in range(1, PLANES):
        q = (z + d) % PLANES
        arrived(found_in.at[q], emb_r.at[q])
        summed = summed + found_in[q].astype(jnp.float32)
    pair_out[...] = summed.astype(jnp.bfloat16)
    send(pair_out, pair_in, one_s.at[1], one_r.at[1], across)
    down_second(0)
    att_pass(0, 1)
    end_got(dn, dn_r, 1)
    down_first(1)
    arrived(pair_in, one_r.at[1])
    half = (pair_out[...].astype(jnp.float32) + pair_in[...].astype(jnp.float32)).astype(jnp.bfloat16)
    half_in[n] = half
    send(half_in.at[n], half_in.at[n], one_s.at[2], one_r.at[2], twin)
    down_second(1)
    att_pass(0, 2)
    att_pass(1, 1)
    att_pass(2, 1)
    down_third(0)
    end_got(dn, dn_r, 2)
    down_first(2)
    arrived(half_in.at[1 - n], one_r.at[2])
    embedded = jnp.concatenate([half_in[0], half_in[1]], axis=1).astype(jnp.float32)
    dec_rows[0] = rms_scale(embedded, gain_dec[...][None]).astype(jnp.bfloat16)
    send(dec_rows.at[0], dec_rows.at[1], one_s.at[5], one_r.at[5], aside)
    down_second(2)
    att_pass(0, 3)
    down_third(1)
    down_fourth(0)
    att_end(0, 1)
    att_side_send(0, 1)
    end_got(dn, dn_r, 3)
    down_first(3)
    down_second(3)
    att_pass(1, 2)
    att_pass(1, 3)
    down_third(2)
    att_end(0, 2)
    att_side_send(0, 2)
    att_pass(2, 2)
    down_fourth(1)
    down_third(3)
    att_end(0, 3)
    att_side_send(0, 3)
    att_pass(2, 3)
    down_fourth(2)
    for k in range(1, PLANES):
        att_end(1, k)
    for k in range(PLANES):
        for side in range(2):
            weight_q[pl.ds((2 * k + side) * depth, depth), :] = at_q[k, side]
    arrived(dec_rows.at[1], one_r.at[5])
    both = dec_rows[...].reshape(2 * answers, dec_rows.shape[2])
    query_two = add_rows(both, weight_q[...]).astype(jnp.bfloat16)
    query_rows[0] = query_two[:answers]
    query_out[...] = query_two[answers:]
    send(query_out, query_rows.at[1], one_s.at[6], one_r.at[6], aside)
    down_fourth(3)
    for k in range(1, PLANES):
        att_end(2, k)
        att_side_send(2, k)
    for k in range(PLANES):
        arrived(at_kv.at[1, k], at_yr.at[0, k])
        for side in range(2):
            rows = pl.ds((2 * k + side) * depth, depth)
            for h in range(2):
                cols = pl.ds(h * head_cols, head_cols)
                weight_k[rows, cols] = at_kv[h, k, side, pl.ds(0, depth), :]
                weight_v[rows, cols] = at_kv[h, k, side, pl.ds(depth, depth), :]
    for k in range(PLANES):
        at_z = order[k]
        arrived(full_in.at[at_z], full_r.at[at_z])
        resid[1, :, wing_cols(at_z, 0)] = decode(full_in[at_z])
    spots = [2 * x + n, 2 * (1 - x) + n, 2 * x + 1 - n, 2 * (1 - x) + 1 - n]
    for i in range(2):
        mem[spots[i]] = rms_scale(resid[i], gain_out[...][None]).astype(jnp.bfloat16)
        send(mem.at[spots[i]], mem.at[spots[i]], mem_s.at[i], mem_r.at[spots[i]], twin)

    def project(j):
        keys[j] = add_rows(mem[j], weight_k[...]).astype(jnp.bfloat16)
        values[j] = add_rows(mem[j], weight_v[...]).astype(jnp.bfloat16)

    project(spots[0])
    project(spots[1])
    arrived(mem.at[spots[2]], mem_r.at[spots[2]])
    first = mem[2 * x]
    second = mem[2 * x + 1]
    memory_buf[pl.ds(0, late), :] = first[:late]
    first, second = first.astype(jnp.float32), second.astype(jnp.float32)
    middle = jnp.concatenate([first[late:seg], second[: slot_rows - seg]], axis=0)
    memory_buf[pl.ds(late, slot_rows - late), :] = middle.astype(jnp.bfloat16)
    memory_buf[pl.ds(slot_rows, late), :] = second[slot_rows - seg : seg].astype(jnp.bfloat16)
    memory_copy = pltpu.make_async_copy(memory_buf, memory_out, store_sem.at[PLANES])
    memory_copy.start()
    project(spots[2])
    arrived(mem.at[spots[3]], mem_r.at[spots[3]])
    project(spots[3])
    arrived(lens_all.at[1 - x], one_r.at[0])

    arrived(query_rows.at[1], one_r.at[6])
    query = jnp.concatenate([query_rows[0], query_rows[1]], axis=1)
    columns = 2 * head_cols
    heads = columns // HEAD_DIM
    lane_head = lax.broadcasted_iota(jnp.int32, (answers, columns), 1) // HEAD_DIM
    stacked = jnp.concatenate(
        [jnp.where(lane_head == h, query.astype(jnp.float32), 0.0) for h in range(heads)], axis=0
    ).astype(jnp.bfloat16)
    tokens = 2 * CORES * slot_rows
    key_rows = keys[...].reshape(tokens, columns)
    value_rows = values[...].reshape(tokens, columns)
    scores = dot_t(stacked, key_rows) * (1.0 / math.sqrt(HEAD_DIM))
    token = lax.broadcasted_iota(jnp.int32, (1, tokens), 1)
    live = token < 0
    for j in range(2 * CORES):
        length = lens_all[j // CORES, j % CORES : j % CORES + 1, 0:1]
        live = live | ((token >= j * slot_rows) & (token < j * slot_rows + length))
    scores = jnp.where(live, scores, FLOOR)
    peak = jnp.max(scores, axis=1, keepdims=True)
    weights = jnp.exp(scores - peak)
    total = jnp.sum(weights, axis=1, keepdims=True)
    coarse = weights.astype(jnp.bfloat16)
    fine = (weights - coarse.astype(jnp.float32)).astype(jnp.bfloat16)
    mixed = (add_rows(coarse, value_rows) + add_rows(fine, value_rows)) / total
    attended = jnp.where(lane_head == 0, mixed[:answers], 0.0)
    for h in range(1, heads):
        attended = jnp.where(lane_head == h, mixed[h * answers : (h + 1) * answers], attended)
    for k in range(PLANES):
        arrived(at_o.at[1, k], at_yr.at[1, k])
        for side in range(2):
            for h in range(2):
                cols = pl.ds((2 * k + side) * depth, depth)
                weight_o[pl.ds(h * head_cols, head_cols), cols] = at_o[h, k, side]
    partial = add_rows(attended.astype(jnp.bfloat16), weight_o[...])
    half_cols = partial.shape[1] // 2
    low, high = partial[:, :half_cols], partial[:, half_cols:]

    def encode_wide(value):
        top = jnp.max(jnp.max(jnp.abs(value), axis=0, keepdims=True), axis=1, keepdims=True)
        power = exponent(top)
        coded = jnp.concatenate(
            [jnp.round(value * jnp.exp2(-power)), jnp.broadcast_to(power, (answers, lanes))], axis=1
        )
        return coded.astype(jnp.int32).astype(jnp.int16)

    own = jnp.where(n == 0, low, high)
    tail_out[0] = encode_wide(jnp.where(n == 0, high, low))
    send(tail_out.at[0], tail_in.at[2], tail_s.at[2], tail_r.at[2], across_twin)
    send(tail_out.at[0], tail_in.at[0], tail_s.at[0], tail_r.at[0], twin)
    tail_out[1] = encode_wide(own)
    send(tail_out.at[1], tail_in.at[1], tail_s.at[1], tail_r.at[1], across)
    total = half_in[n].astype(jnp.float32) + own
    for j in range(3):
        arrived(tail_in.at[j], tail_r.at[j])
        coded = tail_in[j].astype(jnp.int32).astype(jnp.float32)
        total = total + coded[:, :half_cols] * jnp.exp2(coded[:, half_cols : half_cols + 1])
    dec_all[z] = total.astype(jnp.bfloat16)
    for d in range(1, PLANES):
        q = (z + d) % PLANES
        send(dec_all.at[z], dec_all.at[z], dec_s.at[d], dec_r.at[z], on(x, y, q, n))
    stores = []
    for d in range(PLANES):
        q = (z + d) % PLANES
        if d:
            arrived(dec_all.at[q], dec_r.at[q])
        rows = pl.ds(pl.multiple_of(q * answers, answers), answers)
        stores.append(pltpu.make_async_copy(dec_all.at[q], decoded_out.at[rows, :], store_sem.at[d]))
        stores[d].start()
    for copy in [memory_copy] + stores:
        copy.wait()
    for copy, cond in pending:
        if cond is None:
            copy().wait_send()
        else:
            pl.when(cond)(lambda copy=copy: copy().wait_send())


def per_device(
    hidden_in,
    ffn_gain,
    wi_gate,
    wi_up,
    wo_down,
    final_gain,
    key_w,
    value_w,
    query_w,
    out_w,
    dec_gain,
    embed,
    lengths,
    answer_ids,
):
    sizes = tuple(lax.axis_size(a) for a in ("groups", "wide", "narrow"))
    rows_ok = hidden_in.shape[0] % 16 == 0 and lengths.shape[0] == CORES
    if sizes != (2, 2 * PLANES, CORES) or QUEST != PLANES or not rows_ok:
        return per_device_any(
            hidden_in,
            ffn_gain,
            wi_gate,
            wi_up,
            wo_down,
            final_gain,
            key_w,
            value_w,
            query_w,
            out_w,
            dec_gain,
            embed,
            lengths,
            answer_ids,
        )
    rows, features = hidden_in.shape
    slot_rows = -(-(rows // CORES) // 16) * 16
    depth = wi_gate.shape[0]
    unit = wi_gate.shape[1] // CHIPS
    head_cols = key_w.shape[1] // CHIPS
    answers = answer_ids.shape[1]
    width = features // PLANES
    half = features // 2
    bf, f32 = jnp.bfloat16, jnp.float32
    slots = CHIPS * CORES
    wing = width // 2
    dma = pltpu.SemaphoreType.DMA
    vmem = pl.BlockSpec(memory_space=pltpu.VMEM)
    hbm = pl.BlockSpec(memory_space=pl.ANY)
    loaded = (hidden_in, wi_gate, wi_up, wo_down, key_w, value_w, query_w, out_w)
    memory, decoded = pl.pallas_call(
        reader,
        out_shape=(
            jax.ShapeDtypeStruct((rows, features), bf),
            jax.ShapeDtypeStruct((QUEST * answers, half), bf),
        ),
        in_specs=[hbm, vmem, hbm, hbm, hbm, vmem, hbm, hbm, hbm, hbm, vmem, hbm]
        + [pl.BlockSpec(memory_space=pltpu.SMEM), vmem],
        out_specs=(hbm, hbm),
        scratch_shapes=[pltpu.VMEM(a.shape, bf) for a in loaded]
        + [
            pltpu.VMEM((slot_rows, features), f32),
            pltpu.VMEM((2, wi_gate.shape[1], depth), bf),
            pltpu.VMEM((PLANES, 2, 2 * unit, depth), bf),
            pltpu.VMEM((2 * unit, depth), bf),
            pltpu.VMEM((PLANES, 2, unit, depth), bf),
            pltpu.VMEM((2, PLANES, 2, 2 * depth, head_cols), bf),
            pltpu.VMEM((PLANES, 2, depth, head_cols), bf),
            pltpu.VMEM((2, PLANES, 2, head_cols, depth), bf),
            pltpu.VMEM((2 * depth, head_cols), bf),
            pltpu.VMEM((depth, head_cols), bf),
            pltpu.VMEM((head_cols, depth), bf),
            pltpu.VMEM((slots, slot_rows, features), bf),
            pltpu.VMEM((2, slots, slot_rows, unit), f32),
            pltpu.VMEM((slots, slot_rows, unit), bf),
            pltpu.VMEM((embed.shape[0], half), bf),
            pltpu.VMEM((CHIPS, slot_rows, width), f32),
            pltpu.VMEM((PLANES, CHIPS, slot_rows, width), f32),
            pltpu.VMEM((PLANES, CHIPS, slot_rows, width), f32),
            pltpu.VMEM((PLANES, 2, 2, slot_rows, wing), jnp.int16),
            pltpu.VMEM((PLANES, 2, 2, slot_rows, wing), jnp.int16),
            pltpu.VMEM((PLANES, 2, 2, slot_rows, wing), f32),
            pltpu.VMEM((PLANES, 3, slot_rows, wing), jnp.int16),
            pltpu.VMEM((PLANES, 3, slot_rows, wing), jnp.int16),
            pltpu.VMEM((PLANES, slot_rows, wing), jnp.int16),
            pltpu.VMEM((PLANES, slot_rows, wing), jnp.int16),
            pltpu.VMEM(hidden_in.shape, bf),
            pltpu.VMEM((2, answers, features), bf),
            pltpu.VMEM((2, answers, head_cols), bf),
            pltpu.VMEM((answers, head_cols), bf),
            pltpu.VMEM((2, slot_rows, features), f32),
            pltpu.VMEM((2 * CORES, slot_rows, features), bf),
            pltpu.VMEM((QUEST, answers, half), bf),
            pltpu.VMEM((QUEST, answers, half), bf),
            pltpu.VMEM((answers, half), bf),
            pltpu.VMEM((answers, half), bf),
            pltpu.VMEM((CORES, answers, half), bf),
            pltpu.VMEM((2, 8, 128), jnp.int32),
            pltpu.VMEM((features, 2 * head_cols), bf),
            pltpu.VMEM((features, 2 * head_cols), bf),
            pltpu.VMEM((features, head_cols), bf),
            pltpu.VMEM((2 * head_cols, features), bf),
            pltpu.VMEM((2 * CORES, slot_rows, 2 * head_cols), bf),
            pltpu.VMEM((2 * CORES, slot_rows, 2 * head_cols), bf),
            pltpu.VMEM((2, answers, half + 128), jnp.int16),
            pltpu.VMEM((3, answers, half + 128), jnp.int16),
            pltpu.VMEM((QUEST, answers, half), bf),
            dma((5, 2)),
            dma((PLANES, 2)),
            dma((2, 2)),
            dma((5,)),
            dma((5, 2)),
            dma((PLANES, 2)),
            dma((3, 5)),
            dma((3, PLANES)),
            dma((2, PLANES)),
            dma((2, PLANES)),
            dma((9,)),
            dma((8,)),
            dma((slots + 2,)),
            dma((PLANES,)),
            dma((PLANES,)),
            dma((PLANES, 2)),
            dma((PLANES, 2)),
            dma((PLANES, 2)),
            dma((PLANES, 2)),
            dma((PLANES,)),
            dma((PLANES,)),
            dma((PLANES + 1,)),
            dma((3,)),
            dma((3,)),
            dma((len(loaded),)),
            dma((PLANES,)),
            dma((PLANES,)),
            dma((7,)),
            dma((7,)),
            dma((3,)),
            dma((2 * CORES,)),
            dma((PLANES,)),
            dma((PLANES,)),
            dma,
        ],
        compiler_params=pltpu.CompilerParams(
            collective_id=0, has_side_effects=True, vmem_limit_bytes=62 * 2**20
        ),
    )(
        hidden_in,
        ffn_gain,
        wi_gate,
        wi_up,
        wo_down,
        final_gain,
        key_w,
        value_w,
        query_w,
        out_w,
        dec_gain,
        embed,
        lengths,
        answer_ids,
    )
    return memory, decoded


def solution(mesh):
    placed = (
        P(("groups", "wide"), None),
        P(),
        P("wide", "narrow"),
        P("wide", "narrow"),
        P("narrow", "wide"),
        P(),
        P("wide", "narrow"),
        P("wide", "narrow"),
        P("wide", "narrow"),
        P("narrow", "wide"),
        P(),
        P("wide", None),
        P(("groups", "wide")),
        P("groups", None),
    )
    return jax.shard_map(
        per_device,
        mesh=mesh,
        in_specs=placed,
        out_specs=(P(("groups", "wide"), None), P("groups", "narrow")),
        check_vma=False,
    )
```

```python
import functools
import math

import jax
import jax.numpy as jnp
from jax import lax
from jax.experimental import pallas as pl
from jax.experimental.pallas import tpu as pltpu
from jax.sharding import PartitionSpec as P

HEAD_DIM = 64
QUEST = 4


EPS = 1e-06
FLOOR = -1e30


def swap(values, axis, distance=1):
    pairs = [(i, i ^ distance) for i in range(lax.axis_size(axis))]
    return jax.tree.map(lambda a: lax.ppermute(a, axis, pairs), values)


def ordered(bit, own, other, dim):
    first = jnp.where(bit == 0, own, other)
    second = jnp.where(bit == 0, other, own)
    return jnp.concatenate([first, second], axis=dim)


def part(values, index, count, dim):
    size = values.shape[dim] // count
    return lax.dynamic_slice_in_dim(values, index * size, size, dim)


def line_gather(block, place, count):
    size = lax.axis_size("wide")
    stride = size // count
    if count > 8:
        groups = [[i * stride + j for i in range(count)] for j in range(stride)]
        return lax.all_gather(block, "wide", axis_index_groups=groups)
    up = [(i, i + stride) for i in range(size - stride)]
    down = [(i + stride, i) for i in range(size - stride)]
    below, above = [], []
    from_below = from_above = block
    for _ in range(count - 1):
        from_below = lax.ppermute(from_below, "wide", up)
        from_above = lax.ppermute(from_above, "wide", down)
        below.insert(0, from_below)
        above.append(from_above)
    return lax.dynamic_slice_in_dim(
        jnp.stack(below + [block] + above), count - 1 - place, count, 0
    )


def rms_scale(values, gain):
    mean_square = jnp.mean(values * values, axis=-1, keepdims=True)
    return values * lax.rsqrt(mean_square + EPS) * gain.astype(jnp.float32)


def add_rows(left, piece):
    return jnp.dot(left, piece, preferred_element_type=jnp.float32)


def join_partial(first, second):
    top = jnp.maximum(first[0], second[0])
    factor_first = jnp.exp(first[0] - top)
    factor_second = jnp.exp(second[0] - top)
    return (
        top,
        first[1] * factor_first + second[1] * factor_second,
        first[2] * factor_first + second[2] * factor_second,
    )


def per_device_any(
    hidden_in,
    ffn_gain,
    wi_gate,
    wi_up,
    wo_down,
    final_gain,
    key_w,
    value_w,
    query_w,
    out_w,
    dec_gain,
    embed,
    lengths,
    answer_ids,
):
    rows, features = hidden_in.shape
    wide = lax.axis_size("wide")
    group, place, core = (lax.axis_index(a) for a in ("groups", "wide", "narrow"))
    side, pair = place % 2, place // 2
    pairs = wide // 2
    quarters = 2 * lax.axis_size("groups")
    lanes = 128

    def for_side(target, pieces):
        quarter = target * (quarters // 2) + group
        return jnp.concatenate(
            [part(a, quarter, quarters, dim).reshape(-1, lanes) for a, dim in pieces]
        )

    def paired(pieces):
        own = for_side(side, pieces)
        other = swap(for_side(1 - side, pieces), "wide")
        return ordered(side, own[None], other[None], 0)

    def gathered(both):
        return line_gather(both, pair, pairs).reshape(wide, *both.shape[1:])

    hidden_units = wi_gate.shape[1] // quarters
    depth = wi_gate.shape[0]
    ffn = gathered(paired(((wi_gate.T, 0), (wi_up.T, 0), (wo_down, 0))))
    ffn = ffn.reshape(wide, 3, hidden_units, depth).transpose(1, 2, 0, 3)
    gate_t, up_t, down = ffn.reshape(3, hidden_units, features)

    def over_plane(own):
        couple = jnp.concatenate([own, swap(own, "wide")])
        return jnp.concatenate([couple, swap(couple, "groups")])

    def both_halves(own):
        return ordered(core, own, swap(own, "narrow"), 1)

    answers = answer_ids.shape[1]
    per_question = wide // QUEST
    qrows = answer_ids.shape[0] * answers
    vocab_rows = embed.shape[0]
    local_ids = answer_ids.reshape(qrows) - place * vocab_rows
    onehot = (local_ids[:, None] == jnp.arange(vocab_rows, dtype=jnp.int32)[None, :]).astype(
        jnp.bfloat16
    )
    found = jnp.dot(onehot, embed, preferred_element_type=jnp.float32).astype(jnp.bfloat16)
    found = part(found, core, 2, 1)
    distance = wide // 2
    while distance:
        if distance >= per_question:
            bit = place // distance % 2
            found = part(found, bit, 2, 0) + swap(part(found, 1 - bit, 2, 0), "wide", distance)
        else:
            found = found + swap(found, "wide", distance)
        distance //= 2
    embedded_half = found.astype(jnp.float32)
    dec_own = rms_scale(both_halves(found).astype(jnp.float32), dec_gain).astype(jnp.bfloat16)
    dec_in = jnp.concatenate([dec_own, swap(dec_own, "groups")])

    columns = key_w.shape[1] // quarters
    att_pair = paired(((key_w, 1), (value_w, 1), (query_w, 1), (out_w, 0)))
    lengths_all = over_plane(lengths)

    resid_in = hidden_in.astype(jnp.float32)
    enc_own = rms_scale(resid_in, ffn_gain).astype(jnp.bfloat16)
    enc_in = both_halves(over_plane(part(enc_own, core, 2, 1)))
    enc_in, dec_in, lengths_all, att_pair, embedded_half = lax.optimization_barrier(
        (enc_in, dec_in, lengths_all, att_pair, embedded_half)
    )
    contract_last = (((1,), (1,)), ((), ()))
    gate = lax.dot_general(enc_in, gate_t, contract_last, preferred_element_type=jnp.float32)
    up = lax.dot_general(enc_in, up_t, contract_last, preferred_element_type=jnp.float32)
    inner = (jax.nn.gelu(gate, approximate=True) * up).astype(jnp.bfloat16)
    sent_half = add_rows(inner, part(down, 1 - core, 2, 1))
    received_half = swap(sent_half, "narrow")
    sums = add_rows(inner, part(down, core, 2, 1)) + received_half

    def keep_half(values):
        return part(values, core, 2, 1) + swap(part(values, 1 - core, 2, 1), "narrow")

    blocks = sums.reshape(4, rows, -1)
    middle = blocks.shape[2] // 2
    early, late = blocks[:, :, :middle], blocks[:, :, middle:]
    early = early[:2] + swap(early[2:], "groups")
    late = late[::2] + swap(late[1::2], "wide")
    early = early[0] + swap(early[1], "wide")
    late = late[0] + swap(late[1], "groups")
    share = jnp.concatenate([early, late], axis=1)
    resid_half = part(resid_in, core, 2, 1) + share
    own_squares = jnp.sum(resid_half * resid_half, axis=1)
    squares = (own_squares + swap(own_squares, "narrow"))[:, None]
    gain_half = part(final_gain, core, 2, 0).astype(jnp.float32)
    memory_half = (resid_half * lax.rsqrt(squares / features + EPS) * gain_half).astype(
        jnp.bfloat16
    )
    memory_early, memory_late = memory_half[:, :middle], memory_half[:, middle:]
    twin = jnp.stack([memory_late, swap(memory_late, "groups")])
    late_all = jnp.stack([twin, swap(twin, "wide")], axis=1).reshape(4 * rows, middle)
    early_all = over_plane(memory_early)
    early_other, late_other = swap(early_all, "narrow"), swap(late_all, "narrow")
    other_half = jnp.concatenate([early_other[:rows], late_other[:rows]], axis=1)
    memory = ordered(core, memory_half, other_half, 1)

    att = gathered(att_pair)
    att = att.reshape(wide, 4, -1)
    key_q, value_q, query_q = (att[:, i].reshape(features, columns) for i in range(3))
    out_q = att[:, 3].reshape(wide, columns, depth).transpose(1, 0, 2).reshape(columns, features)

    def project(weight):
        own, other = part(weight, core, 2, 0), part(weight, 1 - core, 2, 0)
        return (
            add_rows(early_all, own[:middle])
            + add_rows(late_all, own[middle:])
            + add_rows(early_other, other[:middle])
            + add_rows(late_other, other[middle:])
        ).astype(jnp.bfloat16)

    heads = columns // HEAD_DIM
    keys = project(key_q).reshape(2, 2 * rows, columns)
    values = project(value_q).reshape(2, 2 * rows, columns).astype(jnp.float32)
    query = add_rows(dec_in, query_q).astype(jnp.bfloat16)
    in_head = (
        jnp.arange(columns, dtype=jnp.int32)[None, :] // HEAD_DIM
        == jnp.arange(heads, dtype=jnp.int32)[:, None]
    )[None, :, None, :]
    query_heads = jnp.where(in_head, query.reshape(2, 1, answers, columns), 0)
    scores = jnp.einsum(
        "qhac,qkc->qhak", query_heads, keys, preferred_element_type=jnp.float32
    ) * (1.0 / math.sqrt(HEAD_DIM))
    passage_len = rows // lengths.shape[0]
    live = jnp.arange(passage_len, dtype=jnp.int32)[None, :] < lengths_all[:, None]
    scores = jnp.where(live.reshape(2, 1, 1, 2 * rows), scores, FLOOR)
    top = jnp.max(scores, axis=3, keepdims=True)
    weights = jnp.exp(scores - top)
    total = jnp.sum(weights, axis=3, keepdims=True)
    acc = jnp.einsum("qhak,qkc->qhac", weights, values, precision=lax.Precision.HIGHEST)
    state = (top, total, acc)
    distance = 2
    while distance < per_question:
        state = join_partial(state, swap(state, "wide", distance))
        distance *= 2
    attended = jnp.sum(jnp.where(in_head, state[2] / state[1], 0.0), axis=1)
    attended = attended.astype(jnp.bfloat16).reshape(2 * answers, columns)
    partial_out = keep_half(jnp.dot(attended, out_q, preferred_element_type=jnp.float32))
    share_out = partial_out[:answers] + swap(partial_out[answers:], "groups")
    share_out = share_out + swap(share_out, "wide")
    decoded = (embedded_half + share_out).astype(jnp.bfloat16)
    distance = per_question
    while distance < wide:
        decoded = ordered(place // distance % 2, decoded, swap(decoded, "wide", distance), 0)
        distance *= 2
    return (memory, decoded)


MESH = pl.DeviceIdType.MESH
PLANES = 4
CHIPS = 4
CORES = 2
QUANT = 32767.0


def dot_t(left, right):
    return lax.dot_general(
        left, right, (((1,), (1,)), ((), ())), preferred_element_type=jnp.float32
    )


def reader(
    hidden_hbm,
    gain_in,
    gate_hbm,
    up_hbm,
    down_hbm,
    gain_out,
    key_hbm,
    value_hbm,
    query_hbm,
    out_hbm,
    gain_dec,
    embed,
    lengths,
    ids,
    memory_out,
    decoded_out,
    hidden,
    gate_w,
    up_w,
    down_w,
    key_w,
    value_w,
    query_w,
    out_w,
    hid,
    turned,
    gu,
    gu_side,
    dn,
    at_kv,
    at_q,
    at_o,
    side_kv,
    side_q,
    side_o,
    enc,
    acts,
    inner,
    table,
    part_own,
    part_out,
    part_in,
    share_out,
    share_in,
    kept,
    last_out,
    last_in,
    full_out,
    full_in,
    dec_rows,
    query_rows,
    query_out,
    resid,
    mem,
    found,
    found_in,
    pair_out,
    pair_in,
    half_in,
    lens_all,
    weight_k,
    weight_v,
    weight_q,
    weight_o,
    keys,
    values,
    tail_out,
    tail_in,
    dec_all,
    gu_s,
    gu_r,
    gu_half_s,
    x_r,
    dn_s,
    dn_r,
    at_s,
    at_r,
    at_ys,
    at_yr,
    at_ds,
    x_s,
    enc_s,
    enc_r,
    part_s,
    part_r,
    share_s,
    share_r,
    last_s,
    last_r,
    full_s,
    full_r,
    tail_s,
    tail_r,
    load_sem,
    emb_s,
    emb_r,
    one_s,
    one_r,
    mem_s,
    mem_r,
    dec_s,
    dec_r,
    table_sem,
):
    y, place, n = (lax.axis_index(a) for a in ("groups", "wide", "narrow"))
    z, x = place // 2, place % 2
    upper = z // 2
    w = z + upper * (PLANES - 1 - 2 * z)

    def plane(mirrored):
        return mirrored + upper * (PLANES - 1 - 2 * mirrored)

    order = [z, plane(1 - w), plane(2), plane(3)]
    slot_rows = hid.shape[0]
    unit = gu.shape[2] // 2
    head_cols = at_kv.shape[4]

    def on(x_at, y_at, z_at, n_at):
        return {"groups": y_at, "wide": z_at * 2 + x_at, "narrow": n_at}

    across = on(1 - x, y, z, n)
    aside = on(x, 1 - y, z, n)
    corner = on(1 - x, 1 - y, z, n)
    twin = on(x, y, z, 1 - n)
    across_twin = on(1 - x, y, z, 1 - n)
    next_a = on(x, y, order[1], n)
    next_b = on(x, y, plane(2), n)
    inside = w == 1
    ends = w == 0
    pending = []

    def send(source, target, send_sem, recv_sem, device, cond=None):
        def copy():
            return pltpu.make_async_remote_copy(
                source, target, send_sem, recv_sem, device_id=device, device_id_type=MESH
            )

        if cond is None:
            copy().start()
        else:
            pl.when(cond)(lambda: copy().start())
        pending.append((copy, cond))

    def arrived(target, recv_sem):
        pltpu.make_async_remote_copy(
            target, target, recv_sem, recv_sem, device_id=twin, device_id_type=MESH
        ).wait_recv()

    barrier = pltpu.get_barrier_semaphore()
    peers = [across, aside, corner, twin, across_twin]
    peers += [on(x, y, (z + d) % PLANES, n) for d in range(1, PLANES)]
    for peer in peers:
        pl.semaphore_signal(barrier, inc=1, device_id=peer, device_id_type=MESH)

    loads = [
        pltpu.make_async_copy(source, target, load_sem.at[j])
        for j, (source, target) in enumerate(
            (
                (gate_hbm, gate_w),
                (up_hbm, up_w),
                (hidden_hbm, hidden),
                (down_hbm, down_w),
                (key_hbm, key_w),
                (value_hbm, value_w),
                (query_hbm, query_w),
                (out_hbm, out_w),
            )
        )
    ]
    for copy in loads:
        copy.start()
    table_copy = pltpu.make_async_copy(
        embed.at[:, pl.ds(pl.multiple_of(n * table.shape[1], 128), table.shape[1])],
        table,
        table_sem,
    )
    table_copy.start()

    lanes = 128
    for j, array in enumerate((gate_w, up_w)):
        loads[j].wait()
        for k in range(array.shape[1] // lanes):
            cols = pl.ds(k * lanes, lanes)
            turned[j, cols, :] = array[:, cols].T
    mine = pl.multiple_of((2 * x + y) * unit, 16)
    theirs = pl.multiple_of((2 * (1 - x) + y) * unit, 16)
    for j in range(2):
        gu_side[pl.ds(j * unit, unit), :] = turned[j, pl.ds(theirs, unit), :]
        gu[z, x, pl.ds(j * unit, unit), :] = turned[j, pl.ds(mine, unit), :]
    pl.semaphore_wait(barrier, len(peers))

    def stream(buf, s_sem, r_sem, k, side):
        at_z = order[k]
        if k == 0:
            send(buf.at[at_z, side], buf.at[at_z, side], s_sem.at[0, side], r_sem.at[at_z, side], next_a)
            send(buf.at[at_z, side], buf.at[at_z, side], s_sem.at[4, side], r_sem.at[at_z, side], next_b, inside)
        else:
            target = next_b if k == 1 else next_a
            send(buf.at[at_z, side], buf.at[at_z, side], s_sem.at[k, side], r_sem.at[at_z, side], target, inside)

    streams = ((at_kv.at[0], 0), (at_q, 1), (at_o.at[0], 2))

    def att_stream(j, k, cond=None):
        buf = streams[j][0].at[order[k]]
        if k == 0:
            sem = at_s.at[j, 0]
            send(buf, buf, sem, at_r.at[j, order[0]], next_a, cond)
            if cond is not ends:
                send(buf, buf, at_s.at[j, 4], at_r.at[j, order[0]], next_b, inside)
        else:
            send(buf, buf, at_s.at[j, k], at_r.at[j, order[k]], next_b if k == 1 else next_a, inside)

    def double_stream(sem, device, cond):
        buf = at_kv.at[1, z]
        send(buf, buf, at_ds.at[sem], at_yr.at[0, z], device, cond)

    def double_pass():
        buf, sem = at_kv.at[1, order[1]], at_yr.at[0, order[1]]
        pl.when(inside)(lambda: arrived(buf, sem))
        send(buf, buf, at_ds.at[2], sem, next_b, inside)

    def att_got(j, k):
        arrived(streams[j][0].at[order[k]], at_r.at[j, order[k]])

    def att_pass(j, k):
        pl.when(inside)(lambda: att_got(j, k))
        att_stream(j, k)

    def att_end(j, k):
        pl.when(w == 0)(lambda: att_got(j, k))

    def att_side_send(j, k, cond=None):
        buf, sem = ((at_kv, 0), None, (at_o, 1))[j]
        at_z = order[k]
        send(buf.at[0, at_z], buf.at[1, at_z], at_ys.at[sem, at_z], at_yr.at[sem, at_z], aside, cond)

    def got(buf, r_sem, k, side):
        arrived(buf.at[order[k], side], r_sem.at[order[k], side])

    for j in range(2):
        rows = pl.ds(j * unit, unit)
        send(gu_side.at[rows], gu.at[z, x, rows], x_s.at[4 + j], x_r.at[j], across)
    stream(gu, gu_s, gu_r, 0, x)

    loads[2].wait()
    seg = hidden.shape[0] // CORES
    late = hidden.shape[0] - slot_rows
    low = hidden[pl.ds(0, slot_rows), :].astype(jnp.float32)
    high = hidden[pl.ds(late, slot_rows), :].astype(jnp.float32)
    skip = seg - late
    hid[...] = jnp.where(n == 0, low, jnp.concatenate([high[skip:], high[:skip]], axis=0))
    enc[n] = rms_scale(hid[...], gain_in[...][None]).astype(jnp.bfloat16)
    for j, (peer, r) in enumerate(((across, 1), (aside, 2), (twin, 0))):
        send(enc.at[n], enc.at[2 * r + n], enc_s.at[j], enc_r.at[2 * r + n], peer)
    for copy in loads[3:]:
        copy.wait()
    dn[z, x] = down_w[pl.ds(mine, unit), :]
    depth = key_w.shape[0]

    def columns_of(x_at, y_at):
        return pl.ds(pl.multiple_of((2 * x_at + y_at) * head_cols, head_cols), head_cols)

    for x_at, kv_of, q_of, o_of in (
        (x, [at_kv.at[h, z, x] for h in range(2)], at_q.at[z, x], at_o.at[0, z, x]),
        (1 - x, [side_kv.at[h] for h in range(2)], side_q, side_o),
    ):
        for h, y_at in enumerate((y, 1 - y)):
            for j, array in enumerate((key_w, value_w)):
                kv_of[h][pl.ds(j * depth, depth), :] = array[:, columns_of(x_at, y_at)]
        q_of[...] = query_w[:, columns_of(x_at, y)]
        o_of[...] = out_w[columns_of(x_at, y), :]
    tile_row = lax.broadcasted_iota(jnp.int32, lens_all.shape[1:], 0)
    lens_all[x] = jnp.where(tile_row == 0, lengths[0], lengths[1])

    send(down_w.at[pl.ds(theirs, unit), :], dn.at[z, x], x_s.at[1], dn_r.at[z, x], across)
    send(lens_all.at[x], lens_all.at[x], x_s.at[3], one_r.at[0], across)
    att_sides = (
        (side_kv.at[0], at_kv.at[0]),
        (side_q, at_q),
        (side_o, at_o.at[0]),
        (side_kv.at[1], at_kv.at[1]),
    )

    def pass_on(buf, s_sem, r_sem, k, side):
        @pl.when(inside)
        def _():
            got(buf, r_sem, k, side)

        stream(buf, s_sem, r_sem, k, side)

    def end_got(buf, r_sem, k):
        @pl.when(w == 0)
        def _():
            for side in (x, 1 - x):
                got(buf, r_sem, k, side)

    for j in range(2):
        rows = pl.ds(j * unit, unit)
        piece = gu.at[z, 1 - x, rows]
        arrived(piece, x_r.at[j])
        send(piece, piece, gu_half_s.at[j, 0], gu_r.at[z, 1 - x], next_a)
        send(piece, piece, gu_half_s.at[j, 1], gu_r.at[z, 1 - x], next_b, inside)
    for side in (x, 1 - x):
        for k in (2, 1):
            pass_on(gu, gu_s, gu_r, k, side)

    feat_half = enc.shape[2] // 2
    halves = [pl.ds(0, feat_half), pl.ds(feat_half, feat_half)]
    for j, (r, peer) in enumerate(((1, aside), (2, across))):
        arrived(enc.at[2 * r + n], enc_r.at[2 * r + n])
        send(
            enc.at[2 * r + n, :, halves[j]], enc.at[6 + n, :, halves[j]], enc_s.at[3 + j], enc_r.at[8 + j], peer
        )
    for r in (1, 2):
        send(enc.at[2 * r + n], enc.at[2 * r + n], enc_s.at[4 + r], enc_r.at[2 * r + n], twin)
    for j, (source, target) in enumerate(att_sides):
        send(source, target.at[z, x], x_s.at[6 + j], x_r.at[2 + j], across)

    pass_on(gu, gu_s, gu_r, 3, x)

    table_copy.wait()
    vocab = table.shape[0]
    total_ids = ids.shape[0] * ids.shape[1]
    all_ids = jnp.concatenate([ids[q : q + 1, :] for q in range(ids.shape[0])], axis=1)
    chunk = 1024
    hits = jnp.zeros((total_ids, table.shape[1]), jnp.float32)
    for base in range(0, vocab, chunk):
        size = min(chunk, vocab - base)
        row = lax.broadcasted_iota(jnp.int32, (size, total_ids), 0) + (place * vocab + base)
        onehot = (row == all_ids).astype(jnp.bfloat16)
        hits = hits + lax.dot_general(
            onehot,
            table[pl.ds(base, size), :],
            (((0,), (0,)), ((), ())),
            preferred_element_type=jnp.float32,
        )
    answers = found.shape[1]
    for q in range(PLANES):
        found[q] = hits[q * answers : (q + 1) * answers].astype(jnp.bfloat16)

    def gate_up(k, first_r, last_r, which=None, group=0):
        at_z = order[k]
        width = 2 * gu.shape[3]
        cols = pl.ds(pl.multiple_of(at_z * width, width), width)
        weights = [
            jnp.concatenate(
                [gu[at_z, 0, pl.ds(j * unit, unit), :], gu[at_z, 1, pl.ds(j * unit, unit), :]], axis=1
            )
            for j in range(2)
        ]

        def rows_of(first, second):
            rows = jnp.concatenate([enc[first, :, cols], enc[second, :, cols]], axis=0)
            for j in range(2):
                value = dot_t(rows, weights[j])
                for i, at_slot in enumerate((first, second)):
                    part_value = value[i * slot_rows : (i + 1) * slot_rows]
                    acts[j, at_slot] = part_value + acts[j, at_slot] if k else part_value

        def body(i, carry):
            rows_of(2 * i, 2 * i + 1)
            return carry

        if which is None:
            lax.fori_loop(first_r, last_r, body, 0)
        else:
            first, second = (1, 3) if group == 0 else (0, 2)
            rows_of(2 * first + which, 2 * second + which)

    for r in (0, 1, 2):
        arrived(enc.at[2 * r + 1 - n], enc_r.at[2 * r + 1 - n])
    gate_up(0, 0, 3)
    pass_on(gu, gu_s, gu_r, 3, 1 - x)
    for d in range(1, PLANES):
        q = (z + d) % PLANES
        send(found.at[q], found_in.at[z], emb_s.at[d], emb_r.at[z], on(x, y, q, n))
    stream(dn, dn_s, dn_r, 0, x)
    end_got(gu, gu_r, 1)
    gate_up(1, 0, 3)
    end_got(gu, gu_r, 2)
    gate_up(2, 0, 3)
    got(dn, dn_r, 0, 1 - x)
    stream(dn, dn_s, dn_r, 0, 1 - x)
    for j in range(2):
        arrived(enc.at[6 + n, :, halves[j]], enc_r.at[8 + j])
    send(enc.at[6 + n], enc.at[6 + n], enc_s.at[7], enc_r.at[6 + n], twin)
    pass_on(dn, dn_s, dn_r, 2, x)
    pass_on(dn, dn_s, dn_r, 1, x)
    arrived(enc.at[7 - n], enc_r.at[7 - n])
    for k in range(3):
        gate_up(k, 3, 4)
    pass_on(dn, dn_s, dn_r, 2, 1 - x)
    pass_on(dn, dn_s, dn_r, 1, 1 - x)
    end_got(gu, gu_r, 3)

    def exponent(top):
        return jnp.ceil(jnp.log(jnp.maximum(top, 1e-30) / QUANT) * (1.0 / math.log(2.0)) + 0.01)

    def encode(total):
        top = jnp.max(jnp.max(jnp.abs(total), axis=0, keepdims=True), axis=1, keepdims=True)
        power = exponent(top)
        coded = jnp.round(total * jnp.exp2(-power))
        row = lax.broadcasted_iota(jnp.int32, coded.shape, 0)
        return jnp.where(row < slot_rows - 8, coded, power).astype(jnp.int32).astype(jnp.int16)

    def decode(coded):
        coded = coded.astype(jnp.int32).astype(jnp.float32)
        return coded * jnp.exp2(coded[slot_rows - 8 : slot_rows - 7, 0:1])

    by_x, far, here, by_y = range(CHIPS)
    chip_at = (1, 3, 0, 2)
    wing = dn.shape[3]

    def wing_cols(at_z, j):
        return pl.ds(pl.multiple_of((at_z * 2 + j) * wing, wing), wing)

    def down_half(k, which, first=0, last=CHIPS):
        at_z = order[k]
        weights = jnp.concatenate([dn[at_z, 0], dn[at_z, 1]], axis=1)
        rows = jnp.concatenate([inner[2 * r + which] for r in chip_at[first:last]], axis=0)
        return add_rows(rows, weights).reshape(last - first, slot_rows, weights.shape[1])

    def down_send(k, first=0, last=CHIPS, sem=None):
        at_z = order[k]
        span = pl.ds(first, last - first)
        sem = at_z if sem is None else sem
        part_out[at_z, span] = down_half(k, 1 - n, first, last)
        send(
            part_out.at[at_z, span], part_in.at[at_z, span], part_s.at[sem], part_r.at[sem], twin
        )

    def down_own(k):
        part_own[k % 2] = down_half(k, n)

    def down_wing(k, j):
        at_z = order[k]
        peer, away, stay = ((across, (by_x, far), (here, by_y)), (aside, (by_y, far), (here, by_x)))[j]
        lane = pl.ds(j * wing, wing)

        def total(c):
            return part_own[k % 2, c, :, lane] + part_in[at_z, c, :, lane]

        for i, c in enumerate(away):
            share_out[at_z, j, i] = encode(total(c))
        send(share_out.at[at_z, j], share_in.at[at_z, j], share_s.at[at_z, j], share_r.at[at_z, j], peer)
        return total, stay

    def down_keep(k, j, total, stay):
        at_z = order[k]
        kept[at_z, j, 0] = total(stay[0]) + hid[:, wing_cols(at_z, j)]
        kept[at_z, j, 1] = total(stay[1])

    def down_second(k):
        at_z = order[k]
        arrived(part_in.at[at_z], part_r.at[at_z])
        for j in range(2):
            down_keep(k, j, *down_wing(k, j))

    def down_third(k):
        at_z = order[k]
        arrived(share_in.at[at_z, 0], share_r.at[at_z, 0])
        last_out[at_z, 2] = encode(kept[at_z, 0, 1] + decode(share_in[at_z, 0, 1]))
        send(last_out.at[at_z, 2], last_in.at[at_z, 2], last_s.at[at_z, 0], last_r.at[at_z, 0], aside)
        resid[0, :, wing_cols(at_z, 0)] = kept[at_z, 0, 0] + decode(share_in[at_z, 0, 0])
        arrived(share_in.at[at_z, 1], share_r.at[at_z, 1])
        pair = pl.ds(0, 2)
        for i in range(2):
            total = kept[at_z, 1, i] + decode(share_in[at_z, 1, i])
            last_out[at_z, i] = encode(total)
            resid[i, :, wing_cols(at_z, 1)] = total
        send(last_out.at[at_z, pair], last_in.at[at_z, pair], last_s.at[at_z, 1], last_r.at[at_z, 1], across)

    def down_fourth(k):
        at_z = order[k]
        arrived(last_in.at[at_z, 2], last_r.at[at_z, 0])
        cols = wing_cols(at_z, 0)
        total = resid[0, :, cols] + decode(last_in[at_z, 2])
        resid[0, :, cols] = total
        full_out[at_z] = encode(total)
        send(full_out.at[at_z], full_in.at[at_z], full_s.at[at_z], full_r.at[at_z], across)
        arrived(last_in.at[at_z, pl.ds(0, 2)], last_r.at[at_z, 1])
        cols = wing_cols(at_z, 1)
        for i in range(2):
            resid[i, :, cols] = resid[i, :, cols] + decode(last_in[at_z, 1 - i])

    def finish(which, group):
        gate_up(3, 0, 0, which, group)
        for r in chip_at[2 * group : 2 * group + 2]:
            at_slot = 2 * r + which
            inner[at_slot] = (
                jax.nn.gelu(acts[0, at_slot], approximate=True) * acts[1, at_slot]
            ).astype(jnp.bfloat16)

    for j, (_, target) in enumerate(att_sides):
        arrived(target.at[z, 1 - x], x_r.at[2 + j])
    att_side_send(2, 0)
    att_stream(0, 0, ends)
    double_stream(0, next_a, ends)
    finish(1 - n, 0)
    down_send(0, 0, 2, PLANES)
    summed = found[z].astype(jnp.float32)
    for d in range(1, PLANES):
        q = (z + d) % PLANES
        arrived(found_in.at[q], emb_r.at[q])
        summed = summed + found_in[q].astype(jnp.float32)
    pair_out[...] = summed.astype(jnp.bfloat16)
    send(pair_out, pair_in, one_s.at[1], one_r.at[1], across)
    finish(n, 0)
    part_own[0, pl.ds(0, 2)] = down_half(0, n, 0, 2)
    pass_on(dn, dn_s, dn_r, 3, x)
    finish(1 - n, 1)
    down_send(0, 2, CHIPS, PLANES + 1)
    arrived(part_in.at[z, pl.ds(0, 2)], part_r.at[PLANES])
    wing_a = down_wing(0, 0)
    finish(n, 1)
    part_own[0, pl.ds(2, 2)] = down_half(0, n, 2, CHIPS)
    pass_on(dn, dn_s, dn_r, 3, 1 - x)
    att_stream(0, 0, inside)
    for j in (2, 1):
        att_stream(j, 0, ends)
    arrived(part_in.at[z, pl.ds(2, 2)], part_r.at[PLANES + 1])
    wing_b = down_wing(0, 1)
    end_got(dn, dn_r, 1)
    down_send(1)
    down_keep(0, 0, *wing_a)
    down_keep(0, 1, *wing_b)
    arrived(pair_in, one_r.at[1])
    half = (pair_out[...].astype(jnp.float32) + pair_in[...].astype(jnp.float32)).astype(jnp.bfloat16)
    half_in[n] = half
    send(half_in.at[n], half_in.at[n], one_s.at[2], one_r.at[2], twin)
    att_pass(0, 1)
    down_own(1)
    down_second(1)
    att_pass(0, 2)
    end_got(dn, dn_r, 2)
    down_send(2)
    down_third(0)
    down_own(2)
    arrived(half_in.at[1 - n], one_r.at[2])
    embedded = jnp.concatenate([half_in[0], half_in[1]], axis=1).astype(jnp.float32)
    dec_rows[0] = rms_scale(embedded, gain_dec[...][None]).astype(jnp.bfloat16)
    send(dec_rows.at[0], dec_rows.at[1], one_s.at[5], one_r.at[5], aside)
    down_second(2)
    att_pass(0, 3)
    double_stream(3, next_a, inside)
    for j in (2, 1):
        att_stream(j, 0, inside)
    att_pass(2, 1)
    att_pass(1, 1)
    double_stream(1, next_b, inside)
    down_third(1)
    end_got(dn, dn_r, 3)
    down_send(3)
    down_fourth(0)
    down_own(3)
    down_second(3)
    att_end(0, 1)
    att_pass(2, 2)
    double_pass()
    down_third(2)
    att_pass(1, 2)
    att_end(0, 2)
    att_side_send(0, 2, ends)
    down_fourth(1)
    att_pass(1, 3)
    down_third(3)
    att_pass(2, 3)
    att_end(0, 3)
    att_side_send(0, 3, ends)
    down_fourth(2)
    down_fourth(3)
    for k in (1, 2):
        att_end(2, k)
        att_side_send(2, k)
    for k in range(1, PLANES):
        take = functools.partial(arrived, at_kv.at[1, order[k]], at_yr.at[0, order[k]])
        if k == 1:
            pl.when(ends)(take)
        else:
            take()
    for k in range(PLANES):
        for side in range(2):
            rows = pl.ds((2 * k + side) * depth, depth)
            for h in range(2):
                cols = pl.ds(h * head_cols, head_cols)
                weight_k[rows, cols] = at_kv[h, k, side, pl.ds(0, depth), :]
                weight_v[rows, cols] = at_kv[h, k, side, pl.ds(depth, depth), :]
    for k in range(PLANES):
        at_z = order[k]
        arrived(full_in.at[at_z], full_r.at[at_z])
        resid[1, :, wing_cols(at_z, 0)] = decode(full_in[at_z])
    spots = [2 * x + n, 2 * (1 - x) + n, 2 * x + 1 - n, 2 * (1 - x) + 1 - n]
    for i in range(2):
        mem[spots[i]] = rms_scale(resid[i], gain_out[...][None]).astype(jnp.bfloat16)
        send(mem.at[spots[i]], mem.at[spots[i]], mem_s.at[i], mem_r.at[spots[i]], twin)

    def project(j):
        keys[j] = add_rows(mem[j], weight_k[...]).astype(jnp.bfloat16)
        values[j] = add_rows(mem[j], weight_v[...]).astype(jnp.bfloat16)

    for k in range(1, PLANES):
        att_end(1, k)
    for k in range(PLANES):
        for side in range(2):
            weight_q[pl.ds((2 * k + side) * depth, depth), :] = at_q[k, side]
    arrived(dec_rows.at[1], one_r.at[5])
    both = dec_rows[...].reshape(2 * answers, dec_rows.shape[2])
    query_two = add_rows(both, weight_q[...]).astype(jnp.bfloat16)
    query_rows[0] = query_two[:answers]
    query_out[...] = query_two[answers:]
    send(query_out, query_rows.at[1], one_s.at[6], one_r.at[6], aside)
    att_end(2, 3)
    att_side_send(2, 3)
    project(spots[0])
    project(spots[1])
    arrived(mem.at[spots[2]], mem_r.at[spots[2]])
    first = mem[2 * x]
    second = mem[2 * x + 1]
    memory_out[pl.ds(0, late), :] = first[:late]
    first, second = first.astype(jnp.float32), second.astype(jnp.float32)
    middle = jnp.concatenate([first[late:seg], second[: slot_rows - seg]], axis=0)
    memory_out[pl.ds(late, slot_rows - late), :] = middle.astype(jnp.bfloat16)
    memory_out[pl.ds(slot_rows, late), :] = second[slot_rows - seg : seg].astype(jnp.bfloat16)
    project(spots[2])
    arrived(mem.at[spots[3]], mem_r.at[spots[3]])
    project(spots[3])
    arrived(lens_all.at[1 - x], one_r.at[0])

    arrived(query_rows.at[1], one_r.at[6])
    query = jnp.concatenate([query_rows[0], query_rows[1]], axis=1)
    columns = 2 * head_cols
    heads = columns // HEAD_DIM
    lane_head = lax.broadcasted_iota(jnp.int32, (answers, columns), 1) // HEAD_DIM
    stacked = jnp.concatenate(
        [jnp.where(lane_head == h, query.astype(jnp.float32), 0.0) for h in range(heads)], axis=0
    ).astype(jnp.bfloat16)
    tokens = 2 * CORES * slot_rows
    key_rows = keys[...].reshape(tokens, columns)
    value_rows = values[...].reshape(tokens, columns)
    scores = dot_t(stacked, key_rows) * (1.0 / math.sqrt(HEAD_DIM))
    token = lax.broadcasted_iota(jnp.int32, (1, tokens), 1)
    live = token < 0
    for j in range(2 * CORES):
        length = lens_all[j // CORES, j % CORES : j % CORES + 1, 0:1]
        live = live | ((token >= j * slot_rows) & (token < j * slot_rows + length))
    scores = jnp.where(live, scores, FLOOR)
    peak = jnp.max(scores, axis=1, keepdims=True)
    weights = jnp.exp(scores - peak)
    total = jnp.sum(weights, axis=1, keepdims=True)
    coarse = weights.astype(jnp.bfloat16)
    fine = (weights - coarse.astype(jnp.float32)).astype(jnp.bfloat16)
    mixed = (add_rows(coarse, value_rows) + add_rows(fine, value_rows)) / total
    attended = jnp.where(lane_head == 0, mixed[:answers], 0.0)
    for h in range(1, heads):
        attended = jnp.where(lane_head == h, mixed[h * answers : (h + 1) * answers], attended)
    for k in range(PLANES):
        arrived(at_o.at[1, k], at_yr.at[1, k])
        for side in range(2):
            for h in range(2):
                cols = pl.ds((2 * k + side) * depth, depth)
                weight_o[pl.ds(h * head_cols, head_cols), cols] = at_o[h, k, side]
    partial = add_rows(attended.astype(jnp.bfloat16), weight_o[...])
    half_cols = partial.shape[1] // 2
    low, high = partial[:, :half_cols], partial[:, half_cols:]

    own = jnp.where(n == 0, low, high)
    tail_out[0] = jnp.where(n == 0, high, low).astype(jnp.bfloat16)
    send(tail_out.at[0], tail_in.at[2], tail_s.at[2], tail_r.at[2], across_twin)
    send(tail_out.at[0], tail_in.at[0], tail_s.at[0], tail_r.at[0], twin)
    tail_out[1] = own.astype(jnp.bfloat16)
    send(tail_out.at[1], tail_in.at[1], tail_s.at[1], tail_r.at[1], across)
    total = half_in[n].astype(jnp.float32) + own
    for j in range(3):
        arrived(tail_in.at[j], tail_r.at[j])
        total = total + tail_in[j].astype(jnp.float32)
    dec_all[z] = total.astype(jnp.bfloat16)
    for d in range(PLANES - 1, 0, -1):
        send(dec_all.at[z], dec_all.at[z], dec_s.at[d], dec_r.at[z], on(x, y, order[d], n))
    for d in range(PLANES):
        q = order[d]
        if d:
            arrived(dec_all.at[q], dec_r.at[q])
        decoded_out[pl.ds(pl.multiple_of(q * answers, answers), answers), :] = dec_all[q]
    for copy, cond in pending:
        if cond is None:
            copy().wait_send()
        else:
            pl.when(cond)(lambda copy=copy: copy().wait_send())


def hand_over(memory, decoded, memory_out, decoded_out, sems):
    copies = [
        pltpu.make_async_copy(source, target, sems.at[j])
        for j, (source, target) in enumerate(((memory, memory_out), (decoded, decoded_out)))
    ]
    for copy in copies:
        copy.start()
    for copy in copies:
        copy.wait()


def per_device(
    hidden_in,
    ffn_gain,
    wi_gate,
    wi_up,
    wo_down,
    final_gain,
    key_w,
    value_w,
    query_w,
    out_w,
    dec_gain,
    embed,
    lengths,
    answer_ids,
):
    sizes = tuple(lax.axis_size(a) for a in ("groups", "wide", "narrow"))
    rows_ok = hidden_in.shape[0] % 16 == 0 and lengths.shape[0] == CORES
    if sizes != (2, 2 * PLANES, CORES) or QUEST != PLANES or not rows_ok:
        return per_device_any(
            hidden_in,
            ffn_gain,
            wi_gate,
            wi_up,
            wo_down,
            final_gain,
            key_w,
            value_w,
            query_w,
            out_w,
            dec_gain,
            embed,
            lengths,
            answer_ids,
        )
    rows, features = hidden_in.shape
    slot_rows = -(-(rows // CORES) // 16) * 16
    depth = wi_gate.shape[0]
    unit = wi_gate.shape[1] // CHIPS
    head_cols = key_w.shape[1] // CHIPS
    answers = answer_ids.shape[1]
    width = features // PLANES
    half = features // 2
    bf, f32 = jnp.bfloat16, jnp.float32
    slots = CHIPS * CORES
    wing = width // 2
    dma = pltpu.SemaphoreType.DMA
    vmem = pl.BlockSpec(memory_space=pltpu.VMEM)
    hbm = pl.BlockSpec(memory_space=pl.ANY)
    loaded = (hidden_in, wi_gate, wi_up, wo_down, key_w, value_w, query_w, out_w)
    memory, decoded = pl.pallas_call(
        reader,
        out_shape=(
            pltpu.VMEM((rows, features), bf),
            pltpu.VMEM((QUEST * answers, half), bf),
        ),
        in_specs=[hbm, vmem, hbm, hbm, hbm, vmem, hbm, hbm, hbm, hbm, vmem, hbm]
        + [pl.BlockSpec(memory_space=pltpu.SMEM), vmem],
        out_specs=(vmem, vmem),
        scratch_shapes=[pltpu.VMEM(a.shape, bf) for a in loaded]
        + [
            pltpu.VMEM((slot_rows, features), f32),
            pltpu.VMEM((2, wi_gate.shape[1], depth), bf),
            pltpu.VMEM((PLANES, 2, 2 * unit, depth), bf),
            pltpu.VMEM((2 * unit, depth), bf),
            pltpu.VMEM((PLANES, 2, unit, depth), bf),
            pltpu.VMEM((2, PLANES, 2, 2 * depth, head_cols), bf),
            pltpu.VMEM((PLANES, 2, depth, head_cols), bf),
            pltpu.VMEM((2, PLANES, 2, head_cols, depth), bf),
            pltpu.VMEM((2, 2 * depth, head_cols), bf),
            pltpu.VMEM((depth, head_cols), bf),
            pltpu.VMEM((head_cols, depth), bf),
            pltpu.VMEM((slots, slot_rows, features), bf),
            pltpu.VMEM((2, slots, slot_rows, unit), f32),
            pltpu.VMEM((slots, slot_rows, unit), bf),
            pltpu.VMEM((embed.shape[0], half), bf),
            pltpu.VMEM((2, CHIPS, slot_rows, width), f32),
            pltpu.VMEM((PLANES, CHIPS, slot_rows, width), f32),
            pltpu.VMEM((PLANES, CHIPS, slot_rows, width), f32),
            pltpu.VMEM((PLANES, 2, 2, slot_rows, wing), jnp.int16),
            pltpu.VMEM((PLANES, 2, 2, slot_rows, wing), jnp.int16),
            pltpu.VMEM((PLANES, 2, 2, slot_rows, wing), f32),
            pltpu.VMEM((PLANES, 3, slot_rows, wing), jnp.int16),
            pltpu.VMEM((PLANES, 3, slot_rows, wing), jnp.int16),
            pltpu.VMEM((PLANES, slot_rows, wing), jnp.int16),
            pltpu.VMEM((PLANES, slot_rows, wing), jnp.int16),
            pltpu.VMEM((2, answers, features), bf),
            pltpu.VMEM((2, answers, head_cols), bf),
            pltpu.VMEM((answers, head_cols), bf),
            pltpu.VMEM((2, slot_rows, features), f32),
            pltpu.VMEM((2 * CORES, slot_rows, features), bf),
            pltpu.VMEM((QUEST, answers, half), bf),
            pltpu.VMEM((QUEST, answers, half), bf),
            pltpu.VMEM((answers, half), bf),
            pltpu.VMEM((answers, half), bf),
            pltpu.VMEM((CORES, answers, half), bf),
            pltpu.VMEM((2, 8, 128), jnp.int32),
            pltpu.VMEM((features, 2 * head_cols), bf),
            pltpu.VMEM((features, 2 * head_cols), bf),
            pltpu.VMEM((features, head_cols), bf),
            pltpu.VMEM((2 * head_cols, features), bf),
            pltpu.VMEM((2 * CORES, slot_rows, 2 * head_cols), bf),
            pltpu.VMEM((2 * CORES, slot_rows, 2 * head_cols), bf),
            pltpu.VMEM((2, answers, half), bf),
            pltpu.VMEM((3, answers, half), bf),
            pltpu.VMEM((QUEST, answers, half), bf),
            dma((5, 2)),
            dma((PLANES, 2)),
            dma((2, 2)),
            dma((6,)),
            dma((5, 2)),
            dma((PLANES, 2)),
            dma((3, 5)),
            dma((3, PLANES)),
            dma((2, PLANES)),
            dma((2, PLANES)),
            dma((4,)),
            dma((10,)),
            dma((8,)),
            dma((slots + 2,)),
            dma((PLANES + 2,)),
            dma((PLANES + 2,)),
            dma((PLANES, 2)),
            dma((PLANES, 2)),
            dma((PLANES, 2)),
            dma((PLANES, 2)),
            dma((PLANES,)),
            dma((PLANES,)),
            dma((3,)),
            dma((3,)),
            dma((len(loaded),)),
            dma((PLANES,)),
            dma((PLANES,)),
            dma((7,)),
            dma((7,)),
            dma((3,)),
            dma((2 * CORES,)),
            dma((PLANES,)),
            dma((PLANES,)),
            dma,
        ],
        compiler_params=pltpu.CompilerParams(
            collective_id=0, has_side_effects=True, vmem_limit_bytes=54 * 2**20
        ),
    )(
        hidden_in,
        ffn_gain,
        wi_gate,
        wi_up,
        wo_down,
        final_gain,
        key_w,
        value_w,
        query_w,
        out_w,
        dec_gain,
        embed,
        lengths,
        answer_ids,
    )
    shapes = [jax.ShapeDtypeStruct(a.shape, bf) for a in (memory, decoded)]
    return pl.pallas_call(
        hand_over,
        out_shape=shapes,
        in_specs=[vmem, vmem],
        out_specs=[hbm, hbm],
        scratch_shapes=[dma((2,))],
        compiler_params=pltpu.CompilerParams(vmem_limit_bytes=2**20),
    )(memory, decoded)


def solution(mesh):
    placed = (
        P(("groups", "wide"), None),
        P(),
        P("wide", "narrow"),
        P("wide", "narrow"),
        P("narrow", "wide"),
        P(),
        P("wide", "narrow"),
        P("wide", "narrow"),
        P("wide", "narrow"),
        P("narrow", "wide"),
        P(),
        P("wide", None),
        P(("groups", "wide")),
        P("groups", None),
    )
    return jax.shard_map(
        per_device,
        mesh=mesh,
        in_specs=placed,
        out_specs=(P(("groups", "wide"), None), P("groups", "narrow")),
        check_vma=False,
    )
```

```python
import functools
import math

import jax
import jax.numpy as jnp
from jax import lax
from jax.experimental import pallas as pl
from jax.experimental.pallas import tpu as pltpu
from jax.sharding import PartitionSpec as P

HEAD_DIM = 64
QUEST = 4


EPS = 1e-06
FLOOR = -1e30


def swap(values, axis, distance=1):
    pairs = [(i, i ^ distance) for i in range(lax.axis_size(axis))]
    return jax.tree.map(lambda a: lax.ppermute(a, axis, pairs), values)


def ordered(bit, own, other, dim):
    first = jnp.where(bit == 0, own, other)
    second = jnp.where(bit == 0, other, own)
    return jnp.concatenate([first, second], axis=dim)


def part(values, index, count, dim):
    size = values.shape[dim] // count
    return lax.dynamic_slice_in_dim(values, index * size, size, dim)


def line_gather(block, place, count):
    size = lax.axis_size("wide")
    stride = size // count
    if count > 8:
        groups = [[i * stride + j for i in range(count)] for j in range(stride)]
        return lax.all_gather(block, "wide", axis_index_groups=groups)
    up = [(i, i + stride) for i in range(size - stride)]
    down = [(i + stride, i) for i in range(size - stride)]
    below, above = [], []
    from_below = from_above = block
    for _ in range(count - 1):
        from_below = lax.ppermute(from_below, "wide", up)
        from_above = lax.ppermute(from_above, "wide", down)
        below.insert(0, from_below)
        above.append(from_above)
    return lax.dynamic_slice_in_dim(
        jnp.stack(below + [block] + above), count - 1 - place, count, 0
    )


def rms_scale(values, gain):
    mean_square = jnp.mean(values * values, axis=-1, keepdims=True)
    return values * lax.rsqrt(mean_square + EPS) * gain.astype(jnp.float32)


def add_rows(left, piece):
    return jnp.dot(left, piece, preferred_element_type=jnp.float32)


def join_partial(first, second):
    top = jnp.maximum(first[0], second[0])
    factor_first = jnp.exp(first[0] - top)
    factor_second = jnp.exp(second[0] - top)
    return (
        top,
        first[1] * factor_first + second[1] * factor_second,
        first[2] * factor_first + second[2] * factor_second,
    )


def per_device_any(
    hidden_in,
    ffn_gain,
    wi_gate,
    wi_up,
    wo_down,
    final_gain,
    key_w,
    value_w,
    query_w,
    out_w,
    dec_gain,
    embed,
    lengths,
    answer_ids,
):
    rows, features = hidden_in.shape
    wide = lax.axis_size("wide")
    group, place, core = (lax.axis_index(a) for a in ("groups", "wide", "narrow"))
    side, pair = place % 2, place // 2
    pairs = wide // 2
    quarters = 2 * lax.axis_size("groups")
    lanes = 128

    def for_side(target, pieces):
        quarter = target * (quarters // 2) + group
        return jnp.concatenate(
            [part(a, quarter, quarters, dim).reshape(-1, lanes) for a, dim in pieces]
        )

    def paired(pieces):
        own = for_side(side, pieces)
        other = swap(for_side(1 - side, pieces), "wide")
        return ordered(side, own[None], other[None], 0)

    def gathered(both):
        return line_gather(both, pair, pairs).reshape(wide, *both.shape[1:])

    hidden_units = wi_gate.shape[1] // quarters
    depth = wi_gate.shape[0]
    ffn = gathered(paired(((wi_gate.T, 0), (wi_up.T, 0), (wo_down, 0))))
    ffn = ffn.reshape(wide, 3, hidden_units, depth).transpose(1, 2, 0, 3)
    gate_t, up_t, down = ffn.reshape(3, hidden_units, features)

    def over_plane(own):
        couple = jnp.concatenate([own, swap(own, "wide")])
        return jnp.concatenate([couple, swap(couple, "groups")])

    def both_halves(own):
        return ordered(core, own, swap(own, "narrow"), 1)

    answers = answer_ids.shape[1]
    per_question = wide // QUEST
    qrows = answer_ids.shape[0] * answers
    vocab_rows = embed.shape[0]
    local_ids = answer_ids.reshape(qrows) - place * vocab_rows
    onehot = (local_ids[:, None] == jnp.arange(vocab_rows, dtype=jnp.int32)[None, :]).astype(
        jnp.bfloat16
    )
    found = jnp.dot(onehot, embed, preferred_element_type=jnp.float32).astype(jnp.bfloat16)
    found = part(found, core, 2, 1)
    distance = wide // 2
    while distance:
        if distance >= per_question:
            bit = place // distance % 2
            found = part(found, bit, 2, 0) + swap(part(found, 1 - bit, 2, 0), "wide", distance)
        else:
            found = found + swap(found, "wide", distance)
        distance //= 2
    embedded_half = found.astype(jnp.float32)
    dec_own = rms_scale(both_halves(found).astype(jnp.float32), dec_gain).astype(jnp.bfloat16)
    dec_in = jnp.concatenate([dec_own, swap(dec_own, "groups")])

    columns = key_w.shape[1] // quarters
    att_pair = paired(((key_w, 1), (value_w, 1), (query_w, 1), (out_w, 0)))
    lengths_all = over_plane(lengths)

    resid_in = hidden_in.astype(jnp.float32)
    enc_own = rms_scale(resid_in, ffn_gain).astype(jnp.bfloat16)
    enc_in = both_halves(over_plane(part(enc_own, core, 2, 1)))
    enc_in, dec_in, lengths_all, att_pair, embedded_half = lax.optimization_barrier(
        (enc_in, dec_in, lengths_all, att_pair, embedded_half)
    )
    contract_last = (((1,), (1,)), ((), ()))
    gate = lax.dot_general(enc_in, gate_t, contract_last, preferred_element_type=jnp.float32)
    up = lax.dot_general(enc_in, up_t, contract_last, preferred_element_type=jnp.float32)
    inner = (jax.nn.gelu(gate, approximate=True) * up).astype(jnp.bfloat16)
    sent_half = add_rows(inner, part(down, 1 - core, 2, 1))
    received_half = swap(sent_half, "narrow")
    sums = add_rows(inner, part(down, core, 2, 1)) + received_half

    def keep_half(values):
        return part(values, core, 2, 1) + swap(part(values, 1 - core, 2, 1), "narrow")

    blocks = sums.reshape(4, rows, -1)
    middle = blocks.shape[2] // 2
    early, late = blocks[:, :, :middle], blocks[:, :, middle:]
    early = early[:2] + swap(early[2:], "groups")
    late = late[::2] + swap(late[1::2], "wide")
    early = early[0] + swap(early[1], "wide")
    late = late[0] + swap(late[1], "groups")
    share = jnp.concatenate([early, late], axis=1)
    resid_half = part(resid_in, core, 2, 1) + share
    own_squares = jnp.sum(resid_half * resid_half, axis=1)
    squares = (own_squares + swap(own_squares, "narrow"))[:, None]
    gain_half = part(final_gain, core, 2, 0).astype(jnp.float32)
    memory_half = (resid_half * lax.rsqrt(squares / features + EPS) * gain_half).astype(
        jnp.bfloat16
    )
    memory_early, memory_late = memory_half[:, :middle], memory_half[:, middle:]
    twin = jnp.stack([memory_late, swap(memory_late, "groups")])
    late_all = jnp.stack([twin, swap(twin, "wide")], axis=1).reshape(4 * rows, middle)
    early_all = over_plane(memory_early)
    early_other, late_other = swap(early_all, "narrow"), swap(late_all, "narrow")
    other_half = jnp.concatenate([early_other[:rows], late_other[:rows]], axis=1)
    memory = ordered(core, memory_half, other_half, 1)

    att = gathered(att_pair)
    att = att.reshape(wide, 4, -1)
    key_q, value_q, query_q = (att[:, i].reshape(features, columns) for i in range(3))
    out_q = att[:, 3].reshape(wide, columns, depth).transpose(1, 0, 2).reshape(columns, features)

    def project(weight):
        own, other = part(weight, core, 2, 0), part(weight, 1 - core, 2, 0)
        return (
            add_rows(early_all, own[:middle])
            + add_rows(late_all, own[middle:])
            + add_rows(early_other, other[:middle])
            + add_rows(late_other, other[middle:])
        ).astype(jnp.bfloat16)

    heads = columns // HEAD_DIM
    keys = project(key_q).reshape(2, 2 * rows, columns)
    values = project(value_q).reshape(2, 2 * rows, columns).astype(jnp.float32)
    query = add_rows(dec_in, query_q).astype(jnp.bfloat16)
    in_head = (
        jnp.arange(columns, dtype=jnp.int32)[None, :] // HEAD_DIM
        == jnp.arange(heads, dtype=jnp.int32)[:, None]
    )[None, :, None, :]
    query_heads = jnp.where(in_head, query.reshape(2, 1, answers, columns), 0)
    scores = jnp.einsum(
        "qhac,qkc->qhak", query_heads, keys, preferred_element_type=jnp.float32
    ) * (1.0 / math.sqrt(HEAD_DIM))
    passage_len = rows // lengths.shape[0]
    live = jnp.arange(passage_len, dtype=jnp.int32)[None, :] < lengths_all[:, None]
    scores = jnp.where(live.reshape(2, 1, 1, 2 * rows), scores, FLOOR)
    top = jnp.max(scores, axis=3, keepdims=True)
    weights = jnp.exp(scores - top)
    total = jnp.sum(weights, axis=3, keepdims=True)
    acc = jnp.einsum("qhak,qkc->qhac", weights, values, precision=lax.Precision.HIGHEST)
    state = (top, total, acc)
    distance = 2
    while distance < per_question:
        state = join_partial(state, swap(state, "wide", distance))
        distance *= 2
    attended = jnp.sum(jnp.where(in_head, state[2] / state[1], 0.0), axis=1)
    attended = attended.astype(jnp.bfloat16).reshape(2 * answers, columns)
    partial_out = keep_half(jnp.dot(attended, out_q, preferred_element_type=jnp.float32))
    share_out = partial_out[:answers] + swap(partial_out[answers:], "groups")
    share_out = share_out + swap(share_out, "wide")
    decoded = (embedded_half + share_out).astype(jnp.bfloat16)
    distance = per_question
    while distance < wide:
        decoded = ordered(place // distance % 2, decoded, swap(decoded, "wide", distance), 0)
        distance *= 2
    return (memory, decoded)


MESH = pl.DeviceIdType.MESH
PLANES = 4
CHIPS = 4
CORES = 2
QUANT = 32767.0


def dot_t(left, right):
    return lax.dot_general(
        left, right, (((1,), (1,)), ((), ())), preferred_element_type=jnp.float32
    )


def reader(
    hidden_hbm,
    gain_in,
    gate_hbm,
    up_hbm,
    down_hbm,
    gain_out,
    key_hbm,
    value_hbm,
    query_hbm,
    out_hbm,
    gain_dec,
    embed,
    lengths,
    ids,
    memory_out,
    decoded_out,
    hidden,
    gate_w,
    up_w,
    down_w,
    key_w,
    value_w,
    query_w,
    out_w,
    hid,
    turned,
    gu,
    gu_side,
    dn,
    at_kv,
    at_q,
    at_o,
    side_kv,
    side_q,
    side_o,
    enc,
    acts,
    inner,
    table,
    part_own,
    part_out,
    part_in,
    share_out,
    share_in,
    kept,
    last_out,
    last_in,
    full_out,
    full_in,
    dec_rows,
    query_rows,
    query_out,
    query_end,
    query_back,
    dec_end,
    resid,
    mem,
    found,
    found_in,
    pair_out,
    pair_in,
    half_in,
    lens_all,
    weight_k,
    weight_v,
    weight_q,
    weight_o,
    keys,
    values,
    tail_out,
    tail_in,
    dec_all,
    send_sem,
    gu_r,
    x_r,
    dn_r,
    at_r,
    at_yr,
    enc_r,
    part_r,
    share_r,
    last_r,
    full_r,
    tail_r,
    load_sem,
    emb_r,
    one_r,
    mem_r,
    dec_r,
    table_sem,
):
    y, place, n = (lax.axis_index(a) for a in ("groups", "wide", "narrow"))
    z, x = place // 2, place % 2
    upper = z // 2
    w = z + upper * (PLANES - 1 - 2 * z)

    def plane(mirrored):
        return mirrored + upper * (PLANES - 1 - 2 * mirrored)

    order = [z, plane(1 - w), plane(2), plane(3)]
    slot_rows = hid.shape[0]
    unit = gu.shape[2] // 2
    head_cols = at_kv.shape[4]

    def on(x_at, y_at, z_at, n_at):
        return {"groups": y_at, "wide": z_at * 2 + x_at, "narrow": n_at}

    across = on(1 - x, y, z, n)
    aside = on(x, 1 - y, z, n)
    corner = on(1 - x, 1 - y, z, n)
    twin = on(x, y, z, 1 - n)
    across_twin = on(1 - x, y, z, 1 - n)
    next_a = on(x, y, order[1], n)
    next_b = on(x, y, plane(2), n)
    inside = w == 1
    ends = w == 0
    pending = []

    def settle(entry):
        copy, cond = entry
        if cond is None:
            copy().wait_send()
        else:
            pl.when(cond)(lambda: copy().wait_send())

    def send(source, target, recv_sem, device, cond=None):
        sem = send_sem.at[len(pending) % send_sem.shape[0]]
        if len(pending) >= send_sem.shape[0]:
            settle(pending[-send_sem.shape[0]])

        def copy():
            return pltpu.make_async_remote_copy(
                source, target, sem, recv_sem, device_id=device, device_id_type=MESH
            )

        if cond is None:
            copy().start()
        else:
            pl.when(cond)(lambda: copy().start())
        pending.append((copy, cond))

    def arrived(target, recv_sem):
        pltpu.make_async_remote_copy(
            target, target, recv_sem, recv_sem, device_id=twin, device_id_type=MESH
        ).wait_recv()

    barrier = pltpu.get_barrier_semaphore()
    peers = [across, aside, corner, twin, across_twin]
    peers += [on(x, y, (z + d) % PLANES, n) for d in range(1, PLANES)]
    for peer in peers:
        pl.semaphore_signal(barrier, inc=1, device_id=peer, device_id_type=MESH)

    loads = [
        pltpu.make_async_copy(source, target, load_sem.at[j])
        for j, (source, target) in enumerate(
            (
                (gate_hbm, gate_w),
                (up_hbm, up_w),
                (hidden_hbm, hidden),
                (down_hbm, down_w),
                (key_hbm, key_w),
                (value_hbm, value_w),
                (query_hbm, query_w),
                (out_hbm, out_w),
            )
        )
    ]
    for copy in loads:
        copy.start()
    table_copy = pltpu.make_async_copy(
        embed.at[:, pl.ds(pl.multiple_of(n * table.shape[1], 128), table.shape[1])],
        table,
        table_sem,
    )
    table_copy.start()

    lanes = 128
    for j, array in enumerate((gate_w, up_w)):
        loads[j].wait()
        for k in range(array.shape[1] // lanes):
            cols = pl.ds(k * lanes, lanes)
            turned[j, cols, :] = array[:, cols].T
    mine = pl.multiple_of((2 * x + y) * unit, 16)
    theirs = pl.multiple_of((2 * (1 - x) + y) * unit, 16)
    for j in range(2):
        gu_side[pl.ds(j * unit, unit), :] = turned[j, pl.ds(theirs, unit), :]
        gu[z, x, pl.ds(j * unit, unit), :] = turned[j, pl.ds(mine, unit), :]
    pl.semaphore_wait(barrier, len(peers))

    def stream(buf, r_sem, k, side):
        at_z = order[k]
        if k == 0:
            send(buf.at[at_z, side], buf.at[at_z, side], r_sem.at[at_z, side], next_a)
            send(buf.at[at_z, side], buf.at[at_z, side], r_sem.at[at_z, side], next_b, inside)
        else:
            target = next_b if k == 1 else next_a
            send(buf.at[at_z, side], buf.at[at_z, side], r_sem.at[at_z, side], target, inside)

    streams = ((at_kv.at[0], 0), (at_q, 1), (at_o.at[0], 2))

    def att_stream(j, k, cond=None):
        buf = streams[j][0].at[order[k]]
        if k == 0:
            send(buf, buf, at_r.at[j, order[0]], next_a, cond)
            if cond is not ends:
                send(buf, buf, at_r.at[j, order[0]], next_b, inside)
        else:
            send(buf, buf, at_r.at[j, order[k]], next_b if k == 1 else next_a, inside)

    def double_stream(device, cond):
        buf = at_kv.at[1, z]
        send(buf, buf, at_yr.at[0, z], device, cond)

    def double_pass():
        buf, sem = at_kv.at[1, order[1]], at_yr.at[0, order[1]]
        pl.when(inside)(lambda: arrived(buf, sem))
        send(buf, buf, sem, next_b, inside)

    def att_got(j, k):
        arrived(streams[j][0].at[order[k]], at_r.at[j, order[k]])

    def att_pass(j, k):
        pl.when(inside)(lambda: att_got(j, k))
        att_stream(j, k)

    def att_end(j, k):
        pl.when(w == 0)(lambda: att_got(j, k))

    def att_side_send(j, k, cond=None):
        buf, sem = ((at_kv, 0), None, (at_o, 1))[j]
        at_z = order[k]
        send(buf.at[0, at_z], buf.at[1, at_z], at_yr.at[sem, at_z], aside, cond)

    def got(buf, r_sem, k, side):
        arrived(buf.at[order[k], side], r_sem.at[order[k], side])

    for j in range(2):
        rows = pl.ds(j * unit, unit)
        send(gu_side.at[rows], gu.at[z, x, rows], x_r.at[j], across)
    stream(gu, gu_r, 0, x)

    loads[2].wait()
    seg = hidden.shape[0] // CORES
    late = hidden.shape[0] - slot_rows
    low = hidden[pl.ds(0, slot_rows), :].astype(jnp.float32)
    high = hidden[pl.ds(late, slot_rows), :].astype(jnp.float32)
    skip = seg - late
    hid[...] = jnp.where(n == 0, low, jnp.concatenate([high[skip:], high[:skip]], axis=0))
    enc[n] = rms_scale(hid[...], gain_in[...][None]).astype(jnp.bfloat16)
    for j, (peer, r) in enumerate(((across, 1), (aside, 2), (twin, 0))):
        send(enc.at[n], enc.at[2 * r + n], enc_r.at[2 * r + n], peer)
    for copy in loads[3:]:
        copy.wait()
    dn[z, x] = down_w[pl.ds(mine, unit), :]
    depth = key_w.shape[0]

    def columns_of(x_at, y_at):
        return pl.ds(pl.multiple_of((2 * x_at + y_at) * head_cols, head_cols), head_cols)

    for x_at, kv_of, q_of, o_of in (
        (x, [at_kv.at[h, z, x] for h in range(2)], at_q.at[z, x], at_o.at[0, z, x]),
        (1 - x, [side_kv.at[h] for h in range(2)], side_q, side_o),
    ):
        for h, y_at in enumerate((y, 1 - y)):
            for j, array in enumerate((key_w, value_w)):
                kv_of[h][pl.ds(j * depth, depth), :] = array[:, columns_of(x_at, y_at)]
        q_of[...] = query_w[:, columns_of(x_at, y)]
        o_of[...] = out_w[columns_of(x_at, y), :]
    tile_row = lax.broadcasted_iota(jnp.int32, lens_all.shape[1:], 0)
    lens_all[x] = jnp.where(tile_row == 0, lengths[0], lengths[1])

    send(down_w.at[pl.ds(theirs, unit), :], dn.at[z, x], dn_r.at[z, x], across)
    send(lens_all.at[x], lens_all.at[x], one_r.at[0], across)
    att_sides = (
        (side_kv.at[0], at_kv.at[0]),
        (side_q, at_q),
        (side_o, at_o.at[0]),
        (side_kv.at[1], at_kv.at[1]),
    )

    def pass_on(buf, r_sem, k, side):
        @pl.when(inside)
        def _():
            got(buf, r_sem, k, side)

        stream(buf, r_sem, k, side)

    def end_got(buf, r_sem, k):
        @pl.when(w == 0)
        def _():
            for side in (x, 1 - x):
                got(buf, r_sem, k, side)

    for j in range(2):
        rows = pl.ds(j * unit, unit)
        piece = gu.at[z, 1 - x, rows]
        arrived(piece, x_r.at[j])
        send(piece, piece, gu_r.at[z, 1 - x], next_a)
        send(piece, piece, gu_r.at[z, 1 - x], next_b, inside)
    for side in (x, 1 - x):
        for k in (2, 1):
            pass_on(gu, gu_r, k, side)

    feat_half = enc.shape[2] // 2
    halves = [pl.ds(0, feat_half), pl.ds(feat_half, feat_half)]
    for j, (r, peer) in enumerate(((1, aside), (2, across))):
        arrived(enc.at[2 * r + n], enc_r.at[2 * r + n])
        send(enc.at[2 * r + n, :, halves[j]], enc.at[6 + n, :, halves[j]], enc_r.at[8 + j], peer)
    for r in (1, 2):
        send(enc.at[2 * r + n], enc.at[2 * r + n], enc_r.at[2 * r + n], twin)
    for j, (source, target) in enumerate(att_sides):
        send(source, target.at[z, x], x_r.at[2 + j], across)

    pass_on(gu, gu_r, 3, x)

    table_copy.wait()
    vocab = table.shape[0]
    total_ids = ids.shape[0] * ids.shape[1]
    all_ids = jnp.concatenate([ids[q : q + 1, :] for q in range(ids.shape[0])], axis=1)
    chunk = 1024
    hits = jnp.zeros((total_ids, table.shape[1]), jnp.float32)
    for base in range(0, vocab, chunk):
        size = min(chunk, vocab - base)
        row = lax.broadcasted_iota(jnp.int32, (size, total_ids), 0) + (place * vocab + base)
        onehot = (row == all_ids).astype(jnp.bfloat16)
        hits = hits + lax.dot_general(
            onehot,
            table[pl.ds(base, size), :],
            (((0,), (0,)), ((), ())),
            preferred_element_type=jnp.float32,
        )
    answers = found.shape[1]
    for q in range(PLANES):
        found[q] = hits[q * answers : (q + 1) * answers].astype(jnp.bfloat16)

    def gate_up(k, first_r, last_r, which=None, group=0):
        at_z = order[k]
        width = 2 * gu.shape[3]
        cols = pl.ds(pl.multiple_of(at_z * width, width), width)
        weights = [
            jnp.concatenate(
                [gu[at_z, 0, pl.ds(j * unit, unit), :], gu[at_z, 1, pl.ds(j * unit, unit), :]], axis=1
            )
            for j in range(2)
        ]

        def rows_of(first, second):
            rows = jnp.concatenate([enc[first, :, cols], enc[second, :, cols]], axis=0)
            for j in range(2):
                value = dot_t(rows, weights[j])
                for i, at_slot in enumerate((first, second)):
                    part_value = value[i * slot_rows : (i + 1) * slot_rows]
                    acts[j, at_slot] = part_value + acts[j, at_slot] if k else part_value

        def body(i, carry):
            rows_of(2 * i, 2 * i + 1)
            return carry

        if which is None:
            lax.fori_loop(first_r, last_r, body, 0)
        else:
            first, second = (1, 3) if group == 0 else (0, 2)
            rows_of(2 * first + which, 2 * second + which)

    for r in (0, 1, 2):
        arrived(enc.at[2 * r + 1 - n], enc_r.at[2 * r + 1 - n])
    gate_up(0, 0, 3)
    pass_on(gu, gu_r, 3, 1 - x)
    for d in range(1, PLANES):
        q = (z + d) % PLANES
        send(found.at[q], found_in.at[z], emb_r.at[z], on(x, y, q, n))
    stream(dn, dn_r, 0, x)
    end_got(gu, gu_r, 1)
    gate_up(1, 0, 3)
    end_got(gu, gu_r, 2)
    gate_up(2, 0, 3)
    got(dn, dn_r, 0, 1 - x)
    stream(dn, dn_r, 0, 1 - x)
    for j in range(2):
        arrived(enc.at[6 + n, :, halves[j]], enc_r.at[8 + j])
    send(enc.at[6 + n], enc.at[6 + n], enc_r.at[6 + n], twin)
    pass_on(dn, dn_r, 2, x)
    pass_on(dn, dn_r, 1, x)
    arrived(enc.at[7 - n], enc_r.at[7 - n])
    for k in range(3):
        gate_up(k, 3, 4)
    pass_on(dn, dn_r, 2, 1 - x)
    pass_on(dn, dn_r, 1, 1 - x)
    end_got(gu, gu_r, 3)

    def exponent(top):
        return jnp.ceil(jnp.log(jnp.maximum(top, 1e-30) / QUANT) * (1.0 / math.log(2.0)) + 0.01)

    def encode(total):
        top = jnp.max(jnp.max(jnp.abs(total), axis=0, keepdims=True), axis=1, keepdims=True)
        power = exponent(top)
        coded = jnp.round(total * jnp.exp2(-power))
        row = lax.broadcasted_iota(jnp.int32, coded.shape, 0)
        return jnp.where(row < slot_rows - 8, coded, power).astype(jnp.int32).astype(jnp.int16)

    def decode(coded):
        coded = coded.astype(jnp.int32).astype(jnp.float32)
        return coded * jnp.exp2(coded[slot_rows - 8 : slot_rows - 7, 0:1])

    by_x, far, here, by_y = range(CHIPS)
    chip_at = (1, 3, 0, 2)
    wing = dn.shape[3]

    def wing_cols(at_z, j):
        return pl.ds(pl.multiple_of((at_z * 2 + j) * wing, wing), wing)

    def down_half(k, which, first=0, last=CHIPS):
        at_z = order[k]
        weights = jnp.concatenate([dn[at_z, 0], dn[at_z, 1]], axis=1)
        rows = jnp.concatenate([inner[2 * r + which] for r in chip_at[first:last]], axis=0)
        return add_rows(rows, weights).reshape(last - first, slot_rows, weights.shape[1])

    def down_send(k, first=0, last=CHIPS, sem=None):
        at_z = order[k]
        span = pl.ds(first, last - first)
        sem = at_z if sem is None else sem
        part_out[at_z, span] = down_half(k, 1 - n, first, last)
        send(part_out.at[at_z, span], part_in.at[at_z, span], part_r.at[sem], twin)

    def down_own(k):
        part_own[k % 2] = down_half(k, n)

    def down_wing(k, j):
        at_z = order[k]
        peer, away, stay = ((across, (by_x, far), (here, by_y)), (aside, (by_y, far), (here, by_x)))[j]
        lane = pl.ds(j * wing, wing)

        def total(c):
            return part_own[k % 2, c, :, lane] + part_in[at_z, c, :, lane]

        for i, c in enumerate(away):
            share_out[at_z, j, i] = encode(total(c))
        send(share_out.at[at_z, j], share_in.at[at_z, j], share_r.at[at_z, j], peer)
        return total, stay

    def down_keep(k, j, total, stay):
        at_z = order[k]
        kept[at_z, j, 0] = total(stay[0]) + hid[:, wing_cols(at_z, j)]
        kept[at_z, j, 1] = total(stay[1])

    def down_second(k):
        at_z = order[k]
        arrived(part_in.at[at_z], part_r.at[at_z])
        for j in range(2):
            down_keep(k, j, *down_wing(k, j))

    def down_third(k):
        at_z = order[k]
        arrived(share_in.at[at_z, 0], share_r.at[at_z, 0])
        last_out[at_z, 2] = encode(kept[at_z, 0, 1] + decode(share_in[at_z, 0, 1]))
        send(last_out.at[at_z, 2], last_in.at[at_z, 2], last_r.at[at_z, 0], aside)
        resid[0, :, wing_cols(at_z, 0)] = kept[at_z, 0, 0] + decode(share_in[at_z, 0, 0])
        arrived(share_in.at[at_z, 1], share_r.at[at_z, 1])
        pair = pl.ds(0, 2)
        for i in range(2):
            total = kept[at_z, 1, i] + decode(share_in[at_z, 1, i])
            last_out[at_z, i] = encode(total)
            resid[i, :, wing_cols(at_z, 1)] = total
        send(last_out.at[at_z, pair], last_in.at[at_z, pair], last_r.at[at_z, 1], across)

    def down_fourth(k):
        at_z = order[k]
        arrived(last_in.at[at_z, 2], last_r.at[at_z, 0])
        cols = wing_cols(at_z, 0)
        total = resid[0, :, cols] + decode(last_in[at_z, 2])
        resid[0, :, cols] = total
        full_out[at_z] = encode(total)
        send(full_out.at[at_z], full_in.at[at_z], full_r.at[at_z], across)
        arrived(last_in.at[at_z, pl.ds(0, 2)], last_r.at[at_z, 1])
        cols = wing_cols(at_z, 1)
        for i in range(2):
            resid[i, :, cols] = resid[i, :, cols] + decode(last_in[at_z, 1 - i])

    def finish(which, group):
        gate_up(3, 0, 0, which, group)
        for r in chip_at[2 * group : 2 * group + 2]:
            at_slot = 2 * r + which
            inner[at_slot] = (
                jax.nn.gelu(acts[0, at_slot], approximate=True) * acts[1, at_slot]
            ).astype(jnp.bfloat16)

    for j, (_, target) in enumerate(att_sides):
        arrived(target.at[z, 1 - x], x_r.at[2 + j])
    att_side_send(2, 0)
    att_stream(0, 0, ends)
    double_stream(next_a, ends)
    finish(1 - n, 0)
    down_send(0, 0, 2, PLANES)
    summed = found[z].astype(jnp.float32)
    for d in range(1, PLANES):
        q = (z + d) % PLANES
        arrived(found_in.at[q], emb_r.at[q])
        summed = summed + found_in[q].astype(jnp.float32)
    pair_out[...] = summed.astype(jnp.bfloat16)
    send(pair_out, pair_in, one_r.at[1], across)
    finish(n, 0)
    part_own[0, pl.ds(0, 2)] = down_half(0, n, 0, 2)
    pass_on(dn, dn_r, 3, x)
    finish(1 - n, 1)
    down_send(0, 2, CHIPS, PLANES + 1)
    arrived(part_in.at[z, pl.ds(0, 2)], part_r.at[PLANES])
    wing_a = down_wing(0, 0)
    finish(n, 1)
    part_own[0, pl.ds(2, 2)] = down_half(0, n, 2, CHIPS)
    pass_on(dn, dn_r, 3, 1 - x)
    att_stream(0, 0, inside)
    for j in (2, 1):
        att_stream(j, 0, ends)
    arrived(part_in.at[z, pl.ds(2, 2)], part_r.at[PLANES + 1])
    wing_b = down_wing(0, 1)
    end_got(dn, dn_r, 1)
    down_send(1)
    down_keep(0, 0, *wing_a)
    down_keep(0, 1, *wing_b)
    arrived(pair_in, one_r.at[1])
    half = (pair_out[...].astype(jnp.float32) + pair_in[...].astype(jnp.float32)).astype(jnp.bfloat16)
    half_in[n] = half
    send(half_in.at[n], half_in.at[n], one_r.at[2], twin)
    att_pass(0, 1)
    down_own(1)
    down_second(1)
    att_pass(0, 2)
    end_got(dn, dn_r, 2)
    down_send(2)
    down_third(0)
    down_own(2)
    arrived(half_in.at[1 - n], one_r.at[2])
    embedded = jnp.concatenate([half_in[0], half_in[1]], axis=1).astype(jnp.float32)
    dec_rows[0] = rms_scale(embedded, gain_dec[...][None]).astype(jnp.bfloat16)
    send(dec_rows.at[0], dec_rows.at[1], one_r.at[5], aside)
    down_second(2)
    att_pass(0, 3)
    double_stream(next_a, inside)
    att_stream(2, 0, inside)
    send(at_q.at[z], at_q.at[z], at_r.at[1, z], next_b, inside)
    att_pass(2, 1)
    att_pass(1, 1)
    double_stream(next_b, inside)
    down_third(1)
    end_got(dn, dn_r, 3)
    down_send(3)
    down_fourth(0)
    down_own(3)
    down_second(3)
    pl.when(ends)(lambda: arrived(dec_rows.at[1], one_r.at[5]))
    send(dec_rows, dec_end, one_r.at[7], next_a, ends)
    att_end(0, 1)
    att_pass(2, 2)
    double_pass()
    down_third(2)
    pl.when(inside)(lambda: att_got(1, 2))
    att_end(0, 2)
    att_side_send(0, 2, ends)
    down_fourth(1)
    pl.when(inside)(lambda: att_got(1, 3))
    down_third(3)
    att_pass(2, 3)

    @pl.when(inside)
    def _():
        for k in range(PLANES):
            for side in range(2):
                weight_q[pl.ds((2 * k + side) * depth, depth), :] = at_q[k, side]
        arrived(dec_rows.at[1], one_r.at[5])
        arrived(dec_end, one_r.at[7])
        asked = jnp.concatenate([dec_rows[0], dec_rows[1], dec_end[0], dec_end[1]], axis=0)
        asked = add_rows(asked, weight_q[...]).astype(jnp.bfloat16)
        query_rows[0] = asked[:answers]
        query_out[...] = asked[answers : 2 * answers]
        query_end[...] = asked[2 * answers :]

    send(query_out, query_rows.at[1], one_r.at[6], aside, inside)
    send(query_end, query_back, one_r.at[8], next_a, inside)
    for k in range(1, PLANES):
        att_side_send(2, k, inside)
    att_end(0, 3)
    att_side_send(0, 3, ends)
    down_fourth(2)
    att_end(2, 1)
    att_side_send(2, 1, ends)
    down_fourth(3)
    @pl.when(ends)
    def _():
        arrived(query_back, one_r.at[8])
        query_rows[0] = query_back[pl.ds(0, answers), :]
        query_out[...] = query_back[pl.ds(answers, answers), :]

    send(query_out, query_rows.at[1], one_r.at[6], aside, ends)
    for k in (2, 3):
        att_end(2, k)
        att_side_send(2, k, ends)
    for k in range(1, PLANES):
        take = functools.partial(arrived, at_kv.at[1, order[k]], at_yr.at[0, order[k]])
        if k == 1:
            pl.when(ends)(take)
        else:
            take()
    for k in range(PLANES):
        for side in range(2):
            rows = pl.ds((2 * k + side) * depth, depth)
            for h in range(2):
                cols = pl.ds(h * head_cols, head_cols)
                weight_k[rows, cols] = at_kv[h, k, side, pl.ds(0, depth), :]
                weight_v[rows, cols] = at_kv[h, k, side, pl.ds(depth, depth), :]
    for k in range(PLANES):
        at_z = order[k]
        arrived(full_in.at[at_z], full_r.at[at_z])
        resid[1, :, wing_cols(at_z, 0)] = decode(full_in[at_z])
    spots = [2 * x + n, 2 * (1 - x) + n, 2 * x + 1 - n, 2 * (1 - x) + 1 - n]
    for i in range(2):
        mem[spots[i]] = rms_scale(resid[i], gain_out[...][None]).astype(jnp.bfloat16)
        send(mem.at[spots[i]], mem.at[spots[i]], mem_r.at[spots[i]], twin)

    def project(j):
        keys[j] = add_rows(mem[j], weight_k[...]).astype(jnp.bfloat16)
        values[j] = add_rows(mem[j], weight_v[...]).astype(jnp.bfloat16)

    project(spots[0])
    project(spots[1])
    arrived(mem.at[spots[2]], mem_r.at[spots[2]])
    first = mem[2 * x]
    second = mem[2 * x + 1]
    memory_out[pl.ds(0, late), :] = first[:late]
    first, second = first.astype(jnp.float32), second.astype(jnp.float32)
    middle = jnp.concatenate([first[late:seg], second[: slot_rows - seg]], axis=0)
    memory_out[pl.ds(late, slot_rows - late), :] = middle.astype(jnp.bfloat16)
    memory_out[pl.ds(slot_rows, late), :] = second[slot_rows - seg : seg].astype(jnp.bfloat16)
    project(spots[2])
    arrived(mem.at[spots[3]], mem_r.at[spots[3]])
    project(spots[3])
    arrived(lens_all.at[1 - x], one_r.at[0])

    arrived(query_rows.at[1], one_r.at[6])
    query = jnp.concatenate([query_rows[0], query_rows[1]], axis=1)
    columns = 2 * head_cols
    heads = columns // HEAD_DIM
    lane_head = lax.broadcasted_iota(jnp.int32, (answers, columns), 1) // HEAD_DIM
    stacked = jnp.concatenate(
        [jnp.where(lane_head == h, query.astype(jnp.float32), 0.0) for h in range(heads)], axis=0
    ).astype(jnp.bfloat16)
    tokens = 2 * CORES * slot_rows
    key_rows = keys[...].reshape(tokens, columns)
    value_rows = values[...].reshape(tokens, columns)
    scores = dot_t(stacked, key_rows) * (1.0 / math.sqrt(HEAD_DIM))
    token = lax.broadcasted_iota(jnp.int32, (1, tokens), 1)
    live = token < 0
    for j in range(2 * CORES):
        length = lens_all[j // CORES, j % CORES : j % CORES + 1, 0:1]
        live = live | ((token >= j * slot_rows) & (token < j * slot_rows + length))
    scores = jnp.where(live, scores, FLOOR)
    peak = jnp.max(scores, axis=1, keepdims=True)
    weights = jnp.exp(scores - peak)
    total = jnp.sum(weights, axis=1, keepdims=True)
    coarse = weights.astype(jnp.bfloat16)
    fine = (weights - coarse.astype(jnp.float32)).astype(jnp.bfloat16)
    mixed = (add_rows(coarse, value_rows) + add_rows(fine, value_rows)) / total
    attended = jnp.where(lane_head == 0, mixed[:answers], 0.0)
    for h in range(1, heads):
        attended = jnp.where(lane_head == h, mixed[h * answers : (h + 1) * answers], attended)
    for k in range(PLANES):
        arrived(at_o.at[1, k], at_yr.at[1, k])
        for side in range(2):
            for h in range(2):
                cols = pl.ds((2 * k + side) * depth, depth)
                weight_o[pl.ds(h * head_cols, head_cols), cols] = at_o[h, k, side]
    partial = add_rows(attended.astype(jnp.bfloat16), weight_o[...])
    half_cols = partial.shape[1] // 2
    low, high = partial[:, :half_cols], partial[:, half_cols:]

    own = jnp.where(n == 0, low, high)
    tail_out[0] = jnp.where(n == 0, high, low).astype(jnp.bfloat16)
    send(tail_out.at[0], tail_in.at[2], tail_r.at[2], across_twin)
    send(tail_out.at[0], tail_in.at[0], tail_r.at[0], twin)
    tail_out[1] = own.astype(jnp.bfloat16)
    send(tail_out.at[1], tail_in.at[1], tail_r.at[1], across)
    total = half_in[n].astype(jnp.float32) + own
    for j in range(3):
        arrived(tail_in.at[j], tail_r.at[j])
        total = total + tail_in[j].astype(jnp.float32)
    dec_all[z] = total.astype(jnp.bfloat16)
    for d in range(PLANES - 1, 0, -1):
        send(dec_all.at[z], dec_all.at[z], dec_r.at[z], on(x, y, order[d], n))
    for d in range(PLANES):
        q = order[d]
        if d:
            arrived(dec_all.at[q], dec_r.at[q])
        decoded_out[pl.ds(pl.multiple_of(q * answers, answers), answers), :] = dec_all[q]
    for entry in pending[-send_sem.shape[0] :]:
        settle(entry)


def hand_over(memory, decoded, memory_out, decoded_out, sems):
    copies = [
        pltpu.make_async_copy(source, target, sems.at[j])
        for j, (source, target) in enumerate(((memory, memory_out), (decoded, decoded_out)))
    ]
    for copy in copies:
        copy.start()
    for copy in copies:
        copy.wait()


def per_device(
    hidden_in,
    ffn_gain,
    wi_gate,
    wi_up,
    wo_down,
    final_gain,
    key_w,
    value_w,
    query_w,
    out_w,
    dec_gain,
    embed,
    lengths,
    answer_ids,
):
    sizes = tuple(lax.axis_size(a) for a in ("groups", "wide", "narrow"))
    rows_ok = hidden_in.shape[0] % 16 == 0 and lengths.shape[0] == CORES
    if sizes != (2, 2 * PLANES, CORES) or QUEST != PLANES or not rows_ok:
        return per_device_any(
            hidden_in,
            ffn_gain,
            wi_gate,
            wi_up,
            wo_down,
            final_gain,
            key_w,
            value_w,
            query_w,
            out_w,
            dec_gain,
            embed,
            lengths,
            answer_ids,
        )
    rows, features = hidden_in.shape
    slot_rows = -(-(rows // CORES) // 16) * 16
    depth = wi_gate.shape[0]
    unit = wi_gate.shape[1] // CHIPS
    head_cols = key_w.shape[1] // CHIPS
    answers = answer_ids.shape[1]
    width = features // PLANES
    half = features // 2
    bf, f32 = jnp.bfloat16, jnp.float32
    slots = CHIPS * CORES
    wing = width // 2
    dma = pltpu.SemaphoreType.DMA
    vmem = pl.BlockSpec(memory_space=pltpu.VMEM)
    hbm = pl.BlockSpec(memory_space=pl.ANY)
    loaded = (hidden_in, wi_gate, wi_up, wo_down, key_w, value_w, query_w, out_w)
    memory, decoded = pl.pallas_call(
        reader,
        out_shape=(
            pltpu.VMEM((rows, features), bf),
            pltpu.VMEM((QUEST * answers, half), bf),
        ),
        in_specs=[hbm, vmem, hbm, hbm, hbm, vmem, hbm, hbm, hbm, hbm, vmem, hbm]
        + [pl.BlockSpec(memory_space=pltpu.SMEM), vmem],
        out_specs=(vmem, vmem),
        scratch_shapes=[pltpu.VMEM(a.shape, bf) for a in loaded]
        + [
            pltpu.VMEM((slot_rows, features), f32),
            pltpu.VMEM((2, wi_gate.shape[1], depth), bf),
            pltpu.VMEM((PLANES, 2, 2 * unit, depth), bf),
            pltpu.VMEM((2 * unit, depth), bf),
            pltpu.VMEM((PLANES, 2, unit, depth), bf),
            pltpu.VMEM((2, PLANES, 2, 2 * depth, head_cols), bf),
            pltpu.VMEM((PLANES, 2, depth, head_cols), bf),
            pltpu.VMEM((2, PLANES, 2, head_cols, depth), bf),
            pltpu.VMEM((2, 2 * depth, head_cols), bf),
            pltpu.VMEM((depth, head_cols), bf),
            pltpu.VMEM((head_cols, depth), bf),
            pltpu.VMEM((slots, slot_rows, features), bf),
            pltpu.VMEM((2, slots, slot_rows, unit), f32),
            pltpu.VMEM((slots, slot_rows, unit), bf),
            pltpu.VMEM((embed.shape[0], half), bf),
            pltpu.VMEM((2, CHIPS, slot_rows, width), f32),
            pltpu.VMEM((PLANES, CHIPS, slot_rows, width), f32),
            pltpu.VMEM((PLANES, CHIPS, slot_rows, width), f32),
            pltpu.VMEM((PLANES, 2, 2, slot_rows, wing), jnp.int16),
            pltpu.VMEM((PLANES, 2, 2, slot_rows, wing), jnp.int16),
            pltpu.VMEM((PLANES, 2, 2, slot_rows, wing), f32),
            pltpu.VMEM((PLANES, 3, slot_rows, wing), jnp.int16),
            pltpu.VMEM((PLANES, 3, slot_rows, wing), jnp.int16),
            pltpu.VMEM((PLANES, slot_rows, wing), jnp.int16),
            pltpu.VMEM((PLANES, slot_rows, wing), jnp.int16),
            pltpu.VMEM((2, answers, features), bf),
            pltpu.VMEM((2, answers, head_cols), bf),
            pltpu.VMEM((answers, head_cols), bf),
            pltpu.VMEM((2 * answers, head_cols), bf),
            pltpu.VMEM((2 * answers, head_cols), bf),
            pltpu.VMEM((2, answers, features), bf),
            pltpu.VMEM((2, slot_rows, features), f32),
            pltpu.VMEM((2 * CORES, slot_rows, features), bf),
            pltpu.VMEM((QUEST, answers, half), bf),
            pltpu.VMEM((QUEST, answers, half), bf),
            pltpu.VMEM((answers, half), bf),
            pltpu.VMEM((answers, half), bf),
            pltpu.VMEM((CORES, answers, half), bf),
            pltpu.VMEM((2, 8, 128), jnp.int32),
            pltpu.VMEM((features, 2 * head_cols), bf),
            pltpu.VMEM((features, 2 * head_cols), bf),
            pltpu.VMEM((features, head_cols), bf),
            pltpu.VMEM((2 * head_cols, features), bf),
            pltpu.VMEM((2 * CORES, slot_rows, 2 * head_cols), bf),
            pltpu.VMEM((2 * CORES, slot_rows, 2 * head_cols), bf),
            pltpu.VMEM((2, answers, half), bf),
            pltpu.VMEM((3, answers, half), bf),
            pltpu.VMEM((QUEST, answers, half), bf),
            dma((28,)),
            dma((PLANES, 2)),
            dma((6,)),
            dma((PLANES, 2)),
            dma((3, PLANES)),
            dma((2, PLANES)),
            dma((slots + 2,)),
            dma((PLANES + 2,)),
            dma((PLANES, 2)),
            dma((PLANES, 2)),
            dma((PLANES,)),
            dma((3,)),
            dma((len(loaded),)),
            dma((PLANES,)),
            dma((9,)),
            dma((2 * CORES,)),
            dma((PLANES,)),
            dma,
        ],
        compiler_params=pltpu.CompilerParams(
            collective_id=0, has_side_effects=True, vmem_limit_bytes=54 * 2**20
        ),
    )(
        hidden_in,
        ffn_gain,
        wi_gate,
        wi_up,
        wo_down,
        final_gain,
        key_w,
        value_w,
        query_w,
        out_w,
        dec_gain,
        embed,
        lengths,
        answer_ids,
    )
    shapes = [jax.ShapeDtypeStruct(a.shape, bf) for a in (memory, decoded)]
    return pl.pallas_call(
        hand_over,
        out_shape=shapes,
        in_specs=[vmem, vmem],
        out_specs=[hbm, hbm],
        scratch_shapes=[dma((2,))],
        compiler_params=pltpu.CompilerParams(vmem_limit_bytes=2**20),
    )(memory, decoded)


def solution(mesh):
    placed = (
        P(("groups", "wide"), None),
        P(),
        P("wide", "narrow"),
        P("wide", "narrow"),
        P("narrow", "wide"),
        P(),
        P("wide", "narrow"),
        P("wide", "narrow"),
        P("wide", "narrow"),
        P("narrow", "wide"),
        P(),
        P("wide", None),
        P(("groups", "wide")),
        P("groups", None),
    )
    return jax.shard_map(
        per_device,
        mesh=mesh,
        in_specs=placed,
        out_specs=(P(("groups", "wide"), None), P("groups", "narrow")),
        check_vma=False,
    )
```

```python
import functools
import math

import jax
import jax.numpy as jnp
from jax import lax
from jax.experimental import pallas as pl
from jax.experimental.pallas import tpu as pltpu
from jax.sharding import PartitionSpec as P

HEAD_DIM = 64
QUEST = 4


EPS = 1e-06
FLOOR = -1e30


def swap(values, axis, distance=1):
    pairs = [(i, i ^ distance) for i in range(lax.axis_size(axis))]
    return jax.tree.map(lambda a: lax.ppermute(a, axis, pairs), values)


def ordered(bit, own, other, dim):
    first = jnp.where(bit == 0, own, other)
    second = jnp.where(bit == 0, other, own)
    return jnp.concatenate([first, second], axis=dim)


def part(values, index, count, dim):
    size = values.shape[dim] // count
    return lax.dynamic_slice_in_dim(values, index * size, size, dim)


def line_gather(block, place, count):
    size = lax.axis_size("wide")
    stride = size // count
    if count > 8:
        groups = [[i * stride + j for i in range(count)] for j in range(stride)]
        return lax.all_gather(block, "wide", axis_index_groups=groups)
    up = [(i, i + stride) for i in range(size - stride)]
    down = [(i + stride, i) for i in range(size - stride)]
    below, above = [], []
    from_below = from_above = block
    for _ in range(count - 1):
        from_below = lax.ppermute(from_below, "wide", up)
        from_above = lax.ppermute(from_above, "wide", down)
        below.insert(0, from_below)
        above.append(from_above)
    return lax.dynamic_slice_in_dim(
        jnp.stack(below + [block] + above), count - 1 - place, count, 0
    )


def rms_scale(values, gain):
    mean_square = jnp.mean(values * values, axis=-1, keepdims=True)
    return values * lax.rsqrt(mean_square + EPS) * gain.astype(jnp.float32)


def add_rows(left, piece):
    return jnp.dot(left, piece, preferred_element_type=jnp.float32)


def join_partial(first, second):
    top = jnp.maximum(first[0], second[0])
    factor_first = jnp.exp(first[0] - top)
    factor_second = jnp.exp(second[0] - top)
    return (
        top,
        first[1] * factor_first + second[1] * factor_second,
        first[2] * factor_first + second[2] * factor_second,
    )


def per_device_any(
    hidden_in,
    ffn_gain,
    wi_gate,
    wi_up,
    wo_down,
    final_gain,
    key_w,
    value_w,
    query_w,
    out_w,
    dec_gain,
    embed,
    lengths,
    answer_ids,
):
    rows, features = hidden_in.shape
    wide = lax.axis_size("wide")
    group, place, core = (lax.axis_index(a) for a in ("groups", "wide", "narrow"))
    side, pair = place % 2, place // 2
    pairs = wide // 2
    quarters = 2 * lax.axis_size("groups")
    lanes = 128

    def for_side(target, pieces):
        quarter = target * (quarters // 2) + group
        return jnp.concatenate(
            [part(a, quarter, quarters, dim).reshape(-1, lanes) for a, dim in pieces]
        )

    def paired(pieces):
        own = for_side(side, pieces)
        other = swap(for_side(1 - side, pieces), "wide")
        return ordered(side, own[None], other[None], 0)

    def gathered(both):
        return line_gather(both, pair, pairs).reshape(wide, *both.shape[1:])

    hidden_units = wi_gate.shape[1] // quarters
    depth = wi_gate.shape[0]
    ffn = gathered(paired(((wi_gate.T, 0), (wi_up.T, 0), (wo_down, 0))))
    ffn = ffn.reshape(wide, 3, hidden_units, depth).transpose(1, 2, 0, 3)
    gate_t, up_t, down = ffn.reshape(3, hidden_units, features)

    def over_plane(own):
        couple = jnp.concatenate([own, swap(own, "wide")])
        return jnp.concatenate([couple, swap(couple, "groups")])

    def both_halves(own):
        return ordered(core, own, swap(own, "narrow"), 1)

    answers = answer_ids.shape[1]
    per_question = wide // QUEST
    qrows = answer_ids.shape[0] * answers
    vocab_rows = embed.shape[0]
    local_ids = answer_ids.reshape(qrows) - place * vocab_rows
    onehot = (local_ids[:, None] == jnp.arange(vocab_rows, dtype=jnp.int32)[None, :]).astype(
        jnp.bfloat16
    )
    found = jnp.dot(onehot, embed, preferred_element_type=jnp.float32).astype(jnp.bfloat16)
    found = part(found, core, 2, 1)
    distance = wide // 2
    while distance:
        if distance >= per_question:
            bit = place // distance % 2
            found = part(found, bit, 2, 0) + swap(part(found, 1 - bit, 2, 0), "wide", distance)
        else:
            found = found + swap(found, "wide", distance)
        distance //= 2
    embedded_half = found.astype(jnp.float32)
    dec_own = rms_scale(both_halves(found).astype(jnp.float32), dec_gain).astype(jnp.bfloat16)
    dec_in = jnp.concatenate([dec_own, swap(dec_own, "groups")])

    columns = key_w.shape[1] // quarters
    att_pair = paired(((key_w, 1), (value_w, 1), (query_w, 1), (out_w, 0)))
    lengths_all = over_plane(lengths)

    resid_in = hidden_in.astype(jnp.float32)
    enc_own = rms_scale(resid_in, ffn_gain).astype(jnp.bfloat16)
    enc_in = both_halves(over_plane(part(enc_own, core, 2, 1)))
    enc_in, dec_in, lengths_all, att_pair, embedded_half = lax.optimization_barrier(
        (enc_in, dec_in, lengths_all, att_pair, embedded_half)
    )
    contract_last = (((1,), (1,)), ((), ()))
    gate = lax.dot_general(enc_in, gate_t, contract_last, preferred_element_type=jnp.float32)
    up = lax.dot_general(enc_in, up_t, contract_last, preferred_element_type=jnp.float32)
    inner = (jax.nn.gelu(gate, approximate=True) * up).astype(jnp.bfloat16)
    sent_half = add_rows(inner, part(down, 1 - core, 2, 1))
    received_half = swap(sent_half, "narrow")
    sums = add_rows(inner, part(down, core, 2, 1)) + received_half

    def keep_half(values):
        return part(values, core, 2, 1) + swap(part(values, 1 - core, 2, 1), "narrow")

    blocks = sums.reshape(4, rows, -1)
    middle = blocks.shape[2] // 2
    early, late = blocks[:, :, :middle], blocks[:, :, middle:]
    early = early[:2] + swap(early[2:], "groups")
    late = late[::2] + swap(late[1::2], "wide")
    early = early[0] + swap(early[1], "wide")
    late = late[0] + swap(late[1], "groups")
    share = jnp.concatenate([early, late], axis=1)
    resid_half = part(resid_in, core, 2, 1) + share
    own_squares = jnp.sum(resid_half * resid_half, axis=1)
    squares = (own_squares + swap(own_squares, "narrow"))[:, None]
    gain_half = part(final_gain, core, 2, 0).astype(jnp.float32)
    memory_half = (resid_half * lax.rsqrt(squares / features + EPS) * gain_half).astype(
        jnp.bfloat16
    )
    memory_early, memory_late = memory_half[:, :middle], memory_half[:, middle:]
    twin = jnp.stack([memory_late, swap(memory_late, "groups")])
    late_all = jnp.stack([twin, swap(twin, "wide")], axis=1).reshape(4 * rows, middle)
    early_all = over_plane(memory_early)
    early_other, late_other = swap(early_all, "narrow"), swap(late_all, "narrow")
    other_half = jnp.concatenate([early_other[:rows], late_other[:rows]], axis=1)
    memory = ordered(core, memory_half, other_half, 1)

    att = gathered(att_pair)
    att = att.reshape(wide, 4, -1)
    key_q, value_q, query_q = (att[:, i].reshape(features, columns) for i in range(3))
    out_q = att[:, 3].reshape(wide, columns, depth).transpose(1, 0, 2).reshape(columns, features)

    def project(weight):
        own, other = part(weight, core, 2, 0), part(weight, 1 - core, 2, 0)
        return (
            add_rows(early_all, own[:middle])
            + add_rows(late_all, own[middle:])
            + add_rows(early_other, other[:middle])
            + add_rows(late_other, other[middle:])
        ).astype(jnp.bfloat16)

    heads = columns // HEAD_DIM
    keys = project(key_q).reshape(2, 2 * rows, columns)
    values = project(value_q).reshape(2, 2 * rows, columns).astype(jnp.float32)
    query = add_rows(dec_in, query_q).astype(jnp.bfloat16)
    in_head = (
        jnp.arange(columns, dtype=jnp.int32)[None, :] // HEAD_DIM
        == jnp.arange(heads, dtype=jnp.int32)[:, None]
    )[None, :, None, :]
    query_heads = jnp.where(in_head, query.reshape(2, 1, answers, columns), 0)
    scores = jnp.einsum(
        "qhac,qkc->qhak", query_heads, keys, preferred_element_type=jnp.float32
    ) * (1.0 / math.sqrt(HEAD_DIM))
    passage_len = rows // lengths.shape[0]
    live = jnp.arange(passage_len, dtype=jnp.int32)[None, :] < lengths_all[:, None]
    scores = jnp.where(live.reshape(2, 1, 1, 2 * rows), scores, FLOOR)
    top = jnp.max(scores, axis=3, keepdims=True)
    weights = jnp.exp(scores - top)
    total = jnp.sum(weights, axis=3, keepdims=True)
    acc = jnp.einsum("qhak,qkc->qhac", weights, values, precision=lax.Precision.HIGHEST)
    state = (top, total, acc)
    distance = 2
    while distance < per_question:
        state = join_partial(state, swap(state, "wide", distance))
        distance *= 2
    attended = jnp.sum(jnp.where(in_head, state[2] / state[1], 0.0), axis=1)
    attended = attended.astype(jnp.bfloat16).reshape(2 * answers, columns)
    partial_out = keep_half(jnp.dot(attended, out_q, preferred_element_type=jnp.float32))
    share_out = partial_out[:answers] + swap(partial_out[answers:], "groups")
    share_out = share_out + swap(share_out, "wide")
    decoded = (embedded_half + share_out).astype(jnp.bfloat16)
    distance = per_question
    while distance < wide:
        decoded = ordered(place // distance % 2, decoded, swap(decoded, "wide", distance), 0)
        distance *= 2
    return (memory, decoded)


MESH = pl.DeviceIdType.MESH
PLANES = 4
CHIPS = 4
CORES = 2
QUANT = 32767.0


def dot_t(left, right):
    return lax.dot_general(
        left, right, (((1,), (1,)), ((), ())), preferred_element_type=jnp.float32
    )


def reader(
    hidden_hbm,
    gain_in,
    gate_hbm,
    up_hbm,
    down_hbm,
    gain_out,
    key_hbm,
    value_hbm,
    query_hbm,
    out_hbm,
    gain_dec,
    embed,
    lengths,
    ids,
    memory_out,
    decoded_out,
    hidden,
    gate_w,
    up_w,
    down_w,
    key_w,
    value_w,
    query_w,
    out_w,
    hid,
    turned,
    gu,
    gu_side,
    dn,
    at_kv,
    at_q,
    at_o,
    side_kv,
    side_q,
    side_o,
    enc,
    acts,
    inner,
    table,
    part_own,
    part_out,
    part_in,
    share_out,
    share_in,
    kept,
    last_out,
    last_in,
    full_out,
    full_in,
    dec_rows,
    query_rows,
    query_out,
    query_end,
    query_back,
    dec_end,
    resid,
    mem,
    found,
    found_in,
    pair_out,
    pair_in,
    half_in,
    lens_all,
    weight_k,
    weight_v,
    weight_q,
    weight_o,
    keys,
    values,
    tail_out,
    tail_in,
    dec_all,
    send_sem,
    gu_r,
    x_r,
    dn_r,
    at_r,
    at_yr,
    enc_r,
    part_r,
    share_r,
    last_r,
    full_r,
    tail_r,
    load_sem,
    emb_r,
    one_r,
    mem_r,
    dec_r,
    table_sem,
):
    y, place, n = (lax.axis_index(a) for a in ("groups", "wide", "narrow"))
    z, x = place // 2, place % 2
    upper = z // 2
    w = z + upper * (PLANES - 1 - 2 * z)

    def plane(mirrored):
        return mirrored + upper * (PLANES - 1 - 2 * mirrored)

    order = [z, plane(1 - w), plane(2), plane(3)]
    slot_rows = hid.shape[0]
    unit = gu.shape[2] // 2
    head_cols = at_kv.shape[4]

    def on(x_at, y_at, z_at, n_at):
        return {"groups": y_at, "wide": z_at * 2 + x_at, "narrow": n_at}

    across = on(1 - x, y, z, n)
    aside = on(x, 1 - y, z, n)
    corner = on(1 - x, 1 - y, z, n)
    twin = on(x, y, z, 1 - n)
    across_twin = on(1 - x, y, z, 1 - n)
    next_a = on(x, y, order[1], n)
    next_b = on(x, y, plane(2), n)
    inside = w == 1
    ends = w == 0
    pending = []

    def settle(entry):
        copy, cond = entry
        if cond is None:
            copy().wait_send()
        else:
            pl.when(cond)(lambda: copy().wait_send())

    def send(source, target, recv_sem, device, cond=None):
        sem = send_sem.at[len(pending) % send_sem.shape[0]]
        if len(pending) >= send_sem.shape[0]:
            settle(pending[-send_sem.shape[0]])

        def copy():
            return pltpu.make_async_remote_copy(
                source, target, sem, recv_sem, device_id=device, device_id_type=MESH
            )

        if cond is None:
            copy().start()
        else:
            pl.when(cond)(lambda: copy().start())
        pending.append((copy, cond))

    def arrived(target, recv_sem):
        pltpu.make_async_remote_copy(
            target, target, recv_sem, recv_sem, device_id=twin, device_id_type=MESH
        ).wait_recv()

    barrier = pltpu.get_barrier_semaphore()
    peers = [across, aside, corner, twin, across_twin]
    peers += [on(x, y, (z + d) % PLANES, n) for d in range(1, PLANES)]
    for peer in peers:
        pl.semaphore_signal(barrier, inc=1, device_id=peer, device_id_type=MESH)

    loads = [
        pltpu.make_async_copy(source, target, load_sem.at[j])
        for j, (source, target) in enumerate(
            (
                (gate_hbm, gate_w),
                (up_hbm, up_w),
                (hidden_hbm, hidden),
                (down_hbm, down_w),
                (key_hbm, key_w),
                (value_hbm, value_w),
                (query_hbm, query_w),
                (out_hbm, out_w),
            )
        )
    ]
    for copy in loads:
        copy.start()
    table_copy = pltpu.make_async_copy(
        embed.at[:, pl.ds(pl.multiple_of(n * table.shape[1], 128), table.shape[1])],
        table,
        table_sem,
    )
    table_copy.start()

    lanes = 128
    for j, array in enumerate((gate_w, up_w)):
        loads[j].wait()
        for k in range(array.shape[1] // lanes):
            cols = pl.ds(k * lanes, lanes)
            turned[j, cols, :] = array[:, cols].T
    mine = pl.multiple_of((2 * x + y) * unit, 16)
    theirs = pl.multiple_of((2 * (1 - x) + y) * unit, 16)
    for j in range(2):
        gu_side[pl.ds(j * unit, unit), :] = turned[j, pl.ds(theirs, unit), :]
        gu[z, x, pl.ds(j * unit, unit), :] = turned[j, pl.ds(mine, unit), :]
    pl.semaphore_wait(barrier, len(peers))

    def stream(buf, r_sem, k, side):
        at_z = order[k]
        if k == 0:
            send(buf.at[at_z, side], buf.at[at_z, side], r_sem.at[at_z, side], next_a)
            send(buf.at[at_z, side], buf.at[at_z, side], r_sem.at[at_z, side], next_b, inside)
        else:
            target = next_b if k == 1 else next_a
            send(buf.at[at_z, side], buf.at[at_z, side], r_sem.at[at_z, side], target, inside)

    streams = ((at_kv.at[0], 0), (at_q, 1), (at_o.at[0], 2))

    def att_stream(j, k, cond=None):
        buf = streams[j][0].at[order[k]]
        if k == 0:
            send(buf, buf, at_r.at[j, order[0]], next_a, cond)
            if cond is not ends:
                send(buf, buf, at_r.at[j, order[0]], next_b, inside)
        else:
            send(buf, buf, at_r.at[j, order[k]], next_b if k == 1 else next_a, inside)

    def double_stream(device, cond):
        buf = at_kv.at[1, z]
        send(buf, buf, at_yr.at[0, z], device, cond)

    def double_pass():
        buf, sem = at_kv.at[1, order[1]], at_yr.at[0, order[1]]
        pl.when(inside)(lambda: arrived(buf, sem))
        send(buf, buf, sem, next_b, inside)

    def att_got(j, k):
        arrived(streams[j][0].at[order[k]], at_r.at[j, order[k]])

    def att_pass(j, k):
        pl.when(inside)(lambda: att_got(j, k))
        att_stream(j, k)

    def att_end(j, k):
        pl.when(w == 0)(lambda: att_got(j, k))

    def att_side_send(j, k, cond=None):
        buf, sem = ((at_kv, 0), None, (at_o, 1))[j]
        at_z = order[k]
        send(buf.at[0, at_z], buf.at[1, at_z], at_yr.at[sem, at_z], aside, cond)

    def got(buf, r_sem, k, side):
        arrived(buf.at[order[k], side], r_sem.at[order[k], side])

    for j in range(2):
        rows = pl.ds(j * unit, unit)
        send(gu_side.at[rows], gu.at[z, x, rows], x_r.at[j], across)
    stream(gu, gu_r, 0, x)

    loads[2].wait()
    seg = hidden.shape[0] // CORES
    late = hidden.shape[0] - slot_rows
    low = hidden[pl.ds(0, slot_rows), :].astype(jnp.float32)
    high = hidden[pl.ds(late, slot_rows), :].astype(jnp.float32)
    skip = seg - late
    hid[...] = jnp.where(n == 0, low, jnp.concatenate([high[skip:], high[:skip]], axis=0))
    enc[n] = rms_scale(hid[...], gain_in[...][None]).astype(jnp.bfloat16)
    for j, (peer, r) in enumerate(((across, 1), (aside, 2), (twin, 0))):
        send(enc.at[n], enc.at[2 * r + n], enc_r.at[2 * r + n], peer)
    for copy in loads[3:]:
        copy.wait()
    dn[z, x] = down_w[pl.ds(mine, unit), :]
    depth = key_w.shape[0]

    def columns_of(x_at, y_at):
        return pl.ds(pl.multiple_of((2 * x_at + y_at) * head_cols, head_cols), head_cols)

    for x_at, kv_of, q_of, o_of in (
        (x, [at_kv.at[h, z, x] for h in range(2)], at_q.at[z, x], at_o.at[0, z, x]),
        (1 - x, [side_kv.at[h] for h in range(2)], side_q, side_o),
    ):
        for h, y_at in enumerate((y, 1 - y)):
            for j, array in enumerate((key_w, value_w)):
                kv_of[h][pl.ds(j * depth, depth), :] = array[:, columns_of(x_at, y_at)]
        q_of[...] = query_w[:, columns_of(x_at, y)]
        o_of[...] = out_w[columns_of(x_at, y), :]
    tile_row = lax.broadcasted_iota(jnp.int32, lens_all.shape[1:], 0)
    lens_all[x] = jnp.where(tile_row == 0, lengths[0], lengths[1])

    send(down_w.at[pl.ds(theirs, unit), :], dn.at[z, x], dn_r.at[z, x], across)
    send(lens_all.at[x], lens_all.at[x], one_r.at[0], across)
    att_sides = (
        (side_kv.at[0], at_kv.at[0]),
        (side_q, at_q),
        (side_o, at_o.at[0]),
        (side_kv.at[1], at_kv.at[1]),
    )

    def pass_on(buf, r_sem, k, side):
        @pl.when(inside)
        def _():
            got(buf, r_sem, k, side)

        stream(buf, r_sem, k, side)

    def end_got(buf, r_sem, k):
        @pl.when(w == 0)
        def _():
            for side in (x, 1 - x):
                got(buf, r_sem, k, side)

    for j in range(2):
        rows = pl.ds(j * unit, unit)
        piece = gu.at[z, 1 - x, rows]
        arrived(piece, x_r.at[j])
        send(piece, piece, gu_r.at[z, 1 - x], next_a)
        send(piece, piece, gu_r.at[z, 1 - x], next_b, inside)
    for side in (x, 1 - x):
        for k in (2, 1):
            pass_on(gu, gu_r, k, side)

    feat_half = enc.shape[2] // 2
    halves = [pl.ds(0, feat_half), pl.ds(feat_half, feat_half)]
    for j, (r, peer) in enumerate(((1, aside), (2, across))):
        arrived(enc.at[2 * r + n], enc_r.at[2 * r + n])
        send(enc.at[2 * r + n, :, halves[j]], enc.at[6 + n, :, halves[j]], enc_r.at[8 + j], peer)
    for r in (1, 2):
        send(enc.at[2 * r + n], enc.at[2 * r + n], enc_r.at[2 * r + n], twin)
    for j, (source, target) in enumerate(att_sides):
        send(source, target.at[z, x], x_r.at[2 + j], across)

    pass_on(gu, gu_r, 3, x)

    table_copy.wait()
    vocab = table.shape[0]
    total_ids = ids.shape[0] * ids.shape[1]
    all_ids = jnp.concatenate([ids[q : q + 1, :] for q in range(ids.shape[0])], axis=1)
    chunk = 1024
    hits = jnp.zeros((total_ids, table.shape[1]), jnp.float32)
    for base in range(0, vocab, chunk):
        size = min(chunk, vocab - base)
        row = lax.broadcasted_iota(jnp.int32, (size, total_ids), 0) + (place * vocab + base)
        onehot = (row == all_ids).astype(jnp.bfloat16)
        hits = hits + lax.dot_general(
            onehot,
            table[pl.ds(base, size), :],
            (((0,), (0,)), ((), ())),
            preferred_element_type=jnp.float32,
        )
    answers = found.shape[1]
    for q in range(PLANES):
        found[q] = hits[q * answers : (q + 1) * answers].astype(jnp.bfloat16)

    def gate_up(k, first_r, last_r, which=None, group=0):
        at_z = order[k]
        width = 2 * gu.shape[3]
        cols = pl.ds(pl.multiple_of(at_z * width, width), width)
        weights = [
            jnp.concatenate(
                [gu[at_z, 0, pl.ds(j * unit, unit), :], gu[at_z, 1, pl.ds(j * unit, unit), :]], axis=1
            )
            for j in range(2)
        ]

        def rows_of(first, second):
            rows = jnp.concatenate([enc[first, :, cols], enc[second, :, cols]], axis=0)
            for j in range(2):
                value = dot_t(rows, weights[j])
                for i, at_slot in enumerate((first, second)):
                    part_value = value[i * slot_rows : (i + 1) * slot_rows]
                    acts[j, at_slot] = part_value + acts[j, at_slot] if k else part_value

        def body(i, carry):
            rows_of(2 * i, 2 * i + 1)
            return carry

        if which is None:
            lax.fori_loop(first_r, last_r, body, 0)
        else:
            first, second = (1, 3) if group == 0 else (0, 2)
            rows_of(2 * first + which, 2 * second + which)

    for r in (0, 1, 2):
        arrived(enc.at[2 * r + 1 - n], enc_r.at[2 * r + 1 - n])
    gate_up(0, 0, 3)
    pass_on(gu, gu_r, 3, 1 - x)
    for d in range(1, PLANES):
        q = (z + d) % PLANES
        send(found.at[q], found_in.at[z], emb_r.at[z], on(x, y, q, n))
    stream(dn, dn_r, 0, x)
    end_got(gu, gu_r, 1)
    gate_up(1, 0, 3)
    end_got(gu, gu_r, 2)
    gate_up(2, 0, 3)
    got(dn, dn_r, 0, 1 - x)
    stream(dn, dn_r, 0, 1 - x)
    for j in range(2):
        arrived(enc.at[6 + n, :, halves[j]], enc_r.at[8 + j])
    send(enc.at[6 + n], enc.at[6 + n], enc_r.at[6 + n], twin)
    pass_on(dn, dn_r, 2, x)
    pass_on(dn, dn_r, 1, x)
    arrived(enc.at[7 - n], enc_r.at[7 - n])
    for k in range(3):
        gate_up(k, 3, 4)
    pass_on(dn, dn_r, 2, 1 - x)
    pass_on(dn, dn_r, 1, 1 - x)
    end_got(gu, gu_r, 3)

    def exponent(top):
        return jnp.ceil(jnp.log(jnp.maximum(top, 1e-30) / QUANT) * (1.0 / math.log(2.0)) + 0.01)

    def encode(total):
        top = jnp.max(jnp.max(jnp.abs(total), axis=0, keepdims=True), axis=1, keepdims=True)
        power = exponent(top)
        coded = jnp.round(total * jnp.exp2(-power))
        row = lax.broadcasted_iota(jnp.int32, coded.shape, 0)
        return jnp.where(row < slot_rows - 8, coded, power).astype(jnp.int32).astype(jnp.int16)

    def decode(coded):
        coded = coded.astype(jnp.int32).astype(jnp.float32)
        return coded * jnp.exp2(coded[slot_rows - 8 : slot_rows - 7, 0:1])

    by_x, far, here, by_y = range(CHIPS)
    chip_at = (1, 3, 0, 2)
    wing = dn.shape[3]

    def wing_cols(at_z, j):
        return pl.ds(pl.multiple_of((at_z * 2 + j) * wing, wing), wing)

    def down_half(k, which, first=0, last=CHIPS):
        at_z = order[k]
        weights = jnp.concatenate([dn[at_z, 0], dn[at_z, 1]], axis=1)
        rows = jnp.concatenate([inner[2 * r + which] for r in chip_at[first:last]], axis=0)
        return add_rows(rows, weights).reshape(last - first, slot_rows, weights.shape[1])

    def down_send(k, first=0, last=CHIPS, sem=None):
        at_z = order[k]
        span = pl.ds(first, last - first)
        sem = at_z if sem is None else sem
        part_out[at_z, span] = down_half(k, 1 - n, first, last)
        send(part_out.at[at_z, span], part_in.at[at_z, span], part_r.at[sem], twin)

    def down_own(k):
        part_own[k % 2] = down_half(k, n)

    def down_wing(k, j):
        at_z = order[k]
        peer, away, stay = ((across, (by_x, far), (here, by_y)), (aside, (by_y, far), (here, by_x)))[j]
        lane = pl.ds(j * wing, wing)

        def total(c):
            return part_own[k % 2, c, :, lane] + part_in[at_z, c, :, lane]

        for i, c in enumerate(away):
            share_out[at_z, j, i] = encode(total(c))
        send(share_out.at[at_z, j], share_in.at[at_z, j], share_r.at[at_z, j], peer)
        return total, stay

    def down_keep(k, j, total, stay):
        at_z = order[k]
        kept[at_z, j, 0] = total(stay[0]) + hid[:, wing_cols(at_z, j)]
        kept[at_z, j, 1] = total(stay[1])

    def down_second(k):
        at_z = order[k]
        arrived(part_in.at[at_z], part_r.at[at_z])
        for j in range(2):
            down_keep(k, j, *down_wing(k, j))

    def down_third(k):
        at_z = order[k]
        arrived(share_in.at[at_z, 0], share_r.at[at_z, 0])
        last_out[at_z, 2] = encode(kept[at_z, 0, 1] + decode(share_in[at_z, 0, 1]))
        send(last_out.at[at_z, 2], last_in.at[at_z, 2], last_r.at[at_z, 0], aside)
        resid[0, :, wing_cols(at_z, 0)] = kept[at_z, 0, 0] + decode(share_in[at_z, 0, 0])
        arrived(share_in.at[at_z, 1], share_r.at[at_z, 1])
        pair = pl.ds(0, 2)
        for i in range(2):
            total = kept[at_z, 1, i] + decode(share_in[at_z, 1, i])
            last_out[at_z, i] = encode(total)
            resid[i, :, wing_cols(at_z, 1)] = total
        send(last_out.at[at_z, pair], last_in.at[at_z, pair], last_r.at[at_z, 1], across)

    def down_fourth(k):
        at_z = order[k]
        arrived(last_in.at[at_z, 2], last_r.at[at_z, 0])
        cols = wing_cols(at_z, 0)
        total = resid[0, :, cols] + decode(last_in[at_z, 2])
        resid[0, :, cols] = total
        full_out[at_z] = encode(total)
        send(full_out.at[at_z], full_in.at[at_z], full_r.at[at_z], across)
        arrived(last_in.at[at_z, pl.ds(0, 2)], last_r.at[at_z, 1])
        cols = wing_cols(at_z, 1)
        for i in range(2):
            resid[i, :, cols] = resid[i, :, cols] + decode(last_in[at_z, 1 - i])

    def finish(which, group):
        gate_up(3, 0, 0, which, group)
        for r in chip_at[2 * group : 2 * group + 2]:
            at_slot = 2 * r + which
            inner[at_slot] = (
                jax.nn.gelu(acts[0, at_slot], approximate=True) * acts[1, at_slot]
            ).astype(jnp.bfloat16)

    for j, (_, target) in enumerate(att_sides):
        arrived(target.at[z, 1 - x], x_r.at[2 + j])
    att_side_send(2, 0)
    att_stream(0, 0, ends)
    double_stream(next_a, ends)
    finish(1 - n, 0)
    down_send(0, 0, 2, PLANES)
    summed = found[z].astype(jnp.float32)
    for d in range(1, PLANES):
        q = (z + d) % PLANES
        arrived(found_in.at[q], emb_r.at[q])
        summed = summed + found_in[q].astype(jnp.float32)
    pair_out[...] = summed.astype(jnp.bfloat16)
    send(pair_out, pair_in, one_r.at[1], across)
    finish(n, 0)
    part_own[0, pl.ds(0, 2)] = down_half(0, n, 0, 2)
    pass_on(dn, dn_r, 3, x)
    finish(1 - n, 1)
    down_send(0, 2, CHIPS, PLANES + 1)
    arrived(part_in.at[z, pl.ds(0, 2)], part_r.at[PLANES])
    wing_a = down_wing(0, 0)
    finish(n, 1)
    part_own[0, pl.ds(2, 2)] = down_half(0, n, 2, CHIPS)
    pass_on(dn, dn_r, 3, 1 - x)
    att_stream(0, 0, inside)
    for j in (2, 1):
        att_stream(j, 0, ends)
    arrived(part_in.at[z, pl.ds(2, 2)], part_r.at[PLANES + 1])
    wing_b = down_wing(0, 1)
    end_got(dn, dn_r, 1)
    down_send(1)
    down_keep(0, 0, *wing_a)
    down_keep(0, 1, *wing_b)
    arrived(pair_in, one_r.at[1])
    half = (pair_out[...].astype(jnp.float32) + pair_in[...].astype(jnp.float32)).astype(jnp.bfloat16)
    half_in[n] = half
    send(half_in.at[n], half_in.at[n], one_r.at[2], twin)
    att_pass(0, 1)
    down_own(1)
    down_second(1)
    att_pass(0, 2)
    end_got(dn, dn_r, 2)
    down_send(2)
    down_third(0)
    down_own(2)
    arrived(half_in.at[1 - n], one_r.at[2])
    embedded = jnp.concatenate([half_in[0], half_in[1]], axis=1).astype(jnp.float32)
    dec_rows[0] = rms_scale(embedded, gain_dec[...][None]).astype(jnp.bfloat16)
    send(dec_rows.at[0], dec_rows.at[1], one_r.at[5], aside)
    down_second(2)
    att_pass(0, 3)
    double_stream(next_a, inside)
    att_stream(2, 0, inside)
    send(at_q.at[z], at_q.at[z], at_r.at[1, z], next_b, inside)
    att_pass(2, 1)
    att_pass(1, 1)
    double_stream(next_b, inside)
    down_third(1)
    end_got(dn, dn_r, 3)
    down_send(3)
    down_fourth(0)
    down_own(3)
    down_second(3)
    pl.when(ends)(lambda: arrived(dec_rows.at[1], one_r.at[5]))
    send(dec_rows, dec_end, one_r.at[7], next_a, ends)
    att_end(0, 1)
    att_pass(2, 2)
    double_pass()
    down_third(2)
    pl.when(inside)(lambda: att_got(1, 2))
    att_end(0, 2)
    att_side_send(0, 2, ends)
    down_fourth(1)
    pl.when(inside)(lambda: att_got(1, 3))
    down_third(3)
    att_pass(2, 3)

    @pl.when(inside)
    def _():
        for k in range(PLANES):
            for side in range(2):
                weight_q[pl.ds((2 * k + side) * depth, depth), :] = at_q[k, side]
        arrived(dec_rows.at[1], one_r.at[5])
        arrived(dec_end, one_r.at[7])
        asked = jnp.concatenate([dec_rows[0], dec_rows[1], dec_end[0], dec_end[1]], axis=0)
        asked = add_rows(asked, weight_q[...]).astype(jnp.bfloat16)
        query_rows[0] = asked[:answers]
        query_out[...] = asked[answers : 2 * answers]
        query_end[...] = asked[2 * answers :]

    send(query_out, query_rows.at[1], one_r.at[6], aside, inside)
    send(query_end, query_back, one_r.at[8], next_a, inside)
    for k in range(1, PLANES):
        att_side_send(2, k, inside)
    att_end(0, 3)
    att_side_send(0, 3, ends)
    down_fourth(2)
    att_end(2, 1)
    att_side_send(2, 1, ends)
    down_fourth(3)
    spots = [2 * x + n, 2 * (1 - x) + n, 2 * x + 1 - n, 2 * (1 - x) + 1 - n]
    mem[spots[0]] = rms_scale(resid[0], gain_out[...][None]).astype(jnp.bfloat16)
    send(mem.at[spots[0]], mem.at[spots[0]], mem_r.at[spots[0]], twin)
    @pl.when(ends)
    def _():
        arrived(query_back, one_r.at[8])
        query_rows[0] = query_back[pl.ds(0, answers), :]
        query_out[...] = query_back[pl.ds(answers, answers), :]

    send(query_out, query_rows.at[1], one_r.at[6], aside, ends)
    for k in (2, 3):
        att_end(2, k)
        att_side_send(2, k, ends)
    for k in range(1, PLANES):
        take = functools.partial(arrived, at_kv.at[1, order[k]], at_yr.at[0, order[k]])
        if k == 1:
            pl.when(ends)(take)
        else:
            take()
    for k in range(PLANES):
        for side in range(2):
            rows = pl.ds((2 * k + side) * depth, depth)
            for h in range(2):
                cols = pl.ds(h * head_cols, head_cols)
                weight_k[rows, cols] = at_kv[h, k, side, pl.ds(0, depth), :]
                weight_v[rows, cols] = at_kv[h, k, side, pl.ds(depth, depth), :]
    def project(j):
        keys[j] = add_rows(mem[j], weight_k[...]).astype(jnp.bfloat16)
        values[j] = add_rows(mem[j], weight_v[...]).astype(jnp.bfloat16)

    project(spots[0])
    arrived(mem.at[spots[2]], mem_r.at[spots[2]])
    project(spots[2])
    for k in range(PLANES):
        at_z = order[k]
        arrived(full_in.at[at_z], full_r.at[at_z])
        resid[1, :, wing_cols(at_z, 0)] = decode(full_in[at_z])
    mem[spots[1]] = rms_scale(resid[1], gain_out[...][None]).astype(jnp.bfloat16)
    send(mem.at[spots[1]], mem.at[spots[1]], mem_r.at[spots[1]], twin)
    project(spots[1])
    first = mem[2 * x]
    second = mem[2 * x + 1]
    memory_out[pl.ds(0, late), :] = first[:late]
    first, second = first.astype(jnp.float32), second.astype(jnp.float32)
    middle = jnp.concatenate([first[late:seg], second[: slot_rows - seg]], axis=0)
    memory_out[pl.ds(late, slot_rows - late), :] = middle.astype(jnp.bfloat16)
    memory_out[pl.ds(slot_rows, late), :] = second[slot_rows - seg : seg].astype(jnp.bfloat16)
    arrived(mem.at[spots[3]], mem_r.at[spots[3]])
    project(spots[3])
    arrived(lens_all.at[1 - x], one_r.at[0])

    arrived(query_rows.at[1], one_r.at[6])
    query = jnp.concatenate([query_rows[0], query_rows[1]], axis=1)
    columns = 2 * head_cols
    heads = columns // HEAD_DIM
    lane_head = lax.broadcasted_iota(jnp.int32, (answers, columns), 1) // HEAD_DIM
    stacked = jnp.concatenate(
        [jnp.where(lane_head == h, query.astype(jnp.float32), 0.0) for h in range(heads)], axis=0
    ).astype(jnp.bfloat16)
    tokens = 2 * CORES * slot_rows
    key_rows = keys[...].reshape(tokens, columns)
    value_rows = values[...].reshape(tokens, columns)
    scores = dot_t(stacked, key_rows) * (1.0 / math.sqrt(HEAD_DIM))
    token = lax.broadcasted_iota(jnp.int32, (1, tokens), 1)
    live = token < 0
    for j in range(2 * CORES):
        length = lens_all[j // CORES, j % CORES : j % CORES + 1, 0:1]
        live = live | ((token >= j * slot_rows) & (token < j * slot_rows + length))
    scores = jnp.where(live, scores, FLOOR)
    peak = jnp.max(scores, axis=1, keepdims=True)
    weights = jnp.exp(scores - peak)
    total = jnp.sum(weights, axis=1, keepdims=True)
    coarse = weights.astype(jnp.bfloat16)
    fine = (weights - coarse.astype(jnp.float32)).astype(jnp.bfloat16)
    mixed = (add_rows(coarse, value_rows) + add_rows(fine, value_rows)) / total
    attended = jnp.where(lane_head == 0, mixed[:answers], 0.0)
    for h in range(1, heads):
        attended = jnp.where(lane_head == h, mixed[h * answers : (h + 1) * answers], attended)
    for k in range(PLANES):
        arrived(at_o.at[1, k], at_yr.at[1, k])
        for side in range(2):
            for h in range(2):
                cols = pl.ds((2 * k + side) * depth, depth)
                weight_o[pl.ds(h * head_cols, head_cols), cols] = at_o[h, k, side]
    partial = add_rows(attended.astype(jnp.bfloat16), weight_o[...])
    half_cols = partial.shape[1] // 2
    low, high = partial[:, :half_cols], partial[:, half_cols:]

    own = jnp.where(n == 0, low, high)
    tail_out[0] = jnp.where(n == 0, high, low).astype(jnp.bfloat16)
    send(tail_out.at[0], tail_in.at[2], tail_r.at[2], across_twin)
    send(tail_out.at[0], tail_in.at[0], tail_r.at[0], twin)
    tail_out[1] = own.astype(jnp.bfloat16)
    send(tail_out.at[1], tail_in.at[1], tail_r.at[1], across)
    total = half_in[n].astype(jnp.float32) + own
    for j in range(3):
        arrived(tail_in.at[j], tail_r.at[j])
        total = total + tail_in[j].astype(jnp.float32)
    dec_all[z] = total.astype(jnp.bfloat16)
    for d in range(PLANES - 1, 0, -1):
        send(dec_all.at[z], dec_all.at[z], dec_r.at[z], on(x, y, order[d], n))
    for d in range(PLANES):
        q = order[d]
        if d:
            arrived(dec_all.at[q], dec_r.at[q])
        decoded_out[pl.ds(pl.multiple_of(q * answers, answers), answers), :] = dec_all[q]
    for entry in pending[-send_sem.shape[0] :]:
        settle(entry)


def hand_over(memory, decoded, memory_out, decoded_out, sems):
    copies = [
        pltpu.make_async_copy(source, target, sems.at[j])
        for j, (source, target) in enumerate(((memory, memory_out), (decoded, decoded_out)))
    ]
    for copy in copies:
        copy.start()
    for copy in copies:
        copy.wait()


def per_device(
    hidden_in,
    ffn_gain,
    wi_gate,
    wi_up,
    wo_down,
    final_gain,
    key_w,
    value_w,
    query_w,
    out_w,
    dec_gain,
    embed,
    lengths,
    answer_ids,
):
    sizes = tuple(lax.axis_size(a) for a in ("groups", "wide", "narrow"))
    rows_ok = hidden_in.shape[0] % 16 == 0 and lengths.shape[0] == CORES
    if sizes != (2, 2 * PLANES, CORES) or QUEST != PLANES or not rows_ok:
        return per_device_any(
            hidden_in,
            ffn_gain,
            wi_gate,
            wi_up,
            wo_down,
            final_gain,
            key_w,
            value_w,
            query_w,
            out_w,
            dec_gain,
            embed,
            lengths,
            answer_ids,
        )
    rows, features = hidden_in.shape
    slot_rows = -(-(rows // CORES) // 16) * 16
    depth = wi_gate.shape[0]
    unit = wi_gate.shape[1] // CHIPS
    head_cols = key_w.shape[1] // CHIPS
    answers = answer_ids.shape[1]
    width = features // PLANES
    half = features // 2
    bf, f32 = jnp.bfloat16, jnp.float32
    slots = CHIPS * CORES
    wing = width // 2
    dma = pltpu.SemaphoreType.DMA
    vmem = pl.BlockSpec(memory_space=pltpu.VMEM)
    hbm = pl.BlockSpec(memory_space=pl.ANY)
    loaded = (hidden_in, wi_gate, wi_up, wo_down, key_w, value_w, query_w, out_w)
    memory, decoded = pl.pallas_call(
        reader,
        out_shape=(
            pltpu.VMEM((rows, features), bf),
            pltpu.VMEM((QUEST * answers, half), bf),
        ),
        in_specs=[hbm, vmem, hbm, hbm, hbm, vmem, hbm, hbm, hbm, hbm, vmem, hbm]
        + [pl.BlockSpec(memory_space=pltpu.SMEM), vmem],
        out_specs=(vmem, vmem),
        scratch_shapes=[pltpu.VMEM(a.shape, bf) for a in loaded]
        + [
            pltpu.VMEM((slot_rows, features), f32),
            pltpu.VMEM((2, wi_gate.shape[1], depth), bf),
            pltpu.VMEM((PLANES, 2, 2 * unit, depth), bf),
            pltpu.VMEM((2 * unit, depth), bf),
            pltpu.VMEM((PLANES, 2, unit, depth), bf),
            pltpu.VMEM((2, PLANES, 2, 2 * depth, head_cols), bf),
            pltpu.VMEM((PLANES, 2, depth, head_cols), bf),
            pltpu.VMEM((2, PLANES, 2, head_cols, depth), bf),
            pltpu.VMEM((2, 2 * depth, head_cols), bf),
            pltpu.VMEM((depth, head_cols), bf),
            pltpu.VMEM((head_cols, depth), bf),
            pltpu.VMEM((slots, slot_rows, features), bf),
            pltpu.VMEM((2, slots, slot_rows, unit), f32),
            pltpu.VMEM((slots, slot_rows, unit), bf),
            pltpu.VMEM((embed.shape[0], half), bf),
            pltpu.VMEM((2, CHIPS, slot_rows, width), f32),
            pltpu.VMEM((PLANES, CHIPS, slot_rows, width), f32),
            pltpu.VMEM((PLANES, CHIPS, slot_rows, width), f32),
            pltpu.VMEM((PLANES, 2, 2, slot_rows, wing), jnp.int16),
            pltpu.VMEM((PLANES, 2, 2, slot_rows, wing), jnp.int16),
            pltpu.VMEM((PLANES, 2, 2, slot_rows, wing), f32),
            pltpu.VMEM((PLANES, 3, slot_rows, wing), jnp.int16),
            pltpu.VMEM((PLANES, 3, slot_rows, wing), jnp.int16),
            pltpu.VMEM((PLANES, slot_rows, wing), jnp.int16),
            pltpu.VMEM((PLANES, slot_rows, wing), jnp.int16),
            pltpu.VMEM((2, answers, features), bf),
            pltpu.VMEM((2, answers, head_cols), bf),
            pltpu.VMEM((answers, head_cols), bf),
            pltpu.VMEM((2 * answers, head_cols), bf),
            pltpu.VMEM((2 * answers, head_cols), bf),
            pltpu.VMEM((2, answers, features), bf),
            pltpu.VMEM((2, slot_rows, features), f32),
            pltpu.VMEM((2 * CORES, slot_rows, features), bf),
            pltpu.VMEM((QUEST, answers, half), bf),
            pltpu.VMEM((QUEST, answers, half), bf),
            pltpu.VMEM((answers, half), bf),
            pltpu.VMEM((answers, half), bf),
            pltpu.VMEM((CORES, answers, half), bf),
            pltpu.VMEM((2, 8, 128), jnp.int32),
            pltpu.VMEM((features, 2 * head_cols), bf),
            pltpu.VMEM((features, 2 * head_cols), bf),
            pltpu.VMEM((features, head_cols), bf),
            pltpu.VMEM((2 * head_cols, features), bf),
            pltpu.VMEM((2 * CORES, slot_rows, 2 * head_cols), bf),
            pltpu.VMEM((2 * CORES, slot_rows, 2 * head_cols), bf),
            pltpu.VMEM((2, answers, half), bf),
            pltpu.VMEM((3, answers, half), bf),
            pltpu.VMEM((QUEST, answers, half), bf),
            dma((28,)),
            dma((PLANES, 2)),
            dma((6,)),
            dma((PLANES, 2)),
            dma((3, PLANES)),
            dma((2, PLANES)),
            dma((slots + 2,)),
            dma((PLANES + 2,)),
            dma((PLANES, 2)),
            dma((PLANES, 2)),
            dma((PLANES,)),
            dma((3,)),
            dma((len(loaded),)),
            dma((PLANES,)),
            dma((9,)),
            dma((2 * CORES,)),
            dma((PLANES,)),
            dma,
        ],
        compiler_params=pltpu.CompilerParams(
            collective_id=0, has_side_effects=True, vmem_limit_bytes=54 * 2**20
        ),
    )(
        hidden_in,
        ffn_gain,
        wi_gate,
        wi_up,
        wo_down,
        final_gain,
        key_w,
        value_w,
        query_w,
        out_w,
        dec_gain,
        embed,
        lengths,
        answer_ids,
    )
    shapes = [jax.ShapeDtypeStruct(a.shape, bf) for a in (memory, decoded)]
    return pl.pallas_call(
        hand_over,
        out_shape=shapes,
        in_specs=[vmem, vmem],
        out_specs=[hbm, hbm],
        scratch_shapes=[dma((2,))],
        compiler_params=pltpu.CompilerParams(vmem_limit_bytes=2**20),
    )(memory, decoded)


def solution(mesh):
    placed = (
        P(("groups", "wide"), None),
        P(),
        P("wide", "narrow"),
        P("wide", "narrow"),
        P("narrow", "wide"),
        P(),
        P("wide", "narrow"),
        P("wide", "narrow"),
        P("wide", "narrow"),
        P("narrow", "wide"),
        P(),
        P("wide", None),
        P(("groups", "wide")),
        P("groups", None),
    )
    return jax.shard_map(
        per_device,
        mesh=mesh,
        in_specs=placed,
        out_specs=(P(("groups", "wide"), None), P("groups", "narrow")),
        check_vma=False,
    )
```
